32 devices in a mesh: seq: 8 (over z, y), opt: 4 (over x, core).
Axes of the slice: x: 2, y: 2, z: 4, core: 2. Of those that a mesh axis runs over, the one named last changes fastest.
Arguments:
- layer_in: bfloat16 [4, 4096, 4096], P('opt', 'seq'), may hold values from -48 to 48, as said below
- ssm_input: bfloat16 [4, 4096, 4096], P('opt', 'seq'), may hold values from -0.119628906 to 0.119628906
- grad_out: bfloat16 [4, 4096, 4096], P('opt', 'seq'), may hold values from -0.59765625 to 0.59765625
- log_decay: float32 [4, 32, 4096], P('opt', None, 'seq'), may hold values from -1 to 0, as said below
- skip_gain: float32 [32], replicated, may hold values from 0.5 to 2
- w_bc: float32 [4096, 256], P(('seq', 'opt')), may hold values from -0.0078125 to 0.0078125
- m_code: bfloat16 [4096, 256], P(('seq', 'opt')), may hold values from -1 to 1
- m_scale: float32 [256], replicated, may hold values from 0.0001 to 0.001
- row_stat: float32 [4096], P(('seq', 'opt')), may hold values from 3e-07 to 3e-06
- col_stat: float32 [256], replicated, may hold values from 3e-07 to 3e-06
Outputs:
- grad_input: bfloat16 [4, 4096, 4096], P('opt', 'seq')
- update: float32 [4096, 256], P(('seq', 'opt'))
- code_next: bfloat16 [4096, 256], P(('seq', 'opt'))
- scale_next: float32 [256], replicated
- row_next: float32 [4096], P(('seq', 'opt'))
- col_next: float32 [256], replicated
The draws below stay inside these ranges and needn't reach their ends.
Inputs may be any that keep to these rules, and one draw needn't show every extreme that they name: `layer_in`: real-valued rows of order one. `log_decay`: negative log decays.
All inputs are finite; a program needn't handle non-finite values.
Results may differ from the reference program's by a relative error of at most 0.0095.
Values may be sent and summed in bfloat16 or wider, within the bound.
A program may use at most 256 MiB of HBM per device.

```python
import math
import jax
import jax.numpy as jnp
from jax import lax

D = 4096
N = 128
P_SIZE = 128
H = 32
BLOCK = 256
TOK_DEV = 512
TOKEN_POSITIONS = 4096
SEQUENCE_COUNT = 4


def draw_layer_in(key, part):
    lookup_keys = jax.random.split(key, 2)
    position = jnp.arange(D, dtype=jnp.float32) / (D - 1)
    feature_scale = jnp.exp(math.log(3.0) * position + math.log(10.0) * jax.random.uniform(lookup_keys[0], (D,), jnp.float32)) / 4.0
    base = jnp.clip(jax.random.normal(lookup_keys[1], (SEQUENCE_COUNT, TOKEN_POSITIONS, D), jnp.float32), -6.0, 6.0)
    return (base * feature_scale[None, None, :]).astype(jnp.bfloat16)


def draw_log_decay(key, part):
    lookup_keys = jax.random.split(key, 7)
    share = 0.5
    fast_head = jax.random.uniform(lookup_keys[0], (SEQUENCE_COUNT, H, 1), jnp.float32) < share
    fast_rate = jax.random.uniform(lookup_keys[1], (SEQUENCE_COUNT, H, 1), jnp.float32, 1.0 / 50.0, 1.0 / 30.0)
    slow_rate = jax.random.uniform(lookup_keys[2], (SEQUENCE_COUNT, H, 1), jnp.float32, 0.2, 0.6) / TOKEN_POSITIONS
    rate = jnp.where(fast_head, fast_rate, slow_rate)
    rough = jnp.exp(jax.random.uniform(lookup_keys[3], (SEQUENCE_COUNT, H, TOKEN_POSITIONS), jnp.float32, -0.7, 0.7))
    blocks = TOKEN_POSITIONS // TOK_DEV
    device_factor = jnp.exp(jax.random.uniform(lookup_keys[4], (SEQUENCE_COUNT, H, blocks, 1), jnp.float32, -0.7, 0.7))
    device_factor = jnp.broadcast_to(device_factor, (SEQUENCE_COUNT, H, blocks, TOK_DEV)).reshape(SEQUENCE_COUNT, H, TOKEN_POSITIONS)
    first_spot = jax.random.randint(lookup_keys[5], (SEQUENCE_COUNT, 1, 1, 1), 0, TOKEN_POSITIONS)
    spot_offset = jax.random.randint(jax.random.fold_in(lookup_keys[5], 1), (SEQUENCE_COUNT, 1, 1, 1), 1, TOKEN_POSITIONS)
    second_spot = (first_spot + spot_offset) % TOKEN_POSITIONS
    flurry_position = jnp.concatenate([first_spot, second_spot], axis=-1).astype(jnp.int32)
    flurry_depth = jax.random.uniform(lookup_keys[6], (SEQUENCE_COUNT, 1, 1, 2), jnp.float32, 0.22, 0.69)
    target_spots = jnp.arange(TOKEN_POSITIONS, dtype=jnp.int32)[None, None, :, None]
    match_count = jnp.sum(jnp.where(target_spots == flurry_position, flurry_depth, 0.0), axis=-1)
    return -(rate * rough * device_factor) - match_count


def steps_of(stream_key, shape, pieces, smallest, top_value):
    level, own = 1.0, jax.random.fold_in(stream_key, 6)
    for dim, parts in pieces:
        draws = jnp.exp(jax.random.uniform(jax.random.fold_in(own, dim), (parts,), jnp.float32, smallest / len(pieces), top_value / len(pieces)))
        level = level * jnp.repeat(draws, shape[dim] // parts).reshape([-1 if axis == dim else 1 for axis in range(len(shape))])
    return level


def centred(rng, dims, scale, limit, shards=(), kind=jnp.bfloat16):
    drawn = jax.random.normal(rng, dims, jnp.float32) * scale
    if len(shards) > 0:
        drawn = steps_of(rng, dims, shards, -0.22, 0.18) * drawn
    return jnp.clip(drawn, min=-limit, max=limit).astype(kind)


def setup_inputs(seed: int = 0) -> dict:
    key_of = jax.random.split(jax.random.key(seed), 11)
    layer_in = draw_layer_in(jax.random.fold_in(key_of[10], 71), 0)
    ssm_input = centred(key_of[1], (SEQUENCE_COUNT, TOKEN_POSITIONS, H * P_SIZE), 0.02, 0.119628906, ((0, 4), (1, 8)))
    grad_out = centred(key_of[2], (SEQUENCE_COUNT, TOKEN_POSITIONS, H * P_SIZE), 0.1, 0.59765625, ((0, 4), (1, 8)))
    log_decay = draw_log_decay(jax.random.fold_in(key_of[10], 71), 0)
    skip_gain = jnp.clip(jax.random.uniform(key_of[4], (H,), jnp.float32, 0.5, 2.0), 0.5, 2.0)
    w_bc = centred(key_of[5], (D, 2 * N), (D * N) ** -0.5, 0.0078125, ((0, 32),), jnp.float32)
    m_code = jnp.clip(jax.random.uniform(key_of[6], (D, 2 * N), jnp.float32, -1.0, 1.0) * steps_of(key_of[6], (D, 2 * N), ((0, 32),), -0.4, 0.0), -1.0, 1.0).astype(jnp.bfloat16)
    m_scale = jnp.clip(jnp.exp(jax.random.uniform(key_of[7], (2 * N,), jnp.float32, math.log(0.0001), math.log(0.001))), 0.0001, 0.001)
    row_stat = jnp.clip(jnp.exp(math.log(3.000000106112566e-06) - 2.3025851 * jax.random.uniform(key_of[8], (D,), jnp.float32) ** steps_of(key_of[8], (D,), ((0, 32),), -0.2, 0.2)), 3.000000106112566e-07, 3.000000106112566e-06)
    col_stat = jnp.clip(jnp.exp(jax.random.uniform(key_of[9], (2 * N,), jnp.float32, math.log(3.000000106112566e-07), math.log(3.000000106112566e-06))), 3.000000106112566e-07, 3.000000106112566e-06)
    return {"layer_in": layer_in, "ssm_input": ssm_input, "grad_out": grad_out, "log_decay": log_decay, "skip_gain": skip_gain, "w_bc": w_bc, "m_code": m_code, "m_scale": m_scale, "row_stat": row_stat, "col_stat": col_stat}


beta_one = 0.9
beta_two = 0.95
weight_decay = 0.1
clip_norm = 1.0
tiny_square = 1e-30
adam_floor = 1e-08
peak_floor = 1e-06
norm_floor = 1e-06
highest = lax.Precision.HIGHEST

def lower_decays(running):
    length = running.shape[1]
    row_pos = lax.broadcasted_iota(jnp.int32, (length, length), 0)
    col_pos = lax.broadcasted_iota(jnp.int32, (length, length), 1)
    spread = running[:, :, None] - running[:, None, :]
    return jnp.exp(jnp.where((row_pos >= col_pos)[None], spread, -jnp.inf))

def state_adds(feat_blk, cot_blk, b_rows, c_rows, running):
    closing = running[:, -1]
    shrink = jnp.exp(closing[:, None] - running)
    grow = jnp.exp(running)
    forward_add = jnp.einsum('htn,thp->hnp', shrink[:, :, None] * b_rows[None], feat_blk, precision=highest)
    backward_add = jnp.einsum('htn,thp->hnp', grow[:, :, None] * c_rows[None], cot_blk, precision=highest)
    return (forward_add, backward_add)

def block_terms(feat_blk, cot_blk, b_rows, c_rows, running, state_in, grad_in, skip_gain):
    closing = running[:, -1]
    decays = lower_decays(running)
    grow = jnp.exp(running)
    shrink = jnp.exp(closing[:, None] - running)
    intersection = jnp.einsum('thp,shp->hts', feat_blk, cot_blk, precision=highest)
    affinity = jnp.dot(b_rows, c_rows.T, precision=highest)
    mixing = lax.optimization_barrier(jnp.sum(decays * jnp.transpose(intersection, (0, 2, 1)), axis=0))
    left_in = jnp.einsum('hnp,thp->htn', state_in, cot_blk, precision=highest)
    grad_cmat = jnp.dot(mixing, b_rows, precision=highest) + lax.optimization_barrier(jnp.sum(grow[:, :, None] * left_in, axis=0))
    right_in = jnp.einsum('hnp,thp->htn', grad_in, feat_blk, precision=highest)
    grad_bmat = jnp.dot(mixing.T, c_rows, precision=highest) + lax.optimization_barrier(jnp.sum(shrink[:, :, None] * right_in, axis=0))
    weighted = jnp.transpose(decays, (0, 2, 1)) * affinity[None]
    inner = jnp.einsum('hts,shp->thp', weighted, cot_blk, precision=highest)
    outer = jnp.einsum('tn,hnp->thp', b_rows, grad_in, precision=highest) * shrink.T[:, :, None]
    grad_feat = inner + outer + skip_gain[None, :, None] * cot_blk
    return (grad_feat, jnp.concatenate([grad_bmat, grad_cmat], axis=1))

def one_sequence(layer_rows, feat_rows, cot_rows, log_rows, w_half, skip_gain):
    proj = jnp.dot(layer_rows, w_half, preferred_element_type=jnp.float32).astype(jnp.bfloat16)
    count = TOKEN_POSITIONS // BLOCK
    b_all = proj[:, :N].astype(jnp.float32).reshape(count, BLOCK, N)
    c_all = proj[:, N:].astype(jnp.float32).reshape(count, BLOCK, N)
    feats = feat_rows.astype(jnp.float32).reshape(count, BLOCK, H, P_SIZE)
    cots = cot_rows.astype(jnp.float32).reshape(count, BLOCK, H, P_SIZE)
    logs = jnp.transpose(log_rows.reshape(H, count, BLOCK), (1, 0, 2))

    def forward(state, items):
        feat_blk, cot_blk, b_rows, c_rows, log_blk = items
        running = jnp.cumsum(log_blk, axis=1)
        forward_add, unused = state_adds(feat_blk, cot_blk, b_rows, c_rows, running)
        return (jnp.exp(running[:, -1])[:, None, None] * state + forward_add, state)
    start = jnp.zeros((H, N, P_SIZE), jnp.float32)
    unused_last, states_in = lax.scan(forward, start, (feats, cots, b_all, c_all, logs))

    def backward(grad_in, items):
        feat_blk, cot_blk, b_rows, c_rows, log_blk, state_in = items
        running = jnp.cumsum(log_blk, axis=1)
        grad_feat, grad_bc = block_terms(feat_blk, cot_blk, b_rows, c_rows, running, state_in, grad_in, skip_gain)
        unused, backward_add = state_adds(feat_blk, cot_blk, b_rows, c_rows, running)
        return (jnp.exp(running[:, -1])[:, None, None] * grad_in + backward_add, (grad_feat, grad_bc))
    unused_first, outputs = lax.scan(backward, start, (feats, cots, b_all, c_all, logs, states_in), reverse=True)
    grad_feats, grad_bcs = outputs
    grad_bc = grad_bcs.reshape(TOKEN_POSITIONS, 2 * N).astype(jnp.bfloat16)
    weight_grad = jnp.dot(layer_rows.T, grad_bc, preferred_element_type=jnp.float32)
    return (grad_feats.reshape(TOKEN_POSITIONS, H * P_SIZE).astype(jnp.bfloat16), weight_grad)

def reference(layer_in, ssm_input, grad_out, log_decay, skip_gain, w_bc, m_code, m_scale, row_stat, col_stat):
    w_half = w_bc.astype(jnp.bfloat16)
    results = []
    grad_sum = jnp.zeros((D, 2 * N), jnp.float32)
    for seq_id in range(SEQUENCE_COUNT):
        grad_feat, weight_grad = one_sequence(layer_in[seq_id], ssm_input[seq_id], grad_out[seq_id], log_decay[seq_id], w_half, skip_gain)
        results.append(grad_feat)
        grad_sum = grad_sum + weight_grad
    grad_input = jnp.stack(results)
    norm_sq = jnp.sum(grad_sum * grad_sum) + norm_floor
    factor = jnp.minimum(1.0, clip_norm / jnp.sqrt(norm_sq))
    scaled = grad_sum * factor
    squares = scaled * scaled
    moment = beta_one * m_code.astype(jnp.float32) * m_scale[None, :] + (1.0 - beta_one) * scaled
    row_next = beta_two * row_stat + (1.0 - beta_two) * (lax.optimization_barrier(jnp.mean(squares, axis=1)) + tiny_square)
    col_next = beta_two * col_stat + (1.0 - beta_two) * (lax.optimization_barrier(jnp.mean(squares, axis=0)) + tiny_square)
    second = row_next[:, None] * col_next[None, :] / jnp.mean(row_next)
    update = moment / (jnp.sqrt(second) + adam_floor) + weight_decay * w_bc
    scale_next = lax.optimization_barrier(jnp.max(jnp.abs(moment), axis=0)) + peak_floor
    code_next = (moment / scale_next[None, :]).astype(jnp.bfloat16)
    return (grad_input, update, code_next, scale_next, row_next, col_next)
```

```python
import functools

import jax
import jax.numpy as jnp
from jax import lax
from jax.experimental import pallas as pl
from jax.experimental.pallas import tpu as pltpu
from jax.sharding import PartitionSpec as P

BLOCK = 256
LANES = 128
LAG_SWAP = 3
LAG_CHAIN = 2

beta_one = 0.9
beta_two = 0.95
weight_decay = 0.1
clip_norm = 1.0
tiny_square = 1e-30
adam_floor = 1e-08
peak_floor = 1e-06
norm_floor = 1e-06
highest = lax.Precision.HIGHEST
MESH = pl.DeviceIdType.MESH
VMEM_LIMIT = 60 * 1024 * 1024
f32 = jnp.float32
bf16 = jnp.bfloat16


def dot_nn(a, b):
    return lax.dot_general(a, b, (((1,), (0,)), ((), ())), preferred_element_type=f32)


def dot_nt(a, b):
    return lax.dot_general(a, b, (((1,), (1,)), ((), ())), preferred_element_type=f32)


def dot_tn(a, b):
    return lax.dot_general(a, b, (((0,), (0,)), ((), ())), preferred_element_type=f32)


def as_column(row):
    return jnp.transpose(jnp.broadcast_to(row, (LANES, row.shape[1])))


def widened(column, length):
    return jnp.concatenate([column] * (length // LANES), axis=1)


def mixing_kernel(
    count, n_seq, n_opt, w_ref, x_ref, dy_ref, run_ref, mix_ref, w_out,
    got, send_a, recv_a, send_b, recv_b,
):
    seq = lax.axis_index("seq")
    opt = lax.axis_index("opt")
    h = pl.program_id(0)
    last = pl.num_programs(0) - 1

    def over_seq():
        return swap_all(
            n_seq, seq, lambda s: w_ref, lambda s: got.at[opt, s],
            lambda s: (s, opt), send_a, recv_a,
        )

    def over_opt():
        return swap_all(
            n_opt, opt, lambda o: got.at[opt], lambda o: got.at[o],
            lambda o: (seq, o), send_b, recv_b,
        )

    @pl.when(h == 0)
    def _():
        greet(n_seq * n_opt, seq * n_opt + opt, lambda i: (i // n_opt, lax.rem(i, n_opt)))
        over_seq()[0]()
        got[opt, seq] = w_ref[...]
        mix_ref[...] = jnp.zeros_like(mix_ref)

    @pl.when(h == last // 2)
    def _():
        over_seq()[1]()
        over_opt()[0]()

    row_pos = lax.broadcasted_iota(jnp.int32, (BLOCK, BLOCK), 0)
    col_pos = lax.broadcasted_iota(jnp.int32, (BLOCK, BLOCK), 1)
    for b in range(count):
        rows = slice(b * BLOCK, (b + 1) * BLOCK)
        row = run_ref[0, b : b + 1, :]
        spread = widened(as_column(row), BLOCK) - row
        decays = jnp.exp(jnp.where(row_pos >= col_pos, spread, -jnp.inf))
        mix_ref[b] += decays * dot_nt(dy_ref[rows, :], x_ref[rows, :])

    @pl.when(h == last)
    def _():
        over_opt()[1]()

        def place(s, carry):
            for o in range(n_opt):
                w_out[s, o] = got[o, s]
            return carry

        lax.fori_loop(0, n_seq, place, 0)


def remote(src, dst, send_sem, recv_sem, device):
    return pltpu.make_async_remote_copy(
        src_ref=src, dst_ref=dst, send_sem=send_sem, recv_sem=recv_sem,
        device_id=device, device_id_type=MESH,
    )


def states_kernel(
    count, heads, n_pairs, skip_ref, x_ref, dy_ref, x_far, dy_far, b_ref, c_ref, run_ref, mix_ref,
    gx_ref, gbc_ref,
    b_turned, c_turned, affinity, acc_b, acc_c, starts, outs, mine, got, chain_in, chain_out,
    decay, decay_far, send_d, recv_d, send_y, recv_y, send_c, recv_c,
):
    i = pl.program_id(0)
    seq = lax.axis_index("seq")
    opt = lax.axis_index("opt")
    pair = seq // 2
    side = lax.rem(seq, 2)
    lag = LAG_SWAP + LAG_CHAIN * (n_pairs - 1)
    state_dim = b_ref.shape[1]
    twin = (seq + 1 - 2 * side, opt)
    ahead = (seq + 2, opt)
    behind = (seq - 2, opt)

    def closings_of(h):
        return [run_ref[h, b : b + 1, BLOCK - 1 : BLOCK] for b in range(count)]

    def swap(h):
        return remote(mine.at[h], got.at[h], send_y.at[h], recv_y.at[h], twin)

    def swap_decay():
        return remote(decay, decay_far, send_d, recv_d, twin)

    def pass_on(way, h):
        return remote(
            chain_out.at[way, h], chain_in.at[way, h], send_c.at[way, h], recv_c.at[way, h],
            (ahead, behind)[way],
        )

    has_source = (pair > 0, pair < n_pairs - 1)
    has_target = (pair < n_pairs - 1, pair > 0)

    @pl.when(i == 0)
    def _():
        barrier = pltpu.get_barrier_semaphore()
        pl.semaphore_signal(barrier, inc=1, device_id=twin, device_id_type=MESH)
        for way in range(2):
            @pl.when(has_target[way])
            def _():
                pl.semaphore_signal(
                    barrier, inc=1, device_id=(ahead, behind)[way], device_id_type=MESH
                )

        def decay_of(h, carry):
            total = sum(closings_of(h), jnp.zeros((1, 1), f32))
            decay[h] = jnp.broadcast_to(jnp.exp(total), (1, LANES))
            return carry

        lax.fori_loop(0, heads, decay_of, 0)
        acc_b[...] = jnp.zeros_like(acc_b)
        acc_c[...] = jnp.zeros_like(acc_c)
        b_turned[...] = jnp.transpose(b_ref[...].astype(f32))
        c_turned[...] = jnp.transpose(c_ref[...].astype(f32))
        for b in range(count):
            rows = slice(b * BLOCK, (b + 1) * BLOCK)
            affinity[b] = dot_nt(b_ref[rows, :], c_ref[rows, :])
        for way in range(2):
            @pl.when(jnp.logical_not(has_source[way]))
            def _():
                chain_in[way] = jnp.zeros_like(chain_in[way])
        neighbours = 1 + (pair > 0).astype(jnp.int32) + (pair < n_pairs - 1).astype(jnp.int32)
        pl.semaphore_wait(barrier, neighbours)
        swap_decay().start()

    @pl.when(i < heads)
    def _():
        h = i
        adds = []
        for b in range(count):
            rows = slice(b * BLOCK, (b + 1) * BLOCK)
            row = run_ref[h, b : b + 1, :]
            closing = row[:, BLOCK - 1 : BLOCK]
            b_scaled = (b_turned[:, rows] * jnp.exp(closing - row)).astype(bf16)
            c_scaled = (c_turned[:, rows] * jnp.exp(row)).astype(bf16)
            adds.append(
                (jnp.exp(closing), dot_nn(b_scaled, x_ref[rows, :]), dot_nn(c_scaled, dy_ref[rows, :]))
            )
        state = adds[0][1]
        for b in range(1, count):
            starts[h, b - 1] = state.astype(bf16)
            state = adds[b][0] * state + adds[b][1]
        mine[h, 0] = state.astype(bf16)
        carried = adds[count - 1][2]
        for b in reversed(range(count - 1)):
            outs[h, b] = carried.astype(bf16)
            carried = adds[b][0] * carried + adds[b][2]
        mine[h, 1] = carried.astype(bf16)
        swap(h).start()

    @pl.when(i == LAG_SWAP)
    def _():
        swap_decay().wait_recv()

    j = i - LAG_SWAP

    @pl.when(jnp.logical_and(j >= 0, j < heads))
    def _():
        swap(j).wait_recv()

    for way in range(2):
        place = pair if way == 0 else n_pairs - 1 - pair
        hop = j - LAG_CHAIN * place

        @pl.when(jnp.logical_and(hop >= 0, hop < heads))
        def _():
            @pl.when(has_source[way])
            def _():
                pass_on(way, hop).wait_recv()

            @pl.when(has_target[way])
            def _():
                own_decay = decay[hop]
                other_decay = decay_far[hop]
                first = side == way
                own_scale = jnp.where(first, other_decay, 1.0)
                other_scale = jnp.where(first, 1.0, own_decay)
                total = (
                    own_decay * other_decay * chain_in[way, hop].astype(f32)
                    + own_scale * mine[hop, way].astype(f32)
                    + other_scale * got[hop, way].astype(f32)
                )
                chain_out[way, hop] = total.astype(bf16)
                pass_on(way, hop).start()

    @pl.when(i >= lag)
    def _():
        h = i - lag
        row_pos = lax.broadcasted_iota(jnp.int32, (BLOCK, BLOCK), 0)
        col_pos = lax.broadcasted_iota(jnp.int32, (BLOCK, BLOCK), 1)
        closings = closings_of(h)
        other_decay = decay_far[h]
        fars = []
        for way in range(2):
            second = side != way
            scale = jnp.where(second, other_decay, 1.0)
            extra = jnp.where(second, jnp.ones((1, LANES), f32), 0.0)
            fars.append(scale * chain_in[way, h].astype(f32) + extra * got[h, way].astype(f32))
        far_state, far_grad = fars
        for b in range(count):
            rows = slice(b * BLOCK, (b + 1) * BLOCK)
            row = run_ref[h, b : b + 1, :]
            column = as_column(row)
            before = sum(closings[:b], jnp.zeros((1, 1), f32))
            after = sum(closings[b + 1 :], jnp.zeros((1, 1), f32))
            if b == 0:
                state_in = far_state.astype(bf16)
            else:
                state_in = (starts[h, b - 1].astype(f32) + jnp.exp(before) * far_state).astype(bf16)
            if b == count - 1:
                grad_in = far_grad.astype(bf16)
            else:
                grad_in = (outs[h, b].astype(f32) + jnp.exp(after) * far_grad).astype(bf16)
            grow = jnp.exp(column)
            shrink = jnp.exp(closings[b] - column)
            x_blk = x_far[rows, :]
            dy_blk = dy_far[rows, :]
            spread = row - widened(column, BLOCK)
            decays = jnp.exp(jnp.where(col_pos >= row_pos, spread, -jnp.inf))
            weighted = (decays * affinity[b]).astype(bf16)
            inner = dot_nn(weighted, dy_blk)
            outer = dot_nn(b_ref[rows, :], grad_in) * shrink
            gx_ref[rows, :] = (inner + outer + skip_ref[h] * dy_blk.astype(f32)).astype(bf16)
            acc_c[rows, :] += grow * dot_nt(dy_blk, state_in)
            acc_b[rows, :] += shrink * dot_nt(x_blk, grad_in)

    @pl.when(i == pl.num_programs(0) - 1)
    def _():
        for b in range(count):
            rows = slice(b * BLOCK, (b + 1) * BLOCK)
            mixing = mix_ref[b].astype(bf16)
            gbc_ref[rows, :state_dim] = (acc_b[rows, :] + dot_tn(mixing, c_ref[rows, :])).astype(bf16)
            gbc_ref[rows, state_dim:] = (acc_c[rows, :] + dot_nn(mixing, b_ref[rows, :])).astype(bf16)
        swap_decay().wait_send()

        def sent(h, carry):
            swap(h).wait_send()
            for way in range(2):
                @pl.when(has_target[way])
                def _():
                    pass_on(way, h).wait_send()
            return carry

        lax.fori_loop(0, heads, sent, 0)


def swap_all(n, me, src_of, dst_of, device_of, send_sem, recv_sem):
    def copy_to(distance):
        other = lax.rem(me + distance, n)
        return pltpu.make_async_remote_copy(
            src_ref=src_of(other), dst_ref=dst_of(me), send_sem=send_sem.at[other],
            recv_sem=recv_sem.at[me], device_id=device_of(other), device_id_type=MESH,
        )

    def copy_from(distance):
        other = lax.rem(me + distance, n)
        return pltpu.make_async_remote_copy(
            src_ref=src_of(other), dst_ref=dst_of(other), send_sem=send_sem.at[other],
            recv_sem=recv_sem.at[other], device_id=device_of(other), device_id_type=MESH,
        )

    def start(distance, carry):
        copy_to(distance).start()
        return carry

    def finish(distance, carry):
        copy = copy_from(distance)
        copy.wait_send()
        copy.wait_recv()
        return carry

    return lambda: lax.fori_loop(1, n, start, 0), lambda: lax.fori_loop(1, n, finish, 0)


def begin_swap(*args):
    start, finish = swap_all(*args)
    start()
    return finish


def greet(n, me, device_of):
    barrier = pltpu.get_barrier_semaphore()

    def signal(distance, carry):
        other = lax.rem(me + distance, n)
        pl.semaphore_signal(barrier, inc=1, device_id=device_of(other), device_id_type=MESH)
        return carry

    lax.fori_loop(1, n, signal, 0)
    pl.semaphore_wait(barrier, n - 1)


def step_kernel(
    n_seq, n_opt, part_ref, w_ref, code_ref, scale_ref, row_ref, col_ref,
    update_ref, code_out, scale_out, row_out, col_out,
    got_a, mid, got_b, stats, all_stats, peak, all_peaks,
    send_a, recv_a, send_b, recv_b, send_c, recv_c, send_d, recv_d,
):
    seq = lax.axis_index("seq")
    opt = lax.axis_index("opt")
    n = n_seq * n_opt
    me = seq * n_opt + opt

    def any_device(i):
        return (i // n_opt, lax.rem(i, n_opt))

    greet(n, me, any_device)
    begin_swap(
        n_opt, opt, lambda o: part_ref.at[o], lambda o: got_a.at[o],
        lambda o: (seq, o), send_a, recv_a,
    )()
    got_a[opt] = part_ref[opt]

    def fold(s, carry):
        total = got_a[0, s].astype(f32)
        for o in range(1, n_opt):
            total += got_a[o, s].astype(f32)
        mid[s] = total.astype(bf16)
        return carry

    lax.fori_loop(0, n_seq, fold, 0)
    begin_swap(
        n_seq, seq, lambda s: mid.at[s], lambda s: got_b.at[s],
        lambda s: (s, opt), send_b, recv_b,
    )()
    got_b[seq] = mid[seq]
    grad = got_b[0].astype(f32)
    for s in range(1, n_seq):
        grad += got_b[s].astype(f32)

    rows, cols = grad.shape
    width = n * rows
    squares_raw = grad * grad
    stats[:, :cols] = jnp.sum(squares_raw, axis=0, keepdims=True)
    row_stat = row_ref[...]
    stats[:, cols:] = jnp.broadcast_to(jnp.sum(row_stat, axis=0, keepdims=True), (1, LANES))
    begin_swap(
        n, me, lambda i: stats, lambda i: all_stats.at[i], any_device, send_c, recv_c
    )()
    all_stats[me] = stats[...]
    sums = all_stats[0]
    for i in range(1, n):
        sums += all_stats[i]
    col_raw = sums[:, :cols]
    old_total = sums[:, cols : cols + 1]
    raw_total = jnp.sum(col_raw, axis=1, keepdims=True)
    factor = jnp.minimum(1.0, clip_norm / jnp.sqrt(raw_total + norm_floor))
    scaled = grad * factor
    moment = beta_one * code_ref[...].astype(f32) * scale_ref[...] + (1.0 - beta_one) * scaled
    peak[...] = jnp.max(jnp.abs(moment), axis=0, keepdims=True)
    end_peaks = begin_swap(
        n, me, lambda i: peak, lambda i: all_peaks.at[i], any_device, send_d, recv_d
    )
    col_next = beta_two * col_ref[...] + (1.0 - beta_two) * (
        factor * factor * col_raw / width + tiny_square
    )
    row_next = beta_two * row_stat + (1.0 - beta_two) * (
        jnp.sum(scaled * scaled, axis=1, keepdims=True) / cols + tiny_square
    )
    row_mean = (
        beta_two * old_total
        + (1.0 - beta_two) * (factor * factor * raw_total / cols + width * tiny_square)
    ) / width
    second = row_next * col_next / row_mean
    update_ref[...] = moment / (jnp.sqrt(second) + adam_floor) + weight_decay * w_ref[...]
    row_out[...] = row_next
    col_out[...] = col_next
    end_peaks()
    all_peaks[me] = peak[...]
    scale_next = all_peaks[0]
    for i in range(1, n):
        scale_next = jnp.maximum(scale_next, all_peaks[i])
    scale_next = scale_next + peak_floor
    scale_out[...] = scale_next
    code_out[...] = (moment / scale_next).astype(bf16)


def params(**more):
    return pltpu.CompilerParams(vmem_limit_bytes=VMEM_LIMIT, **more)


def whole():
    return pl.BlockSpec(memory_space=pltpu.VMEM)


def dma(*counts):
    return [pltpu.SemaphoreType.DMA((count,)) for count in counts for _ in range(2)]


def per_device(
    n_seq, n_opt, layer_in, ssm_input, grad_out, log_decay, skip_gain, w_bc, m_code, m_scale,
    row_stat, col_stat,
):
    layer_rows = layer_in[0]
    x = ssm_input[0]
    dy = grad_out[0]
    length, width = layer_rows.shape
    heads = skip_gain.shape[0]
    head_dim = x.shape[1] // heads
    state_dim = w_bc.shape[1] // 2
    count = length // BLOCK
    n_pairs = n_seq // 2
    own_rows = w_bc.shape[0]

    ones = (
        lax.broadcasted_iota(jnp.int32, (BLOCK, BLOCK), 0)
        <= lax.broadcasted_iota(jnp.int32, (BLOCK, BLOCK), 1)
    ).astype(f32)
    running = jnp.dot(
        log_decay[0].reshape(heads * count, BLOCK), ones, precision=highest
    ).reshape(heads, count, BLOCK)
    tokens = pl.BlockSpec((length, head_dim), lambda h: (0, h))
    run_spec = pl.BlockSpec((1, count, BLOCK), lambda h: (h, 0, 0))
    mix_spec = pl.BlockSpec((count, BLOCK, BLOCK), lambda h: (0, 0, 0))
    b_spec = pl.BlockSpec((length, state_dim), lambda h: (0, 0))
    c_spec = pl.BlockSpec((length, state_dim), lambda h: (0, 1))

    w_shape = (own_rows, 2 * state_dim)
    mixing, w_all = pl.pallas_call(
        functools.partial(mixing_kernel, count, n_seq, n_opt),
        grid=(heads,),
        in_specs=[whole(), tokens, tokens, run_spec],
        out_specs=[mix_spec, whole()],
        out_shape=[
            jax.ShapeDtypeStruct((count, BLOCK, BLOCK), f32),
            jax.ShapeDtypeStruct((n_seq, n_opt) + w_shape, bf16),
        ],
        scratch_shapes=[pltpu.VMEM((n_opt, n_seq) + w_shape, bf16)] + dma(n_seq, n_opt),
        compiler_params=params(collective_id=2, has_side_effects=True),
        name="gather_and_mixing",
    )(w_bc.astype(bf16), x, dy, running)
    w_all = w_all.reshape(width, 2 * state_dim)

    proj = jnp.dot(layer_rows, w_all, preferred_element_type=f32).astype(bf16)

    lag = LAG_SWAP + LAG_CHAIN * (n_pairs - 1)
    near = pl.BlockSpec((length, head_dim), lambda i: (0, jnp.minimum(i, heads - 1)))
    late = pl.BlockSpec((length, head_dim), lambda i: (0, jnp.maximum(i - lag, 0)))
    all_run = pl.BlockSpec((heads, count, BLOCK), lambda i: (0, 0, 0))
    per_head = (heads, 2, state_dim, head_dim)
    per_way = (2, heads, state_dim, head_dim)
    grad_input, grad_bc = pl.pallas_call(
        functools.partial(states_kernel, count, heads, n_pairs),
        grid=(heads + lag,),
        in_specs=[
            pl.BlockSpec(memory_space=pltpu.SMEM), near, near, late, late, b_spec, c_spec, all_run,
            mix_spec,
        ],
        out_specs=[late, pl.BlockSpec((length, 2 * state_dim), lambda h: (0, 0))],
        out_shape=[
            jax.ShapeDtypeStruct(x.shape, bf16),
            jax.ShapeDtypeStruct((length, 2 * state_dim), bf16),
        ],
        scratch_shapes=[
            pltpu.VMEM((state_dim, length), f32),
            pltpu.VMEM((state_dim, length), f32),
            pltpu.VMEM((count, BLOCK, BLOCK), f32),
            pltpu.VMEM((length, state_dim), f32),
            pltpu.VMEM((length, state_dim), f32),
            pltpu.VMEM((heads, max(count - 1, 1), state_dim, head_dim), bf16),
            pltpu.VMEM((heads, max(count - 1, 1), state_dim, head_dim), bf16),
            pltpu.VMEM(per_head, bf16),
            pltpu.VMEM(per_head, bf16),
            pltpu.VMEM(per_way, bf16),
            pltpu.VMEM(per_way, bf16),
            pltpu.VMEM((heads, 1, LANES), f32),
            pltpu.VMEM((heads, 1, LANES), f32),
            pltpu.SemaphoreType.DMA,
            pltpu.SemaphoreType.DMA,
            pltpu.SemaphoreType.DMA((heads,)),
            pltpu.SemaphoreType.DMA((heads,)),
            pltpu.SemaphoreType.DMA((2, heads)),
            pltpu.SemaphoreType.DMA((2, heads)),
        ],
        compiler_params=params(collective_id=0, has_side_effects=True),
        name="states_and_grads",
    )(skip_gain, x, dy, x, dy, proj, proj, running, mixing)

    cols = 2 * state_dim
    part = lax.dot_general(
        layer_rows, grad_bc, (((0,), (0,)), ((), ())), preferred_element_type=f32
    ).astype(bf16)
    part = jnp.transpose(part.reshape(n_seq, n_opt, own_rows, cols), (1, 0, 2, 3))

    n = n_seq * n_opt
    update, code_next, scale_next, row_next, col_next = pl.pallas_call(
        functools.partial(step_kernel, n_seq, n_opt),
        in_specs=[whole()] * 6,
        out_specs=[whole()] * 5,
        out_shape=[
            jax.ShapeDtypeStruct((own_rows, cols), f32),
            jax.ShapeDtypeStruct((own_rows, cols), bf16),
            jax.ShapeDtypeStruct((1, cols), f32),
            jax.ShapeDtypeStruct((own_rows, 1), f32),
            jax.ShapeDtypeStruct((1, cols), f32),
        ],
        scratch_shapes=[
            pltpu.VMEM((n_opt, n_seq, own_rows, cols), bf16),
            pltpu.VMEM((n_seq, own_rows, cols), bf16),
            pltpu.VMEM((n_seq, own_rows, cols), bf16),
            pltpu.VMEM((1, cols + LANES), f32),
            pltpu.VMEM((n, 1, cols + LANES), f32),
            pltpu.VMEM((1, cols), f32),
            pltpu.VMEM((n, 1, cols), f32),
        ]
        + dma(n_opt, n_seq, n, n),
        compiler_params=params(collective_id=1, has_side_effects=True),
        name="sum_and_step",
    )(part, w_bc, m_code, m_scale[None, :], row_stat[:, None], col_stat[None, :])
    return (grad_input[None], update, code_next, scale_next[0], row_next[:, 0], col_next[0])


def solution(mesh):
    return jax.shard_map(
        functools.partial(per_device, mesh.shape["seq"], mesh.shape["opt"]),
        mesh=mesh,
        in_specs=(
            P("opt", "seq", None),
            P("opt", "seq", None),
            P("opt", "seq", None),
            P("opt", None, "seq"),
            P(),
            P(("seq", "opt"), None),
            P(("seq", "opt"), None),
            P(),
            P(("seq", "opt")),
            P(),
        ),
        out_specs=(
            P("opt", "seq", None),
            P(("seq", "opt"), None),
            P(("seq", "opt"), None),
            P(),
            P(("seq", "opt")),
            P(),
        ),
        check_vma=False,
    )
```

```python
import functools

import jax
import jax.numpy as jnp
from jax import lax
from jax.experimental import pallas as pl
from jax.experimental.pallas import tpu as pltpu
from jax.sharding import PartitionSpec as P

BLOCK = 256
LANES = 128
LAG_SWAP = 3
LAG_CHAIN = 2
STEP_B = 20
STEP_C = 30

beta_one = 0.9
beta_two = 0.95
weight_decay = 0.1
clip_norm = 1.0
tiny_square = 1e-30
adam_floor = 1e-08
peak_floor = 1e-06
norm_floor = 1e-06
highest = lax.Precision.HIGHEST
MESH = pl.DeviceIdType.MESH
VMEM_LIMIT = 60 * 1024 * 1024
f32 = jnp.float32
bf16 = jnp.bfloat16


def dot_nn(a, b):
    return lax.dot_general(a, b, (((1,), (0,)), ((), ())), preferred_element_type=f32)


def dot_nt(a, b):
    return lax.dot_general(a, b, (((1,), (1,)), ((), ())), preferred_element_type=f32)


def dot_tn(a, b):
    return lax.dot_general(a, b, (((0,), (0,)), ((), ())), preferred_element_type=f32)


def as_column(row):
    return jnp.transpose(jnp.broadcast_to(row, (LANES, row.shape[1])))


def widened(column, length):
    return jnp.concatenate([column] * (length // LANES), axis=1)


def mixing_kernel(
    count, n_seq, n_opt, w_ref, layer_ref, x_ref, dy_ref, run_ref, mix_ref, proj_ref,
    got, layer, load, send_a, recv_a, send_b, recv_b, send_c, recv_c, send_d, recv_d,
):
    seq = lax.axis_index("seq")
    opt = lax.axis_index("opt")
    h = pl.program_id(0)
    last = pl.num_programs(0) - 1
    n_pairs = n_seq // 2
    pair, side, cross, core, twins = place_of(seq, opt)
    core_twin, cross_twin, side_twin = twins
    half = w_ref.shape[0] // 2
    low, high = slice(0, half), slice(half, 2 * half)

    def same(part, send_sem, recv_sem, k, device):
        return remote(part, part, send_sem.at[k], recv_sem.at[k], device)

    def along():
        own = got.at[pair, side, cross, core]
        return swap_all(
            n_pairs, pair, lambda p: own, lambda p: got.at[p, side, cross, core],
            lambda p: (p * 2 + side, opt), send_a, recv_a,
        )

    def second():
        return (
            same(got.at[:, side, cross, core, low], send_b, recv_b, 0, side_twin),
            same(got.at[:, side, cross, core, high], send_b, recv_b, 1, cross_twin),
        )

    def third():
        return (
            same(got.at[:, :, cross, core, low], send_c, recv_c, 0, cross_twin),
            same(got.at[:, side, :, core, high], send_c, recv_c, 1, side_twin),
        )

    def to_core(k):
        parts = (
            lambda: got.at[:, side, cross, core],
            lambda: got.at[:, 1 - side, cross, core, low],
            lambda: got.at[:, side, 1 - cross, core, high],
            lambda: got.at[:, :, 1 - cross, core, low],
            lambda: got.at[:, 1 - side, :, core, high],
        )
        return same(parts[k](), send_d, recv_d, k, core_twin)

    def from_core(k):
        parts = (
            lambda: got.at[:, side, cross, 1 - core],
            lambda: got.at[:, 1 - side, cross, 1 - core, low],
            lambda: got.at[:, side, 1 - cross, 1 - core, high],
            lambda: got.at[:, :, 1 - cross, 1 - core, low],
            lambda: got.at[:, 1 - side, :, 1 - core, high],
        )
        return same(parts[k](), send_d, recv_d, k, core_twin)

    def load_layer():
        return pltpu.make_async_copy(layer_ref, layer, load)

    @pl.when(h == 0)
    def _():
        got[pair, side, cross, core] = w_ref[...].astype(bf16)
        greet_twins(n_pairs, seq, opt)
        along()[0]()
        load_layer().start()
        mix_ref[...] = jnp.zeros_like(mix_ref)

    @pl.when(h == last * STEP_B // 32)
    def _():
        along()[1]()
        for copy in second():
            copy.start()
        to_core(0).start()

    @pl.when(h == last * STEP_C // 32)
    def _():
        for copy in second():
            copy.wait()
        for copy in third():
            copy.start()
        to_core(1).start()
        to_core(2).start()

    row_pos = lax.broadcasted_iota(jnp.int32, (BLOCK, BLOCK), 0)
    col_pos = lax.broadcasted_iota(jnp.int32, (BLOCK, BLOCK), 1)
    for b in range(count):
        rows = slice(b * BLOCK, (b + 1) * BLOCK)
        row = run_ref[0, b : b + 1, :]
        spread = widened(as_column(row), BLOCK) - row
        decays = jnp.exp(jnp.where(row_pos >= col_pos, spread, -jnp.inf))
        mix_ref[b] += decays * dot_nt(dy_ref[rows, :], x_ref[rows, :])

    @pl.when(h == last)
    def _():
        for copy in third():
            copy.wait()
        to_core(3).start()
        to_core(4).start()
        load_layer().wait()
        for k in range(5):
            to_core(k).wait_send()
            from_core(k).wait_recv()
        total = None
        for p in range(n_pairs):
            w_part = got[p].reshape(-1, got.shape[-1])
            depth = w_part.shape[0]
            term = dot_nn(layer[:, p * depth : (p + 1) * depth], w_part)
            total = term if total is None else total + term
        proj_ref[...] = total.astype(bf16)


def place_of(seq, opt):
    side, core, cross = lax.rem(seq, 2), lax.rem(opt, 2), opt // 2
    twins = (
        (seq, opt + 1 - 2 * core), (seq, opt + 2 - 4 * cross), (seq + 1 - 2 * side, opt)
    )
    return seq // 2, side, cross, core, twins


def greet_twins(n_pairs, seq, opt):
    barrier = pltpu.get_barrier_semaphore()
    pair, side, cross, core, twins = place_of(seq, opt)

    def hello(device):
        pl.semaphore_signal(barrier, inc=1, device_id=device, device_id_type=MESH)

    def hello_pair(distance, carry):
        hello((lax.rem(pair + distance, n_pairs) * 2 + side, opt))
        return carry

    for device in twins:
        hello(device)
    lax.fori_loop(1, n_pairs, hello_pair, 0)
    pl.semaphore_wait(barrier, n_pairs + 2)


def remote(src, dst, send_sem, recv_sem, device):
    return pltpu.make_async_remote_copy(
        src_ref=src, dst_ref=dst, send_sem=send_sem, recv_sem=recv_sem,
        device_id=device, device_id_type=MESH,
    )


def states_kernel(
    count, heads, n_pairs, skip_ref, x_ref, dy_ref, x_far, dy_far, b_ref, c_ref, run_ref, mix_ref,
    gx_ref, gbc_ref,
    b_turned, c_turned, affinity, acc_b, acc_c, starts, outs, mine, got, chain_in, chain_out,
    decay, decay_far, send_d, recv_d, send_y, recv_y, send_c, recv_c,
):
    i = pl.program_id(0)
    seq = lax.axis_index("seq")
    opt = lax.axis_index("opt")
    pair = seq // 2
    side = lax.rem(seq, 2)
    lag = LAG_SWAP + LAG_CHAIN * (n_pairs - 1)
    state_dim = b_ref.shape[1]
    twin = (seq + 1 - 2 * side, opt)
    ahead = (seq + 2, opt)
    behind = (seq - 2, opt)

    def closings_of(h):
        return [run_ref[h, b : b + 1, BLOCK - 1 : BLOCK] for b in range(count)]

    def swap(h):
        return remote(mine.at[h], got.at[h], send_y.at[h], recv_y.at[h], twin)

    def swap_decay():
        return remote(decay, decay_far, send_d, recv_d, twin)

    def pass_on(way, h):
        return remote(
            chain_out.at[way, h], chain_in.at[way, h], send_c.at[way, h], recv_c.at[way, h],
            (ahead, behind)[way],
        )

    has_source = (pair > 0, pair < n_pairs - 1)
    has_target = (pair < n_pairs - 1, pair > 0)

    @pl.when(i == 0)
    def _():
        barrier = pltpu.get_barrier_semaphore()
        pl.semaphore_signal(barrier, inc=1, device_id=twin, device_id_type=MESH)
        for way in range(2):
            @pl.when(has_target[way])
            def _():
                pl.semaphore_signal(
                    barrier, inc=1, device_id=(ahead, behind)[way], device_id_type=MESH
                )

        def decay_of(h, carry):
            total = sum(closings_of(h), jnp.zeros((1, 1), f32))
            decay[h] = jnp.broadcast_to(jnp.exp(total), (1, LANES))
            return carry

        lax.fori_loop(0, heads, decay_of, 0)
        acc_b[...] = jnp.zeros_like(acc_b)
        acc_c[...] = jnp.zeros_like(acc_c)
        b_turned[...] = jnp.transpose(b_ref[...].astype(f32))
        c_turned[...] = jnp.transpose(c_ref[...].astype(f32))
        for b in range(count):
            rows = slice(b * BLOCK, (b + 1) * BLOCK)
            affinity[b] = dot_nt(b_ref[rows, :], c_ref[rows, :])
        for way in range(2):
            @pl.when(jnp.logical_not(has_source[way]))
            def _():
                chain_in[way] = jnp.zeros_like(chain_in[way])
        neighbours = 1 + (pair > 0).astype(jnp.int32) + (pair < n_pairs - 1).astype(jnp.int32)
        pl.semaphore_wait(barrier, neighbours)
        swap_decay().start()

    @pl.when(i < heads)
    def _():
        h = i
        adds = []
        for b in range(count):
            rows = slice(b * BLOCK, (b + 1) * BLOCK)
            row = run_ref[h, b : b + 1, :]
            closing = row[:, BLOCK - 1 : BLOCK]
            b_scaled = (b_turned[:, rows] * jnp.exp(closing - row)).astype(bf16)
            c_scaled = (c_turned[:, rows] * jnp.exp(row)).astype(bf16)
            adds.append(
                (jnp.exp(closing), dot_nn(b_scaled, x_ref[rows, :]), dot_nn(c_scaled, dy_ref[rows, :]))
            )
        state = adds[0][1]
        for b in range(1, count):
            starts[h, b - 1] = state.astype(bf16)
            state = adds[b][0] * state + adds[b][1]
        mine[h, 0] = state.astype(bf16)
        carried = adds[count - 1][2]
        for b in reversed(range(count - 1)):
            outs[h, b] = carried.astype(bf16)
            carried = adds[b][0] * carried + adds[b][2]
        mine[h, 1] = carried.astype(bf16)
        swap(h).start()

    @pl.when(i == LAG_SWAP)
    def _():
        swap_decay().wait_recv()

    j = i - LAG_SWAP

    @pl.when(jnp.logical_and(j >= 0, j < heads))
    def _():
        swap(j).wait_recv()

    for way in range(2):
        place = pair if way == 0 else n_pairs - 1 - pair
        hop = j - LAG_CHAIN * place

        @pl.when(jnp.logical_and(hop >= 0, hop < heads))
        def _():
            @pl.when(has_source[way])
            def _():
                pass_on(way, hop).wait_recv()

            @pl.when(has_target[way])
            def _():
                own_decay = decay[hop]
                other_decay = decay_far[hop]
                first = side == way
                own_scale = jnp.where(first, other_decay, 1.0)
                other_scale = jnp.where(first, 1.0, own_decay)
                total = (
                    own_decay * other_decay * chain_in[way, hop].astype(f32)
                    + own_scale * mine[hop, way].astype(f32)
                    + other_scale * got[hop, way].astype(f32)
                )
                chain_out[way, hop] = total.astype(bf16)
                pass_on(way, hop).start()

    @pl.when(i >= lag)
    def _():
        h = i - lag
        row_pos = lax.broadcasted_iota(jnp.int32, (BLOCK, BLOCK), 0)
        col_pos = lax.broadcasted_iota(jnp.int32, (BLOCK, BLOCK), 1)
        closings = closings_of(h)
        other_decay = decay_far[h]
        fars = []
        for way in range(2):
            second = side != way
            scale = jnp.where(second, other_decay, 1.0)
            extra = jnp.where(second, jnp.ones((1, LANES), f32), 0.0)
            fars.append(scale * chain_in[way, h].astype(f32) + extra * got[h, way].astype(f32))
        far_state, far_grad = fars
        for b in range(count):
            rows = slice(b * BLOCK, (b + 1) * BLOCK)
            row = run_ref[h, b : b + 1, :]
            column = as_column(row)
            before = sum(closings[:b], jnp.zeros((1, 1), f32))
            after = sum(closings[b + 1 :], jnp.zeros((1, 1), f32))
            if b == 0:
                state_in = far_state.astype(bf16)
            else:
                state_in = (starts[h, b - 1].astype(f32) + jnp.exp(before) * far_state).astype(bf16)
            if b == count - 1:
                grad_in = far_grad.astype(bf16)
            else:
                grad_in = (outs[h, b].astype(f32) + jnp.exp(after) * far_grad).astype(bf16)
            grow = jnp.exp(column)
            shrink = jnp.exp(closings[b] - column)
            x_blk = x_far[rows, :]
            dy_blk = dy_far[rows, :]
            spread = row - widened(column, BLOCK)
            decays = jnp.exp(jnp.where(col_pos >= row_pos, spread, -jnp.inf))
            weighted = (decays * affinity[b]).astype(bf16)
            inner = dot_nn(weighted, dy_blk)
            outer = dot_nn(b_ref[rows, :], grad_in) * shrink
            gx_ref[rows, :] = (inner + outer + skip_ref[h] * dy_blk.astype(f32)).astype(bf16)
            acc_c[rows, :] += grow * dot_nt(dy_blk, state_in)
            acc_b[rows, :] += shrink * dot_nt(x_blk, grad_in)

    @pl.when(i == pl.num_programs(0) - 1)
    def _():
        for b in range(count):
            rows = slice(b * BLOCK, (b + 1) * BLOCK)
            mixing = mix_ref[b].astype(bf16)
            gbc_ref[rows, :state_dim] = (acc_b[rows, :] + dot_tn(mixing, c_ref[rows, :])).astype(bf16)
            gbc_ref[rows, state_dim:] = (acc_c[rows, :] + dot_nn(mixing, b_ref[rows, :])).astype(bf16)
        swap_decay().wait_send()

        def sent(h, carry):
            swap(h).wait_send()
            for way in range(2):
                @pl.when(has_target[way])
                def _():
                    pass_on(way, h).wait_send()
            return carry

        lax.fori_loop(0, heads, sent, 0)


def swap_all(n, me, src_of, dst_of, device_of, send_sem, recv_sem):
    def copy_to(distance):
        other = lax.rem(me + distance, n)
        return pltpu.make_async_remote_copy(
            src_ref=src_of(other), dst_ref=dst_of(me), send_sem=send_sem.at[other],
            recv_sem=recv_sem.at[me], device_id=device_of(other), device_id_type=MESH,
        )

    def copy_from(distance):
        other = lax.rem(me + distance, n)
        return pltpu.make_async_remote_copy(
            src_ref=src_of(other), dst_ref=dst_of(other), send_sem=send_sem.at[other],
            recv_sem=recv_sem.at[other], device_id=device_of(other), device_id_type=MESH,
        )

    def start(distance, carry):
        copy_to(distance).start()
        return carry

    def finish(distance, carry):
        copy = copy_from(distance)
        copy.wait_send()
        copy.wait_recv()
        return carry

    return lambda: lax.fori_loop(1, n, start, 0), lambda: lax.fori_loop(1, n, finish, 0)


def begin_swap(*args):
    start, finish = swap_all(*args)
    start()
    return finish


def weight_kernel(group, layer_ref, grad_ref, gx_ref, part_ref, gx_out, turned, held, load, store):
    pieces, tall, _ = held.shape
    turned[...] = jnp.transpose(grad_ref[...].astype(f32)).astype(bf16)

    def bring(k):
        return pltpu.make_async_copy(gx_ref.at[pl.ds(k * tall, tall)], held.at[k], load.at[k])

    def put(k):
        return pltpu.make_async_copy(held.at[k], gx_out.at[pl.ds(k * tall, tall)], store.at[k])

    for k in range(pieces):
        bring(k).start()
    spots, half, width = part_ref.shape[2:]
    wide = 2 * group * width
    steps = spots // group

    def step(s, carry):
        both = dot_nn(turned[...], layer_ref[:, pl.ds(pl.multiple_of(s * wide, wide), wide)])
        both = both.astype(bf16)
        for t in range(group):
            for c in range(2):
                lanes = slice((2 * t + c) * width, (2 * t + c + 1) * width)
                for k in range(2):
                    rows = slice(k * half, (k + 1) * half)
                    part_ref[c, k, s * group + t] = both[rows, lanes]
        return carry

    lax.fori_loop(0, steps // 2, step, 0)
    for k in range(pieces):
        bring(k).wait()
        put(k).start()
    lax.fori_loop(steps // 2, steps, step, 0)
    for k in range(pieces):
        put(k).wait()


def step_kernel(
    n_seq, n_opt, part_ref, w_ref, code_ref, scale_ref, row_ref, col_ref,
    update_ref, code_out, small_out,
    take_core, give_two, keep_two, take_two, give_three, keep_three, take_three, give_pair, take_pair,
    stats, all_stats, peak, all_peaks,
    send_core, recv_core, send_two, recv_two, send_three, recv_three, send_pair, recv_pair,
    send_c, recv_c, send_d, recv_d,
):
    seq = lax.axis_index("seq")
    opt = lax.axis_index("opt")
    n = n_seq * n_opt
    n_pairs = n_seq // 2
    me = seq * n_opt + opt
    pair, side, cross, core, twins = place_of(seq, opt)
    core_twin, cross_twin, side_twin = twins

    def any_device(i):
        return (i // n_opt, lax.rem(i, n_opt))

    greet_twins(n_pairs, seq, opt)
    to_core = remote(part_ref.at[1 - core], take_core, send_core, recv_core, core_twin)
    to_core.start()
    to_core.wait()

    def chip_sum(k, spot):
        return part_ref[core, k, spot].astype(f32) + take_core[k, spot].astype(f32)

    targets = ((cross_twin, side_twin), (side_twin, cross_twin))
    own = ((cross, side), (side, cross))

    def spot_of(k, p, a, b):
        return (p * 2 + a) * 2 + b if k == 0 else (p * 2 + b) * 2 + a

    def fill_two(q, carry):
        for k in range(2):
            spot = spot_of(k, q // 2, lax.rem(q, 2), 1 - own[0][k])
            give_two[k, q] = chip_sum(k, spot).astype(bf16)
        return carry

    lax.fori_loop(0, 2 * n_pairs, fill_two, 0)
    second = [
        remote(give_two.at[k], take_two.at[k], send_two.at[k], recv_two.at[k], targets[0][k])
        for k in range(2)
    ]
    for copy in second:
        copy.start()

    def stay_two(q, carry):
        for k in range(2):
            spot = spot_of(k, q // 2, lax.rem(q, 2), own[0][k])
            keep_two[k, q] = chip_sum(k, spot)
        return carry

    lax.fori_loop(0, 2 * n_pairs, stay_two, 0)
    for copy in second:
        copy.wait()

    def fill_three(p, carry):
        for k in range(2):
            q = 2 * p + 1 - own[1][k]
            give_three[k, p] = (keep_two[k, q] + take_two[k, q].astype(f32)).astype(bf16)
        return carry

    lax.fori_loop(0, n_pairs, fill_three, 0)
    third = [
        remote(give_three.at[k], take_three.at[k], send_three.at[k], recv_three.at[k], targets[1][k])
        for k in range(2)
    ]
    for copy in third:
        copy.start()

    def stay_three(p, carry):
        for k in range(2):
            q = 2 * p + own[1][k]
            keep_three[k, p] = keep_two[k, q] + take_two[k, q].astype(f32)
        return carry

    lax.fori_loop(0, n_pairs, stay_three, 0)
    for copy in third:
        copy.wait()

    def fill_pair(p, carry):
        for k in range(2):
            give_pair[p, k] = (keep_three[k, p] + take_three[k, p].astype(f32)).astype(bf16)
        return carry

    lax.fori_loop(0, n_pairs, fill_pair, 0)
    end_pairs = begin_swap(
        n_pairs, pair, lambda p: give_pair.at[p], lambda p: take_pair.at[p],
        lambda p: (p * 2 + side, opt), send_pair, recv_pair,
    )
    take_pair[pair] = jnp.zeros_like(take_pair[pair])
    totals = [keep_three[k, pair] + take_three[k, pair].astype(f32) for k in range(2)]
    turned = jnp.concatenate(totals, axis=0)
    end_pairs()

    def gather_pair(p, total):
        return total + jnp.concatenate([take_pair[p, k].astype(f32) for k in range(2)], axis=0)

    turned = lax.fori_loop(0, n_pairs, gather_pair, turned)
    grad = jnp.transpose(turned)

    rows, cols = grad.shape
    width = n * rows
    stats[:, :cols] = jnp.sum(grad * grad, axis=0, keepdims=True)
    row_stat = row_ref[...]
    stats[:, cols:] = jnp.broadcast_to(jnp.sum(row_stat, axis=1, keepdims=True), (1, LANES))
    end_stats = begin_swap(
        n, me, lambda i: stats, lambda i: all_stats.at[i], any_device, send_c, recv_c
    )
    row_raw = jnp.sum(turned * turned, axis=0, keepdims=True)
    old_moment = beta_one * code_ref[...].astype(f32) * scale_ref[...]
    end_stats()
    all_stats[me] = stats[...]
    sums = all_stats[0]
    for i in range(1, n):
        sums += all_stats[i]
    col_raw = sums[:, :cols]
    old_total = sums[:, cols : cols + 1]
    raw_total = jnp.sum(col_raw, axis=1, keepdims=True)
    factor = jnp.minimum(1.0, clip_norm / jnp.sqrt(raw_total + norm_floor))
    moment = old_moment + (1.0 - beta_one) * (grad * factor)
    peak[...] = jnp.max(jnp.abs(moment), axis=0, keepdims=True)
    end_peaks = begin_swap(
        n, me, lambda i: peak, lambda i: all_peaks.at[i], any_device, send_d, recv_d
    )
    col_next = beta_two * col_ref[...] + (1.0 - beta_two) * (
        factor * factor * col_raw / width + tiny_square
    )
    row_next = beta_two * row_stat + (1.0 - beta_two) * (
        factor * factor * row_raw / cols + tiny_square
    )
    row_mean = (
        beta_two * old_total
        + (1.0 - beta_two) * (factor * factor * raw_total / cols + width * tiny_square)
    ) / width
    small_out[1:2, :] = col_next
    small_out[2:3, :rows] = row_next
    row_column = jnp.transpose(jnp.broadcast_to(row_next / row_mean, (8, rows)))[:, :1]
    second_moment = row_column * col_next
    update_ref[...] = moment / (jnp.sqrt(second_moment) + adam_floor) + weight_decay * w_ref[...]
    end_peaks()
    all_peaks[me] = peak[...]
    scale_next = all_peaks[0]
    for i in range(1, n):
        scale_next = jnp.maximum(scale_next, all_peaks[i])
    scale_next = scale_next + peak_floor
    small_out[0:1, :] = scale_next
    code_out[...] = (moment / scale_next).astype(bf16)


def hand_out(update_ref, code_ref, small_ref, update_out, code_out, scale_out, row_out, col_out):
    update_out[...] = update_ref[...]
    code_out[...] = code_ref[...]
    scale_out[...] = small_ref[0:1, :]
    col_out[...] = small_ref[1:2, :]
    row_out[...] = small_ref[2:3, : row_out.shape[1]]


def params(**more):
    return pltpu.CompilerParams(vmem_limit_bytes=VMEM_LIMIT, **more)


def whole():
    return pl.BlockSpec(memory_space=pltpu.VMEM)


def dma(*counts):
    return [pltpu.SemaphoreType.DMA((count,)) for count in counts for _ in range(2)]


def per_device(
    n_seq, n_opt, layer_in, ssm_input, grad_out, log_decay, skip_gain, w_bc, m_code, m_scale,
    row_stat, col_stat,
):
    layer_rows = layer_in[0]
    x = ssm_input[0]
    dy = grad_out[0]
    length, width = layer_rows.shape
    heads = skip_gain.shape[0]
    head_dim = x.shape[1] // heads
    state_dim = w_bc.shape[1] // 2
    count = length // BLOCK
    n_pairs = n_seq // 2
    own_rows = w_bc.shape[0]

    ones = (
        lax.broadcasted_iota(jnp.int32, (BLOCK, BLOCK), 0)
        <= lax.broadcasted_iota(jnp.int32, (BLOCK, BLOCK), 1)
    ).astype(f32)
    running = jnp.dot(
        log_decay[0].reshape(heads * count, BLOCK), ones, precision=highest
    ).reshape(heads, count, BLOCK)
    tokens = pl.BlockSpec((length, head_dim), lambda h: (0, h))
    run_spec = pl.BlockSpec((1, count, BLOCK), lambda h: (h, 0, 0))
    mix_spec = pl.BlockSpec((count, BLOCK, BLOCK), lambda h: (0, 0, 0))
    b_spec = pl.BlockSpec((length, state_dim), lambda h: (0, 0))
    c_spec = pl.BlockSpec((length, state_dim), lambda h: (0, 1))

    mixing, proj = pl.pallas_call(
        functools.partial(mixing_kernel, count, n_seq, n_opt),
        grid=(heads,),
        in_specs=[
            whole(), pl.BlockSpec(memory_space=pltpu.MemorySpace.HBM), tokens, tokens, run_spec
        ],
        out_specs=[mix_spec, whole()],
        out_shape=[
            jax.ShapeDtypeStruct((count, BLOCK, BLOCK), f32),
            jax.ShapeDtypeStruct((length, 2 * state_dim), bf16),
        ],
        scratch_shapes=[
            pltpu.VMEM((n_pairs, 2, 2, 2, own_rows, 2 * state_dim), bf16),
            pltpu.VMEM((length, width), bf16),
            pltpu.SemaphoreType.DMA,
        ]
        + dma(n_pairs, 2, 2, 5),
        compiler_params=params(collective_id=2, has_side_effects=True),
        name="gather_and_mixing",
    )(w_bc, layer_rows, x, dy, running)

    lag = LAG_SWAP + LAG_CHAIN * (n_pairs - 1)
    near = pl.BlockSpec((length, head_dim), lambda i: (0, jnp.minimum(i, heads - 1)))
    late = pl.BlockSpec((length, head_dim), lambda i: (0, jnp.maximum(i - lag, 0)))
    all_run = pl.BlockSpec((heads, count, BLOCK), lambda i: (0, 0, 0))
    per_head = (heads, 2, state_dim, head_dim)
    per_way = (2, heads, state_dim, head_dim)
    grad_input, grad_bc = pl.pallas_call(
        functools.partial(states_kernel, count, heads, n_pairs),
        grid=(heads + lag,),
        in_specs=[
            pl.BlockSpec(memory_space=pltpu.SMEM), near, near, late, late, b_spec, c_spec, all_run,
            mix_spec,
        ],
        out_specs=[late, pl.BlockSpec((length, 2 * state_dim), lambda h: (0, 0))],
        out_shape=[
            jax.ShapeDtypeStruct(x.shape, bf16),
            jax.ShapeDtypeStruct((length, 2 * state_dim), bf16),
        ],
        scratch_shapes=[
            pltpu.VMEM((state_dim, length), f32),
            pltpu.VMEM((state_dim, length), f32),
            pltpu.VMEM((count, BLOCK, BLOCK), f32),
            pltpu.VMEM((length, state_dim), f32),
            pltpu.VMEM((length, state_dim), f32),
            pltpu.VMEM((heads, max(count - 1, 1), state_dim, head_dim), bf16),
            pltpu.VMEM((heads, max(count - 1, 1), state_dim, head_dim), bf16),
            pltpu.VMEM(per_head, bf16),
            pltpu.VMEM(per_head, bf16),
            pltpu.VMEM(per_way, bf16),
            pltpu.VMEM(per_way, bf16),
            pltpu.VMEM((heads, 1, LANES), f32),
            pltpu.VMEM((heads, 1, LANES), f32),
            pltpu.SemaphoreType.DMA,
            pltpu.SemaphoreType.DMA,
            pltpu.SemaphoreType.DMA((heads,)),
            pltpu.SemaphoreType.DMA((heads,)),
            pltpu.SemaphoreType.DMA((2, heads)),
            pltpu.SemaphoreType.DMA((2, heads)),
        ],
        compiler_params=params(collective_id=0, has_side_effects=True),
        name="states_and_grads",
    )(skip_gain, x, dy, x, dy, proj, proj, running, mixing)

    cols = 2 * state_dim
    n = n_seq * n_opt
    spots = n // 2
    group = max(2, 2 * LANES // own_rows)
    in_hbm = pl.BlockSpec(memory_space=pltpu.MemorySpace.HBM)
    pieces = 8
    part, grad_input = pl.pallas_call(
        functools.partial(weight_kernel, group),
        in_specs=[whole(), whole(), in_hbm],
        out_specs=[whole(), in_hbm],
        out_shape=[
            jax.ShapeDtypeStruct((2, 2, spots, state_dim, own_rows), bf16),
            jax.ShapeDtypeStruct(x.shape, bf16),
        ],
        scratch_shapes=[
            pltpu.VMEM((cols, length), bf16),
            pltpu.VMEM((pieces, length // pieces, x.shape[1]), bf16),
            pltpu.SemaphoreType.DMA((pieces,)),
            pltpu.SemaphoreType.DMA((pieces,)),
        ],
        compiler_params=params(),
        name="weight_gradient",
    )(layer_rows, grad_bc, grad_input)

    block = (state_dim, own_rows)
    tall = jax.ShapeDtypeStruct((own_rows, cols), f32)
    code = jax.ShapeDtypeStruct((own_rows, cols), bf16)
    results = pl.pallas_call(
        functools.partial(step_kernel, n_seq, n_opt),
        in_specs=[whole()] * 6,
        out_specs=[whole()] * 3,
        out_shape=[tall, code, jax.ShapeDtypeStruct((8, cols), f32)],
        scratch_shapes=[
            pltpu.VMEM((2, spots) + block, bf16),
            pltpu.VMEM((2, n_seq) + block, bf16),
            pltpu.VMEM((2, n_seq) + block, f32),
            pltpu.VMEM((2, n_seq) + block, bf16),
            pltpu.VMEM((2, n_pairs) + block, bf16),
            pltpu.VMEM((2, n_pairs) + block, f32),
            pltpu.VMEM((2, n_pairs) + block, bf16),
            pltpu.VMEM((n_pairs, 2) + block, bf16),
            pltpu.VMEM((n_pairs, 2) + block, bf16),
            pltpu.VMEM((1, cols + LANES), f32),
            pltpu.VMEM((n, 1, cols + LANES), f32),
            pltpu.VMEM((1, cols), f32),
            pltpu.VMEM((n, 1, cols), f32),
            pltpu.SemaphoreType.DMA,
            pltpu.SemaphoreType.DMA,
        ]
        + dma(2, 2, n_pairs, n, n),
        compiler_params=params(collective_id=1, has_side_effects=True),
        name="sum_and_step",
    )(part, w_bc, m_code, m_scale[None, :], row_stat[None, :], col_stat[None, :])
    update, code_next, scale_next, row_next, col_next = pl.pallas_call(
        hand_out,
        in_specs=[whole()] * 3,
        out_specs=[whole()] * 5,
        out_shape=[
            tall, code, jax.ShapeDtypeStruct((1, cols), f32),
            jax.ShapeDtypeStruct((1, own_rows), f32), jax.ShapeDtypeStruct((1, cols), f32),
        ],
        compiler_params=params(),
        name="hand_out",
    )(*results)
    return (grad_input[None], update, code_next, scale_next[0], row_next[0], col_next[0])


def solution(mesh):
    return jax.shard_map(
        functools.partial(per_device, mesh.shape["seq"], mesh.shape["opt"]),
        mesh=mesh,
        in_specs=(
            P("opt", "seq", None),
            P("opt", "seq", None),
            P("opt", "seq", None),
            P("opt", None, "seq"),
            P(),
            P(("seq", "opt"), None),
            P(("seq", "opt"), None),
            P(),
            P(("seq", "opt")),
            P(),
        ),
        out_specs=(
            P("opt", "seq", None),
            P(("seq", "opt"), None),
            P(("seq", "opt"), None),
            P(),
            P(("seq", "opt")),
            P(),
        ),
        check_vma=False,
    )
```

```python
import functools

import jax
import jax.numpy as jnp
from jax import lax
from jax.experimental import pallas as pl
from jax.experimental.pallas import tpu as pltpu
from jax.sharding import PartitionSpec as P

BLOCK = 256
LANES = 128
LAG_SWAP = 3
LAG_CHAIN = 2

beta_one = 0.9
beta_two = 0.95
weight_decay = 0.1
clip_norm = 1.0
tiny_square = 1e-30
adam_floor = 1e-08
peak_floor = 1e-06
norm_floor = 1e-06
highest = lax.Precision.HIGHEST
MESH = pl.DeviceIdType.MESH
VMEM_LIMIT = 60 * 1024 * 1024
f32 = jnp.float32
bf16 = jnp.bfloat16


def dot_nn(a, b):
    return lax.dot_general(a, b, (((1,), (0,)), ((), ())), preferred_element_type=f32)


def dot_nt(a, b):
    return lax.dot_general(a, b, (((1,), (1,)), ((), ())), preferred_element_type=f32)


def dot_tn(a, b):
    return lax.dot_general(a, b, (((0,), (0,)), ((), ())), preferred_element_type=f32)


def as_column(row):
    return jnp.transpose(jnp.broadcast_to(row, (LANES, row.shape[1])))


def widened(column, length):
    return jnp.concatenate([column] * (length // LANES), axis=1)


def gather_kernel(
    count, n_seq, n_opt, w_ref, log_ref, layer_ref, proj_ref, run_ref,
    got, layer, total, load, send_a, recv_a, send_b, recv_b, send_c, recv_c, send_d, recv_d,
):
    seq = lax.axis_index("seq")
    opt = lax.axis_index("opt")
    n_pairs = n_seq // 2
    pair, side, cross, core, twins = place_of(seq, opt)
    core_twin, cross_twin, side_twin = twins
    half = w_ref.shape[0] // 2
    low, high = slice(0, half), slice(half, 2 * half)

    def same(part, send_sem, recv_sem, device):
        return remote(part, part, send_sem, recv_sem, device)

    def along(p, owner):
        block = got.at[owner, side, cross, core]
        other = (p * 2 + side, opt)
        return remote(block, block, send_a.at[p], recv_a.at[owner], other)

    def own_to(k, p, s, x):
        device = (cross_twin, side_twin)[k]
        return same(got.at[p, s, x, core], send_b.at[k, p], recv_b.at[k, p], device)

    def relay_to(k, p, s, x):
        device = (cross_twin, side_twin)[k]
        part = got.at[p, s, x, core, (low, high)[k]]
        return same(part, send_c.at[k, p], recv_c.at[k, p], device)

    def to_core(k, p, c):
        s = side if k % 2 == 0 else 1 - side
        x = cross if k // 2 == 0 else 1 - cross
        return same(got.at[p, s, x, c], send_d.at[k, p], recv_d.at[k, p], core_twin)

    layer_copy = pltpu.make_async_copy(layer_ref, layer, load)
    layer_copy.start()
    got[pair, side, cross, core] = w_ref[...].astype(bf16)
    greet_twins(n_pairs, seq, opt)

    def send_along(distance, carry):
        along(lax.rem(pair + distance, n_pairs), pair).start()
        return carry

    lax.fori_loop(1, n_pairs, send_along, 0)
    ones = (
        lax.broadcasted_iota(jnp.int32, (BLOCK, BLOCK), 0)
        <= lax.broadcasted_iota(jnp.int32, (BLOCK, BLOCK), 1)
    ).astype(f32)

    def turn(d, carry):
        @pl.when(d < n_pairs)
        def _():
            p = lax.rem(pair + d, n_pairs)

            @pl.when(d > 0)
            def _():
                along(p, p).wait_recv()

            own_to(0, p, side, cross).start()
            own_to(1, p, side, cross).start()
            to_core(0, p, core).start()

        @pl.when(d == 0)
        def _():
            for b in range(count):
                sums = jnp.dot(
                    log_ref[:, b * BLOCK : (b + 1) * BLOCK], ones,
                    precision=highest, preferred_element_type=f32,
                )
                run_ref[:, b : b + 1, :] = sums[:, None, :]
            total[...] = jnp.zeros_like(total)

        @pl.when(jnp.logical_and(d >= 1, d < n_pairs + 1))
        def _():
            p = lax.rem(pair + d - 1, n_pairs)
            own_to(0, p, side, 1 - cross).wait_recv()
            relay_to(1, p, side, 1 - cross).start()
            own_to(1, p, 1 - side, cross).wait_recv()
            relay_to(0, p, 1 - side, cross).start()
            to_core(1, p, core).start()
            to_core(2, p, core).start()

        @pl.when(jnp.logical_and(d >= 2, d < n_pairs + 2))
        def _():
            p = lax.rem(pair + d - 2, n_pairs)
            relay_to(0, p, 1 - side, 1 - cross).wait_recv()
            relay_to(1, p, 1 - side, 1 - cross).wait_recv()
            to_core(3, p, core).start()

        @pl.when(d == 3)
        def _():
            layer_copy.wait()

        @pl.when(d >= 3)
        def _():
            p = lax.rem(pair + d - 3, n_pairs)
            for k in range(4):
                to_core(k, p, 1 - core).wait_recv()
            w_part = got[p].reshape(-1, got.shape[-1])
            depth = w_part.shape[0]
            columns = pl.ds(pl.multiple_of(p * depth, depth), depth)
            total[...] += dot_nn(layer[:, columns], w_part)

        return carry

    lax.fori_loop(0, n_pairs + 3, turn, 0)
    proj_ref[...] = total[...].astype(bf16)

    def sent(d, carry):
        p = lax.rem(pair + d, n_pairs)

        @pl.when(d > 0)
        def _():
            along(p, pair).wait_send()

        own_to(0, p, side, cross).wait_send()
        own_to(1, p, side, cross).wait_send()
        relay_to(0, p, 1 - side, cross).wait_send()
        relay_to(1, p, side, 1 - cross).wait_send()
        for k in range(4):
            to_core(k, p, core).wait_send()
        return carry

    lax.fori_loop(0, n_pairs, sent, 0)


def place_of(seq, opt):
    side, core, cross = lax.rem(seq, 2), lax.rem(opt, 2), opt // 2
    twins = (
        (seq, opt + 1 - 2 * core), (seq, opt + 2 - 4 * cross), (seq + 1 - 2 * side, opt)
    )
    return seq // 2, side, cross, core, twins


def greet_twins(n_pairs, seq, opt):
    barrier = pltpu.get_barrier_semaphore()
    pair, side, cross, core, twins = place_of(seq, opt)

    def hello(device):
        pl.semaphore_signal(barrier, inc=1, device_id=device, device_id_type=MESH)

    def hello_pair(distance, carry):
        hello((lax.rem(pair + distance, n_pairs) * 2 + side, opt))
        return carry

    for device in twins:
        hello(device)
    lax.fori_loop(1, n_pairs, hello_pair, 0)
    pl.semaphore_wait(barrier, n_pairs + 2)


def remote(src, dst, send_sem, recv_sem, device):
    return pltpu.make_async_remote_copy(
        src_ref=src, dst_ref=dst, send_sem=send_sem, recv_sem=recv_sem,
        device_id=device, device_id_type=MESH,
    )


def states_kernel(
    count, heads, n_pairs, skip_ref, x_ref, dy_ref, x_far, dy_far, b_ref, c_ref, run_ref,
    gx_ref, gbc_ref,
    b_turned, c_turned, affinity, mixing, acc_b, acc_c, starts, outs, mine, got, chain_in, chain_out,
    decay, decay_far, send_d, recv_d, send_y, recv_y, send_c, recv_c,
):
    i = pl.program_id(0)
    seq = lax.axis_index("seq")
    opt = lax.axis_index("opt")
    pair = seq // 2
    side = lax.rem(seq, 2)
    lag = LAG_SWAP + LAG_CHAIN * (n_pairs - 1)
    state_dim = b_ref.shape[1]
    twin = (seq + 1 - 2 * side, opt)
    ahead = (seq + 2, opt)
    behind = (seq - 2, opt)

    def closings_of(h):
        return [run_ref[h, b : b + 1, BLOCK - 1 : BLOCK] for b in range(count)]

    def swap(h):
        return remote(mine.at[h], got.at[h], send_y.at[h], recv_y.at[h], twin)

    def swap_decay():
        return remote(decay, decay_far, send_d, recv_d, twin)

    def pass_on(way, h):
        return remote(
            chain_out.at[way, h], chain_in.at[way, h], send_c.at[way, h], recv_c.at[way, h],
            (ahead, behind)[way],
        )

    has_source = (pair > 0, pair < n_pairs - 1)
    has_target = (pair < n_pairs - 1, pair > 0)

    @pl.when(i == 0)
    def _():
        barrier = pltpu.get_barrier_semaphore()
        pl.semaphore_signal(barrier, inc=1, device_id=twin, device_id_type=MESH)
        for way in range(2):
            @pl.when(has_target[way])
            def _():
                pl.semaphore_signal(
                    barrier, inc=1, device_id=(ahead, behind)[way], device_id_type=MESH
                )

        def decay_of(h, carry):
            total = sum(closings_of(h), jnp.zeros((1, 1), f32))
            decay[h] = jnp.broadcast_to(jnp.exp(total), (1, LANES))
            return carry

        lax.fori_loop(0, heads, decay_of, 0)
        mixing[...] = jnp.zeros_like(mixing)
        acc_b[...] = jnp.zeros_like(acc_b)
        acc_c[...] = jnp.zeros_like(acc_c)
        b_turned[...] = jnp.transpose(b_ref[...].astype(f32))
        c_turned[...] = jnp.transpose(c_ref[...].astype(f32))
        for b in range(count):
            rows = slice(b * BLOCK, (b + 1) * BLOCK)
            affinity[b] = dot_nt(b_ref[rows, :], c_ref[rows, :])
        for way in range(2):
            @pl.when(jnp.logical_not(has_source[way]))
            def _():
                chain_in[way] = jnp.zeros_like(chain_in[way])
        neighbours = 1 + (pair > 0).astype(jnp.int32) + (pair < n_pairs - 1).astype(jnp.int32)
        pl.semaphore_wait(barrier, neighbours)
        swap_decay().start()

    @pl.when(i < heads)
    def _():
        h = i
        adds = []
        for b in range(count):
            rows = slice(b * BLOCK, (b + 1) * BLOCK)
            row = run_ref[h, b : b + 1, :]
            closing = row[:, BLOCK - 1 : BLOCK]
            b_scaled = (b_turned[:, rows] * jnp.exp(closing - row)).astype(bf16)
            c_scaled = (c_turned[:, rows] * jnp.exp(row)).astype(bf16)
            adds.append(
                (jnp.exp(closing), dot_nn(b_scaled, x_ref[rows, :]), dot_nn(c_scaled, dy_ref[rows, :]))
            )
        state = adds[0][1]
        for b in range(1, count):
            starts[h, b - 1] = state.astype(bf16)
            state = adds[b][0] * state + adds[b][1]
        mine[h, 0] = state.astype(bf16)
        carried = adds[count - 1][2]
        for b in reversed(range(count - 1)):
            outs[h, b] = carried.astype(bf16)
            carried = adds[b][0] * carried + adds[b][2]
        mine[h, 1] = carried.astype(bf16)
        swap(h).start()

    @pl.when(i == LAG_SWAP)
    def _():
        swap_decay().wait_recv()

    j = i - LAG_SWAP

    @pl.when(jnp.logical_and(j >= 0, j < heads))
    def _():
        swap(j).wait_recv()

    for way in range(2):
        place = pair if way == 0 else n_pairs - 1 - pair
        hop = j - LAG_CHAIN * place

        @pl.when(jnp.logical_and(hop >= 0, hop < heads))
        def _():
            @pl.when(has_source[way])
            def _():
                pass_on(way, hop).wait_recv()

            @pl.when(has_target[way])
            def _():
                own_decay = decay[hop]
                other_decay = decay_far[hop]
                first = side == way
                own_scale = jnp.where(first, other_decay, 1.0)
                other_scale = jnp.where(first, 1.0, own_decay)
                total = (
                    own_decay * other_decay * chain_in[way, hop].astype(f32)
                    + own_scale * mine[hop, way].astype(f32)
                    + other_scale * got[hop, way].astype(f32)
                )
                chain_out[way, hop] = total.astype(bf16)
                pass_on(way, hop).start()

    @pl.when(i >= lag)
    def _():
        h = i - lag
        row_pos = lax.broadcasted_iota(jnp.int32, (BLOCK, BLOCK), 0)
        col_pos = lax.broadcasted_iota(jnp.int32, (BLOCK, BLOCK), 1)
        closings = closings_of(h)
        other_decay = decay_far[h]
        fars = []
        for way in range(2):
            second = side != way
            scale = jnp.where(second, other_decay, 1.0)
            extra = jnp.where(second, jnp.ones((1, LANES), f32), 0.0)
            fars.append(scale * chain_in[way, h].astype(f32) + extra * got[h, way].astype(f32))
        far_state, far_grad = fars
        for b in range(count):
            rows = slice(b * BLOCK, (b + 1) * BLOCK)
            row = run_ref[h, b : b + 1, :]
            column = as_column(row)
            before = sum(closings[:b], jnp.zeros((1, 1), f32))
            after = sum(closings[b + 1 :], jnp.zeros((1, 1), f32))
            if b == 0:
                state_in = far_state.astype(bf16)
            else:
                state_in = (starts[h, b - 1].astype(f32) + jnp.exp(before) * far_state).astype(bf16)
            if b == count - 1:
                grad_in = far_grad.astype(bf16)
            else:
                grad_in = (outs[h, b].astype(f32) + jnp.exp(after) * far_grad).astype(bf16)
            grow = jnp.exp(column)
            shrink = jnp.exp(closings[b] - column)
            x_blk = x_far[rows, :]
            dy_blk = dy_far[rows, :]
            spread = row - widened(column, BLOCK)
            decays = jnp.exp(jnp.where(col_pos >= row_pos, spread, -jnp.inf))
            mixing[b] += decays * dot_nt(x_blk, dy_blk)
            weighted = (decays * affinity[b]).astype(bf16)
            inner = dot_nn(weighted, dy_blk)
            outer = dot_nn(b_ref[rows, :], grad_in) * shrink
            gx_ref[rows, :] = (inner + outer + skip_ref[h] * dy_blk.astype(f32)).astype(bf16)
            acc_c[rows, :] += grow * dot_nt(dy_blk, state_in)
            acc_b[rows, :] += shrink * dot_nt(x_blk, grad_in)

    @pl.when(i == pl.num_programs(0) - 1)
    def _():
        for b in range(count):
            rows = slice(b * BLOCK, (b + 1) * BLOCK)
            mixed = mixing[b].astype(bf16)
            gbc_ref[rows, :state_dim] = (acc_b[rows, :] + dot_nn(mixed, c_ref[rows, :])).astype(bf16)
            gbc_ref[rows, state_dim:] = (acc_c[rows, :] + dot_tn(mixed, b_ref[rows, :])).astype(bf16)
        swap_decay().wait_send()

        def sent(h, carry):
            swap(h).wait_send()
            for way in range(2):
                @pl.when(has_target[way])
                def _():
                    pass_on(way, h).wait_send()
            return carry

        lax.fori_loop(0, heads, sent, 0)


def swap_all(n, me, src_of, dst_of, device_of, send_sem, recv_sem):
    def copy_to(distance):
        other = lax.rem(me + distance, n)
        return pltpu.make_async_remote_copy(
            src_ref=src_of(other), dst_ref=dst_of(me), send_sem=send_sem.at[other],
            recv_sem=recv_sem.at[me], device_id=device_of(other), device_id_type=MESH,
        )

    def copy_from(distance):
        other = lax.rem(me + distance, n)
        return pltpu.make_async_remote_copy(
            src_ref=src_of(other), dst_ref=dst_of(other), send_sem=send_sem.at[other],
            recv_sem=recv_sem.at[other], device_id=device_of(other), device_id_type=MESH,
        )

    def start(distance, carry):
        copy_to(distance).start()
        return carry

    def finish(distance, carry):
        copy = copy_from(distance)
        copy.wait_send()
        copy.wait_recv()
        return carry

    return lambda: lax.fori_loop(1, n, start, 0), lambda: lax.fori_loop(1, n, finish, 0)


def begin_swap(*args):
    start, finish = swap_all(*args)
    start()
    return finish


def weight_kernel(group, layer_ref, grad_ref, gx_ref, part_ref, gx_out, turned, held, load, store):
    pieces, tall, _ = held.shape
    turned[...] = jnp.transpose(grad_ref[...].astype(f32)).astype(bf16)

    def bring(k):
        return pltpu.make_async_copy(gx_ref.at[pl.ds(k * tall, tall)], held.at[k], load.at[k])

    def put(k):
        return pltpu.make_async_copy(held.at[k], gx_out.at[pl.ds(k * tall, tall)], store.at[k])

    for k in range(pieces):
        bring(k).start()
    _, _, n_i, _, n_r, half, width = part_ref.shape
    wide = 2 * group * width
    steps = 2 * n_i * n_r // group

    def step(s, carry):
        both = dot_nn(turned[...], layer_ref[:, pl.ds(pl.multiple_of(s * wide, wide), wide)])
        both = both.astype(bf16)
        for t in range(group):
            spot = s * group + t
            p = spot // n_r
            for c in range(2):
                lanes = slice((2 * t + c) * width, (2 * t + c + 1) * width)
                for k in range(2):
                    rows = slice(k * half, (k + 1) * half)
                    part_ref[c, k, p // 2, lax.rem(p, 2), lax.rem(spot, n_r)] = both[rows, lanes]
        return carry

    lax.fori_loop(0, steps // 2, step, 0)
    for k in range(pieces):
        bring(k).wait()
        put(k).start()
    lax.fori_loop(steps // 2, steps, step, 0)
    for k in range(pieces):
        put(k).wait()


def step_kernel(
    n_seq, n_opt, part_ref, w_ref, code_ref, scale_ref, row_ref, col_ref,
    update_ref, code_out, small_out,
    take_core, give_two, keep_two, take_two, give_three, keep_three, take_three, give_pair, take_pair,
    stats, all_stats, peak, all_peaks,
    send_core, recv_core, send_two, recv_two, send_three, recv_three, send_pair, recv_pair,
    send_c, recv_c, send_d, recv_d,
):
    seq = lax.axis_index("seq")
    opt = lax.axis_index("opt")
    n = n_seq * n_opt
    n_pairs = n_seq // 2
    me = seq * n_opt + opt
    pair, side, cross, core, twins = place_of(seq, opt)
    core_twin, cross_twin, side_twin = twins

    def any_device(i):
        return (i // n_opt, lax.rem(i, n_opt))

    greet_twins(n_pairs, seq, opt)
    n_i = n_pairs // 2
    targets = ((cross_twin, side_twin), (side_twin, cross_twin))
    own = ((cross, side), (side, cross))
    first = [
        remote(
            part_ref.at[1 - core, :, :, g], take_core.at[:, :, g],
            send_core.at[g], recv_core.at[g], core_twin,
        )
        for g in range(2)
    ]
    second = [
        [
            remote(
                give_two.at[k, g], take_two.at[k, g], send_two.at[k, g], recv_two.at[k, g],
                targets[0][k],
            )
            for k in range(2)
        ]
        for g in range(2)
    ]
    third = [
        [
            remote(
                give_three.at[k, g], take_three.at[k, g], send_three.at[k, g], recv_three.at[k, g],
                targets[1][k],
            )
            for k in range(2)
        ]
        for g in range(2)
    ]

    def chip_sum(k, g, i, a, b):
        r = a * 2 + b if k == 0 else b * 2 + a
        return part_ref[core, k, i, g, r].astype(f32) + take_core[k, i, g, r].astype(f32)

    def fill_two(g):
        def body(q, carry):
            for k in range(2):
                total = chip_sum(k, g, q // 2, lax.rem(q, 2), 1 - own[0][k])
                give_two[k, g, q] = total.astype(bf16)
            return carry

        lax.fori_loop(0, 2 * n_i, body, 0)

    def stay_two(g):
        def body(q, carry):
            for k in range(2):
                keep_two[k, g, q] = chip_sum(k, g, q // 2, lax.rem(q, 2), own[0][k])
            return carry

        lax.fori_loop(0, 2 * n_i, body, 0)

    def fill_three(g):
        def body(i, carry):
            for k in range(2):
                q = 2 * i + 1 - own[1][k]
                total = keep_two[k, g, q] + take_two[k, g, q].astype(f32)
                give_three[k, g, i] = total.astype(bf16)
            return carry

        lax.fori_loop(0, n_i, body, 0)

    def stay_three(g):
        def body(i, carry):
            for k in range(2):
                q = 2 * i + own[1][k]
                keep_three[k, g, i] = keep_two[k, g, q] + take_two[k, g, q].astype(f32)
            return carry

        lax.fori_loop(0, n_i, body, 0)

    def slice_sum(k, g, i):
        return keep_three[k, g, i] + take_three[k, g, i].astype(f32)

    def to_pair(p, source):
        return remote(
            give_pair.at[p], take_pair.at[source], send_pair.at[p], recv_pair.at[source],
            (p * 2 + side, opt),
        )

    for copy in first:
        copy.start()
    for g in range(2):
        first[g].wait()
        fill_two(g)
        for copy in second[g]:
            copy.start()
    for g in range(2):
        stay_two(g)
    for g in range(2):
        for copy in second[g]:
            copy.wait()
        fill_three(g)
        for copy in third[g]:
            copy.start()
    for g in range(2):
        stay_three(g)
    for g in range(2):
        for copy in third[g]:
            copy.wait()

        def send_slices(i, carry):
            p = 2 * i + g

            @pl.when(p != pair)
            def _():
                for k in range(2):
                    give_pair[p, k] = slice_sum(k, g, i).astype(bf16)
                to_pair(p, pair).start()

            return carry

        lax.fori_loop(0, n_i, send_slices, 0)
    take_pair[pair] = jnp.zeros_like(take_pair[pair])
    group_of = lax.rem(pair, 2)
    totals = [slice_sum(k, group_of, pair // 2) for k in range(2)]
    turned = jnp.concatenate(totals, axis=0)

    def end_slices(distance, carry):
        p = lax.rem(pair + distance, n_pairs)
        to_pair(p, p).wait()
        return carry

    lax.fori_loop(1, n_pairs, end_slices, 0)

    def gather_pair(p, total):
        return total + jnp.concatenate([take_pair[p, k].astype(f32) for k in range(2)], axis=0)

    turned = lax.fori_loop(0, n_pairs, gather_pair, turned)
    grad = jnp.transpose(turned)

    rows, cols = grad.shape
    width = n * rows
    stats[:, :cols] = jnp.sum(grad * grad, axis=0, keepdims=True)
    row_stat = row_ref[...]
    stats[:, cols:] = jnp.broadcast_to(jnp.sum(row_stat, axis=1, keepdims=True), (1, LANES))
    end_stats = begin_swap(
        n, me, lambda i: stats, lambda i: all_stats.at[i], any_device, send_c, recv_c
    )
    row_raw = jnp.sum(turned * turned, axis=0, keepdims=True)
    old_moment = beta_one * code_ref[...].astype(f32) * scale_ref[...]
    end_stats()
    all_stats[me] = stats[...]
    sums = all_stats[0]
    for i in range(1, n):
        sums += all_stats[i]
    col_raw = sums[:, :cols]
    old_total = sums[:, cols : cols + 1]
    raw_total = jnp.sum(col_raw, axis=1, keepdims=True)
    factor = jnp.minimum(1.0, clip_norm / jnp.sqrt(raw_total + norm_floor))
    moment = old_moment + (1.0 - beta_one) * (grad * factor)
    peak[...] = jnp.max(jnp.abs(moment), axis=0, keepdims=True)
    end_peaks = begin_swap(
        n, me, lambda i: peak, lambda i: all_peaks.at[i], any_device, send_d, recv_d
    )
    col_next = beta_two * col_ref[...] + (1.0 - beta_two) * (
        factor * factor * col_raw / width + tiny_square
    )
    row_next = beta_two * row_stat + (1.0 - beta_two) * (
        factor * factor * row_raw / cols + tiny_square
    )
    row_mean = (
        beta_two * old_total
        + (1.0 - beta_two) * (factor * factor * raw_total / cols + width * tiny_square)
    ) / width
    small_out[1:2, :] = col_next
    small_out[2:3, :rows] = row_next
    row_column = jnp.transpose(jnp.broadcast_to(row_next / row_mean, (8, rows)))[:, :1]
    second_moment = row_column * col_next
    update_ref[...] = moment / (jnp.sqrt(second_moment) + adam_floor) + weight_decay * w_ref[...]
    end_peaks()
    all_peaks[me] = peak[...]
    scale_next = all_peaks[0]
    for i in range(1, n):
        scale_next = jnp.maximum(scale_next, all_peaks[i])
    scale_next = scale_next + peak_floor
    small_out[0:1, :] = scale_next
    code_out[...] = (moment / scale_next).astype(bf16)


def hand_out(update_ref, code_ref, small_ref, update_out, code_out, scale_out, row_out, col_out):
    update_out[...] = update_ref[...]
    code_out[...] = code_ref[...]
    scale_out[...] = small_ref[0:1, :]
    col_out[...] = small_ref[1:2, :]
    row_out[...] = small_ref[2:3, : row_out.shape[1]]


def params(**more):
    return pltpu.CompilerParams(vmem_limit_bytes=VMEM_LIMIT, **more)


def whole():
    return pl.BlockSpec(memory_space=pltpu.VMEM)


def dma(*counts):
    return [pltpu.SemaphoreType.DMA((count,)) for count in counts for _ in range(2)]


def per_device(
    n_seq, n_opt, layer_in, ssm_input, grad_out, log_decay, skip_gain, w_bc, m_code, m_scale,
    row_stat, col_stat,
):
    layer_rows = layer_in[0]
    x = ssm_input[0]
    dy = grad_out[0]
    length, width = layer_rows.shape
    heads = skip_gain.shape[0]
    head_dim = x.shape[1] // heads
    state_dim = w_bc.shape[1] // 2
    count = length // BLOCK
    n_pairs = n_seq // 2
    own_rows = w_bc.shape[0]

    in_hbm = pl.BlockSpec(memory_space=pltpu.MemorySpace.HBM)
    proj, running = pl.pallas_call(
        functools.partial(gather_kernel, count, n_seq, n_opt),
        in_specs=[whole(), whole(), in_hbm],
        out_specs=[whole(), whole()],
        out_shape=[
            jax.ShapeDtypeStruct((length, 2 * state_dim), bf16),
            jax.ShapeDtypeStruct((heads, count, BLOCK), f32),
        ],
        scratch_shapes=[
            pltpu.VMEM((n_pairs, 2, 2, 2, own_rows, 2 * state_dim), bf16),
            pltpu.VMEM((length, width), bf16),
            pltpu.VMEM((length, 2 * state_dim), f32),
            pltpu.SemaphoreType.DMA,
        ]
        + [pltpu.SemaphoreType.DMA((n_pairs,))] * 2
        + [pltpu.SemaphoreType.DMA((2, n_pairs))] * 4
        + [pltpu.SemaphoreType.DMA((4, n_pairs))] * 2,
        compiler_params=params(collective_id=2, has_side_effects=True),
        name="gather_and_project",
    )(w_bc, log_decay[0], layer_rows)

    b_spec = pl.BlockSpec((length, state_dim), lambda i: (0, 0))
    c_spec = pl.BlockSpec((length, state_dim), lambda i: (0, 1))
    lag = LAG_SWAP + LAG_CHAIN * (n_pairs - 1)
    near = pl.BlockSpec((length, head_dim), lambda i: (0, jnp.minimum(i, heads - 1)))
    late = pl.BlockSpec((length, head_dim), lambda i: (0, jnp.maximum(i - lag, 0)))
    all_run = pl.BlockSpec((heads, count, BLOCK), lambda i: (0, 0, 0))
    per_head = (heads, 2, state_dim, head_dim)
    per_way = (2, heads, state_dim, head_dim)
    grad_input, grad_bc = pl.pallas_call(
        functools.partial(states_kernel, count, heads, n_pairs),
        grid=(heads + lag,),
        in_specs=[
            pl.BlockSpec(memory_space=pltpu.SMEM), near, near, late, late, b_spec, c_spec, all_run,
        ],
        out_specs=[late, pl.BlockSpec((length, 2 * state_dim), lambda h: (0, 0))],
        out_shape=[
            jax.ShapeDtypeStruct(x.shape, bf16),
            jax.ShapeDtypeStruct((length, 2 * state_dim), bf16),
        ],
        scratch_shapes=[
            pltpu.VMEM((state_dim, length), f32),
            pltpu.VMEM((state_dim, length), f32),
            pltpu.VMEM((count, BLOCK, BLOCK), f32),
            pltpu.VMEM((count, BLOCK, BLOCK), f32),
            pltpu.VMEM((length, state_dim), f32),
            pltpu.VMEM((length, state_dim), f32),
            pltpu.VMEM((heads, max(count - 1, 1), state_dim, head_dim), bf16),
            pltpu.VMEM((heads, max(count - 1, 1), state_dim, head_dim), bf16),
            pltpu.VMEM(per_head, bf16),
            pltpu.VMEM(per_head, bf16),
            pltpu.VMEM(per_way, bf16),
            pltpu.VMEM(per_way, bf16),
            pltpu.VMEM((heads, 1, LANES), f32),
            pltpu.VMEM((heads, 1, LANES), f32),
            pltpu.SemaphoreType.DMA,
            pltpu.SemaphoreType.DMA,
            pltpu.SemaphoreType.DMA((heads,)),
            pltpu.SemaphoreType.DMA((heads,)),
            pltpu.SemaphoreType.DMA((2, heads)),
            pltpu.SemaphoreType.DMA((2, heads)),
        ],
        compiler_params=params(collective_id=0, has_side_effects=True),
        name="states_and_grads",
    )(skip_gain, x, dy, x, dy, proj, proj, running)

    cols = 2 * state_dim
    n = n_seq * n_opt
    spots = n // 2
    group = max(2, 2 * LANES // own_rows)
    pieces = 8
    part, grad_input = pl.pallas_call(
        functools.partial(weight_kernel, group),
        in_specs=[whole(), whole(), in_hbm],
        out_specs=[whole(), in_hbm],
        out_shape=[
            jax.ShapeDtypeStruct((2, 2, n_pairs // 2, 2, 4, state_dim, own_rows), bf16),
            jax.ShapeDtypeStruct(x.shape, bf16),
        ],
        scratch_shapes=[
            pltpu.VMEM((cols, length), bf16),
            pltpu.VMEM((pieces, length // pieces, x.shape[1]), bf16),
            pltpu.SemaphoreType.DMA((pieces,)),
            pltpu.SemaphoreType.DMA((pieces,)),
        ],
        compiler_params=params(),
        name="weight_gradient",
    )(layer_rows, grad_bc, grad_input)

    block = (state_dim, own_rows)
    tall = jax.ShapeDtypeStruct((own_rows, cols), f32)
    code = jax.ShapeDtypeStruct((own_rows, cols), bf16)
    results = pl.pallas_call(
        functools.partial(step_kernel, n_seq, n_opt),
        in_specs=[whole()] * 6,
        out_specs=[whole()] * 3,
        out_shape=[tall, code, jax.ShapeDtypeStruct((8, cols), f32)],
        scratch_shapes=[
            pltpu.VMEM((2, n_pairs // 2, 2, 4) + block, bf16),
            pltpu.VMEM((2, 2, n_pairs) + block, bf16),
            pltpu.VMEM((2, 2, n_pairs) + block, f32),
            pltpu.VMEM((2, 2, n_pairs) + block, bf16),
            pltpu.VMEM((2, 2, n_pairs // 2) + block, bf16),
            pltpu.VMEM((2, 2, n_pairs // 2) + block, f32),
            pltpu.VMEM((2, 2, n_pairs // 2) + block, bf16),
            pltpu.VMEM((n_pairs, 2) + block, bf16),
            pltpu.VMEM((n_pairs, 2) + block, bf16),
            pltpu.VMEM((1, cols + LANES), f32),
            pltpu.VMEM((n, 1, cols + LANES), f32),
            pltpu.VMEM((1, cols), f32),
            pltpu.VMEM((n, 1, cols), f32),
        ]
        + dma(2)
        + [pltpu.SemaphoreType.DMA((2, 2))] * 4
        + dma(n_pairs, n, n),
        compiler_params=params(collective_id=1, has_side_effects=True),
        name="sum_and_step",
    )(part, w_bc, m_code, m_scale[None, :], row_stat[None, :], col_stat[None, :])
    update, code_next, scale_next, row_next, col_next = pl.pallas_call(
        hand_out,
        in_specs=[whole()] * 3,
        out_specs=[whole()] * 5,
        out_shape=[
            tall, code, jax.ShapeDtypeStruct((1, cols), f32),
            jax.ShapeDtypeStruct((1, own_rows), f32), jax.ShapeDtypeStruct((1, cols), f32),
        ],
        compiler_params=params(),
        name="hand_out",
    )(*results)
    return (grad_input[None], update, code_next, scale_next[0], row_next[0], col_next[0])


def solution(mesh):
    return jax.shard_map(
        functools.partial(per_device, mesh.shape["seq"], mesh.shape["opt"]),
        mesh=mesh,
        in_specs=(
            P("opt", "seq", None),
            P("opt", "seq", None),
            P("opt", "seq", None),
            P("opt", None, "seq"),
            P(),
            P(("seq", "opt"), None),
            P(("seq", "opt"), None),
            P(),
            P(("seq", "opt")),
            P(),
        ),
        out_specs=(
            P("opt", "seq", None),
            P(("seq", "opt"), None),
            P(("seq", "opt"), None),
            P(),
            P(("seq", "opt")),
            P(),
        ),
        check_vma=False,
    )
```

```python
import functools

import jax
import jax.numpy as jnp
from jax import lax
from jax.experimental import pallas as pl
from jax.experimental.pallas import tpu as pltpu
from jax.sharding import PartitionSpec as P

BLOCK = 256
LANES = 128
LAG_SWAP = 3
LAG_CHAIN = 3

beta_one = 0.9
beta_two = 0.95
weight_decay = 0.1
clip_norm = 1.0
tiny_square = 1e-30
adam_floor = 1e-08
peak_floor = 1e-06
norm_floor = 1e-06
highest = lax.Precision.HIGHEST
MESH = pl.DeviceIdType.MESH
f32 = jnp.float32
bf16 = jnp.bfloat16


def dot_nn(a, b):
    return lax.dot_general(a, b, (((1,), (0,)), ((), ())), preferred_element_type=f32)


def dot_nt(a, b):
    return lax.dot_general(a, b, (((1,), (1,)), ((), ())), preferred_element_type=f32)


def dot_tn(a, b):
    return lax.dot_general(a, b, (((0,), (0,)), ((), ())), preferred_element_type=f32)


def as_column(row):
    return jnp.transpose(jnp.broadcast_to(row, (LANES, row.shape[1])))


def widened(column, length):
    return jnp.concatenate([column] * (length // LANES), axis=1)


def gather_kernel(
    count, n_seq, n_opt, w_ref, log_ref, layer_ref, proj_ref, run_ref, decay_ref,
    got, layer, total, decay, load, send_e, recv_e, send_a, recv_a, send_b, recv_b, send_c, recv_c, send_d, recv_d,
):
    seq = lax.axis_index("seq")
    opt = lax.axis_index("opt")
    n_pairs = n_seq // 2
    pair, side, cross, core, twins = place_of(seq, opt)
    core_twin, cross_twin, side_twin = twins
    half = w_ref.shape[0] // 2
    low, high = slice(0, half), slice(half, 2 * half)

    def same(part, send_sem, recv_sem, device):
        return remote(part, part, send_sem, recv_sem, device)

    def along(p, owner):
        block = got.at[owner, side, cross, core]
        other = (p * 2 + side, opt)
        return remote(block, block, send_a.at[p], recv_a.at[owner], other)

    def own_to(k, p, s, x):
        device = (cross_twin, side_twin)[k]
        return same(got.at[p, s, x, core], send_b.at[k, p], recv_b.at[k, p], device)

    def relay_to(k, p, s, x):
        device = (cross_twin, side_twin)[k]
        part = got.at[p, s, x, core, (low, high)[k]]
        return same(part, send_c.at[k, p], recv_c.at[k, p], device)

    def to_core(k, p, c):
        s = side if k % 2 == 0 else 1 - side
        x = cross if k // 2 == 0 else 1 - cross
        return same(got.at[p, s, x, c], send_d.at[k, p], recv_d.at[k, p], core_twin)

    def decay_copy():
        return remote(decay.at[0], decay.at[1], send_e, recv_e, side_twin)

    layer_copy = pltpu.make_async_copy(layer_ref, layer, load)
    layer_copy.start()
    got[pair, side, cross, core] = w_ref[...].astype(bf16)
    greet_twins(n_pairs, seq, opt)

    def send_along(distance, carry):
        along(lax.rem(pair + distance, n_pairs), pair).start()
        return carry

    lax.fori_loop(1, n_pairs, send_along, 0)
    ones = (
        lax.broadcasted_iota(jnp.int32, (BLOCK, BLOCK), 0)
        <= lax.broadcasted_iota(jnp.int32, (BLOCK, BLOCK), 1)
    ).astype(f32)

    def turn(d, carry):
        @pl.when(d < n_pairs)
        def _():
            p = lax.rem(pair + d, n_pairs)

            @pl.when(d > 0)
            def _():
                along(p, p).wait_recv()

            own_to(0, p, side, cross).start()
            own_to(1, p, side, cross).start()
            to_core(0, p, core).start()

        @pl.when(d == 0)
        def _():
            closing = None
            for b in range(count):
                sums = jnp.dot(
                    log_ref[:, b * BLOCK : (b + 1) * BLOCK], ones,
                    precision=highest, preferred_element_type=f32,
                )
                run_ref[:, b : b + 1, :] = sums[:, None, :]
                tail = sums[:, BLOCK - 1 :]
                closing = tail if closing is None else closing + tail
            decay[0] = jnp.broadcast_to(jnp.exp(closing), (closing.shape[0], LANES))[:, None, :]
            total[...] = jnp.zeros_like(total)

        @pl.when(d == 1)
        def _():
            decay_copy().start()

        @pl.when(jnp.logical_and(d >= 1, d < n_pairs + 1))
        def _():
            p = lax.rem(pair + d - 1, n_pairs)
            own_to(0, p, side, 1 - cross).wait_recv()
            relay_to(1, p, side, 1 - cross).start()
            own_to(1, p, 1 - side, cross).wait_recv()
            relay_to(0, p, 1 - side, cross).start()
            to_core(1, p, core).start()
            to_core(2, p, core).start()

        @pl.when(jnp.logical_and(d >= 2, d < n_pairs + 2))
        def _():
            p = lax.rem(pair + d - 2, n_pairs)
            relay_to(0, p, 1 - side, 1 - cross).wait_recv()
            relay_to(1, p, 1 - side, 1 - cross).wait_recv()
            to_core(3, p, core).start()

        @pl.when(d == 3)
        def _():
            layer_copy.wait()

        @pl.when(d >= 3)
        def _():
            p = lax.rem(pair + d - 3, n_pairs)
            for k in range(4):
                to_core(k, p, 1 - core).wait_recv()
            w_part = got[p].reshape(-1, got.shape[-1])
            depth = w_part.shape[0]
            columns = pl.ds(pl.multiple_of(p * depth, depth), depth)
            total[...] += dot_nn(layer[:, columns], w_part)

        return carry

    lax.fori_loop(0, n_pairs + 3, turn, 0)
    proj_ref[...] = total[...].astype(bf16)
    decay_copy().wait()
    decay_ref[...] = decay[...]

    def sent(d, carry):
        p = lax.rem(pair + d, n_pairs)

        @pl.when(d > 0)
        def _():
            along(p, pair).wait_send()

        own_to(0, p, side, cross).wait_send()
        own_to(1, p, side, cross).wait_send()
        relay_to(0, p, 1 - side, cross).wait_send()
        relay_to(1, p, side, 1 - cross).wait_send()
        for k in range(4):
            to_core(k, p, core).wait_send()
        return carry

    lax.fori_loop(0, n_pairs, sent, 0)


def place_of(seq, opt):
    side, core, cross = lax.rem(seq, 2), lax.rem(opt, 2), opt // 2
    twins = (
        (seq, opt + 1 - 2 * core), (seq, opt + 2 - 4 * cross), (seq + 1 - 2 * side, opt)
    )
    return seq // 2, side, cross, core, twins


def greet_twins(n_pairs, seq, opt):
    barrier = pltpu.get_barrier_semaphore()
    pair, side, cross, core, twins = place_of(seq, opt)

    def hello(device):
        pl.semaphore_signal(barrier, inc=1, device_id=device, device_id_type=MESH)

    def hello_pair(distance, carry):
        hello((lax.rem(pair + distance, n_pairs) * 2 + side, opt))
        return carry

    for device in twins:
        hello(device)
    lax.fori_loop(1, n_pairs, hello_pair, 0)
    pl.semaphore_wait(barrier, n_pairs + 2)


def remote(src, dst, send_sem, recv_sem, device):
    return pltpu.make_async_remote_copy(
        src_ref=src, dst_ref=dst, send_sem=send_sem, recv_sem=recv_sem,
        device_id=device, device_id_type=MESH,
    )


def states_kernel(
    count, heads, n_pairs, skip_ref, x_ref, dy_ref, proj_ref, run_ref, decay_ref,
    gx_ref, gbc_ref,
    b_turned, c_turned, affinity, mixing, acc_b, acc_c, starts, outs, mine, got, chain_in, chain_out,
    send_y, recv_y, send_c, recv_c,
):
    seq = lax.axis_index("seq")
    opt = lax.axis_index("opt")
    pair = seq // 2
    side = lax.rem(seq, 2)
    state_dim = proj_ref.shape[1] // 2
    head_dim = x_ref.shape[1] // heads
    b_cols, c_cols = slice(0, state_dim), slice(state_dim, 2 * state_dim)
    twin = (seq + 1 - 2 * side, opt)
    ahead = (seq + 2, opt)
    behind = (seq - 2, opt)
    has_source = (pair > 0, pair < n_pairs - 1)
    has_target = (pair < n_pairs - 1, pair > 0)
    places = (pair, n_pairs - 1 - pair)

    late = heads // 4
    early = 3 * heads // 16
    reach = LAG_CHAIN * (n_pairs - 1)
    wait = max(0, reach - heads + late)
    swap_lag = late + LAG_SWAP
    steps = max(heads - late + reach, heads + wait) + swap_lag

    def head_of(slot):
        return jnp.where(
            slot < early, slot, jnp.where(slot < heads - late, slot + late, slot - heads + late + early)
        )

    def lanes_of(h):
        return pl.ds(pl.multiple_of(h * head_dim, head_dim), head_dim)

    def closings_of(h):
        return [run_ref[h, b : b + 1, BLOCK - 1 : BLOCK] for b in range(count)]

    def swap(h):
        return remote(mine.at[h], got.at[h], send_y.at[h], recv_y.at[h], twin)

    def swap_late(h):
        return remote(chain_out.at[2, h], got.at[h], send_y.at[h], recv_y.at[h], twin)

    def pass_on(way, h):
        return remote(
            chain_out.at[way, h, 0], chain_in.at[way, h], send_c.at[way, h], recv_c.at[way, h],
            (ahead, behind)[way],
        )

    def hop(way, h, with_other):
        @pl.when(has_source[way])
        def _():
            pass_on(way, h).wait_recv()

        @pl.when(has_target[way])
        def _():
            own_decay = decay_ref[0, h]
            other_decay = decay_ref[1, h]
            first = side == way
            own_scale = jnp.where(first, other_decay, 1.0)
            total = (
                own_decay * other_decay * chain_in[way, h].astype(f32)
                + own_scale * mine[h, way].astype(f32)
            )
            if with_other:
                other_scale = jnp.where(first, 1.0, own_decay)
                total += other_scale * got[h, way].astype(f32)
            chain_out[way, h, 0] = total.astype(bf16)
            pass_on(way, h).start()

    def local(h):
        adds = []
        for b in range(count):
            rows = slice(b * BLOCK, (b + 1) * BLOCK)
            row = run_ref[h, b : b + 1, :]
            closing = row[:, BLOCK - 1 : BLOCK]
            b_scaled = (b_turned[:, rows] * jnp.exp(closing - row)).astype(bf16)
            c_scaled = (c_turned[:, rows] * jnp.exp(row)).astype(bf16)
            x_blk = x_ref[rows, lanes_of(h)]
            dy_blk = dy_ref[rows, lanes_of(h)]
            adds.append((jnp.exp(closing), dot_nn(b_scaled, x_blk), dot_nn(c_scaled, dy_blk)))
        state = adds[0][1]
        for b in range(1, count):
            starts[h, b - 1] = state.astype(bf16)
            state = adds[b][0] * state + adds[b][1]
        mine[h, 0] = state.astype(bf16)
        carried = adds[count - 1][2]
        for b in reversed(range(count - 1)):
            outs[h, b] = carried.astype(bf16)
            carried = adds[b][0] * carried + adds[b][2]
        mine[h, 1] = carried.astype(bf16)

    def finish(h, swapped_late):
        row_pos = lax.broadcasted_iota(jnp.int32, (BLOCK, BLOCK), 0)
        col_pos = lax.broadcasted_iota(jnp.int32, (BLOCK, BLOCK), 1)
        closings = closings_of(h)
        other_decay = decay_ref[1, h]
        fars = []
        for way in range(2):
            second = side != way
            scale = jnp.where(second, other_decay, 1.0)
            extra = jnp.where(jnp.logical_or(second, swapped_late), jnp.ones((1, LANES), f32), 0.0)
            fars.append(scale * chain_in[way, h].astype(f32) + extra * got[h, way].astype(f32))
        far_state, far_grad = fars
        for b in range(count):
            rows = slice(b * BLOCK, (b + 1) * BLOCK)
            row = run_ref[h, b : b + 1, :]
            column = as_column(row)
            before = sum(closings[:b], jnp.zeros((1, 1), f32))
            after = sum(closings[b + 1 :], jnp.zeros((1, 1), f32))
            if b == 0:
                state_in = far_state.astype(bf16)
            else:
                state_in = (starts[h, b - 1].astype(f32) + jnp.exp(before) * far_state).astype(bf16)
            if b == count - 1:
                grad_in = far_grad.astype(bf16)
            else:
                grad_in = (outs[h, b].astype(f32) + jnp.exp(after) * far_grad).astype(bf16)
            grow = jnp.exp(column)
            shrink = jnp.exp(closings[b] - column)
            x_blk = x_ref[rows, lanes_of(h)]
            dy_blk = dy_ref[rows, lanes_of(h)]
            spread = row - widened(column, BLOCK)
            decays = jnp.exp(jnp.where(col_pos >= row_pos, spread, -jnp.inf))
            mixing[b] += decays * dot_nt(x_blk, dy_blk)
            weighted = (decays * affinity[b]).astype(bf16)
            inner = dot_nn(weighted, dy_blk)
            outer = dot_nn(proj_ref[rows, b_cols], grad_in) * shrink
            full = inner + outer + skip_ref[h] * dy_blk.astype(f32)
            gx_ref[rows, lanes_of(h)] = full.astype(bf16)
            acc_c[rows, :] += grow * dot_nt(dy_blk, state_in)
            acc_b[rows, :] += shrink * dot_nt(x_blk, grad_in)

    barrier = pltpu.get_barrier_semaphore()
    pl.semaphore_signal(barrier, inc=1, device_id=twin, device_id_type=MESH)
    for way in range(2):
        @pl.when(has_target[way])
        def _():
            pl.semaphore_signal(barrier, inc=1, device_id=(ahead, behind)[way], device_id_type=MESH)

    b_turned[...] = jnp.transpose(proj_ref[:, b_cols].astype(f32))
    c_turned[...] = jnp.transpose(proj_ref[:, c_cols].astype(f32))
    for way in range(2):
        @pl.when(jnp.logical_not(has_source[way]))
        def _():
            chain_in[way] = jnp.zeros_like(chain_in[way])
    neighbours = 1 + (pair > 0).astype(jnp.int32) + (pair < n_pairs - 1).astype(jnp.int32)
    pl.semaphore_wait(barrier, neighbours)

    def step(i, carry):
        is_late = jnp.logical_and(i >= early, i < early + late)

        @pl.when(i < heads)
        def _():
            local(i)

            @pl.when(jnp.logical_not(is_late))
            def _():
                swap(i).start()

        @pl.when(i == early)
        def _():
            mixing[...] = jnp.zeros_like(mixing)
            acc_b[...] = jnp.zeros_like(acc_b)
            acc_c[...] = jnp.zeros_like(acc_c)
            for b in range(count):
                rows = slice(b * BLOCK, (b + 1) * BLOCK)
                affinity[b] = dot_nt(proj_ref[rows, b_cols], proj_ref[rows, c_cols])

        for way in range(2):
            h = i - 1 - LAG_CHAIN * places[way]

            @pl.when(jnp.logical_and(h >= early, h < early + late))
            def _():
                hop(way, h, False)

        slot = i - late - wait

        @pl.when(jnp.logical_and(slot >= heads - late, slot < heads))
        def _():
            h = head_of(slot)
            own_decay = decay_ref[0, h]
            for way in range(2):
                first = side == way
                scale = jnp.where(first, own_decay, 1.0)
                extra = jnp.where(first, jnp.ones((1, LANES), f32), 0.0)
                total = scale * chain_in[way, h].astype(f32) + extra * mine[h, way].astype(f32)
                chain_out[2, h, way] = total.astype(bf16)
            swap_late(h).start()

        slot = i - swap_lag

        @pl.when(jnp.logical_and(slot >= 0, slot < heads - late))
        def _():
            swap(head_of(slot)).wait_recv()

        for way in range(2):
            slot = i - swap_lag - LAG_CHAIN * places[way]

            @pl.when(jnp.logical_and(slot >= 0, slot < heads - late))
            def _():
                hop(way, head_of(slot), True)

        slot = i - swap_lag - reach

        @pl.when(jnp.logical_and(slot >= 0, slot < heads - late))
        def _():
            finish(head_of(slot), False)

        slot = i - swap_lag - wait

        @pl.when(jnp.logical_and(slot >= heads - late, slot < heads))
        def _():
            h = head_of(slot)
            swap_late(h).wait_recv()
            finish(h, True)

        return carry

    lax.fori_loop(0, steps, step, 0)
    for b in range(count):
        rows = slice(b * BLOCK, (b + 1) * BLOCK)
        mixed = mixing[b].astype(bf16)
        gbc_ref[rows, b_cols] = (acc_b[rows, :] + dot_nn(mixed, proj_ref[rows, c_cols])).astype(bf16)
        gbc_ref[rows, c_cols] = (acc_c[rows, :] + dot_tn(mixed, proj_ref[rows, b_cols])).astype(bf16)

    def sent(h, carry):
        is_late = jnp.logical_and(h >= early, h < early + late)

        @pl.when(is_late)
        def _():
            swap_late(h).wait_send()

        @pl.when(jnp.logical_not(is_late))
        def _():
            swap(h).wait_send()

        for way in range(2):
            @pl.when(has_target[way])
            def _():
                pass_on(way, h).wait_send()

        return carry

    lax.fori_loop(0, heads, sent, 0)


def swap_all(n, me, src_of, dst_of, device_of, send_sem, recv_sem):
    def copy_to(distance):
        other = lax.rem(me + distance, n)
        return pltpu.make_async_remote_copy(
            src_ref=src_of(other), dst_ref=dst_of(me), send_sem=send_sem.at[other],
            recv_sem=recv_sem.at[me], device_id=device_of(other), device_id_type=MESH,
        )

    def copy_from(distance):
        other = lax.rem(me + distance, n)
        return pltpu.make_async_remote_copy(
            src_ref=src_of(other), dst_ref=dst_of(other), send_sem=send_sem.at[other],
            recv_sem=recv_sem.at[other], device_id=device_of(other), device_id_type=MESH,
        )

    def start(distance, carry):
        copy_to(distance).start()
        return carry

    def finish(distance, carry):
        copy = copy_from(distance)
        copy.wait_send()
        copy.wait_recv()
        return carry

    return lambda: lax.fori_loop(1, n, start, 0), lambda: lax.fori_loop(1, n, finish, 0)


def begin_swap(*args):
    start, finish = swap_all(*args)
    start()
    return finish


def weight_kernel(group, layer_ref, grad_ref, gx_ref, part_ref, gx_out, turned, store):
    put = pltpu.make_async_copy(gx_ref, gx_out, store)
    put.start()
    turned[...] = jnp.transpose(grad_ref[...].astype(f32)).astype(bf16)

    _, _, n_i, _, n_r, half, width = part_ref.shape
    wide = 2 * group * width
    steps = 2 * n_i * n_r // group

    def step(s, carry):
        both = dot_nn(turned[...], layer_ref[:, pl.ds(pl.multiple_of(s * wide, wide), wide)])
        both = both.astype(bf16)
        for t in range(group):
            spot = s * group + t
            p = spot // n_r
            for c in range(2):
                lanes = slice((2 * t + c) * width, (2 * t + c + 1) * width)
                for k in range(2):
                    rows = slice(k * half, (k + 1) * half)
                    part_ref[c, k, p // 2, lax.rem(p, 2), lax.rem(spot, n_r)] = both[rows, lanes]
        return carry

    lax.fori_loop(0, steps, step, 0)
    put.wait()


def step_kernel(
    n_seq, n_opt, part_ref, w_ref, code_ref, scale_ref, row_ref, col_ref,
    update_ref, code_out, small_out,
    take_core, give_two, keep_two, take_two, give_three, keep_three, take_three, give_pair, take_pair,
    stats, all_stats, peak, all_peaks,
    send_core, recv_core, send_two, recv_two, send_three, recv_three, send_pair, recv_pair,
    send_c, recv_c, send_d, recv_d,
):
    seq = lax.axis_index("seq")
    opt = lax.axis_index("opt")
    n = n_seq * n_opt
    n_pairs = n_seq // 2
    me = seq * n_opt + opt
    pair, side, cross, core, twins = place_of(seq, opt)
    core_twin, cross_twin, side_twin = twins

    def any_device(i):
        return (i // n_opt, lax.rem(i, n_opt))

    greet_twins(n_pairs, seq, opt)
    n_i = n_pairs // 2
    targets = ((cross_twin, side_twin), (side_twin, cross_twin))
    own = ((cross, side), (side, cross))
    first = [
        remote(
            part_ref.at[1 - core, :, :, g], take_core.at[:, :, g],
            send_core.at[g], recv_core.at[g], core_twin,
        )
        for g in range(2)
    ]
    second = [
        [
            remote(
                give_two.at[k, g], take_two.at[k, g], send_two.at[k, g], recv_two.at[k, g],
                targets[0][k],
            )
            for k in range(2)
        ]
        for g in range(2)
    ]
    third = [
        [
            remote(
                give_three.at[k, g], take_three.at[k, g], send_three.at[k, g], recv_three.at[k, g],
                targets[1][k],
            )
            for k in range(2)
        ]
        for g in range(2)
    ]

    def chip_sum(k, g, i, a, b):
        r = a * 2 + b if k == 0 else b * 2 + a
        return part_ref[core, k, i, g, r].astype(f32) + take_core[k, i, g, r].astype(f32)

    def fill_two(g):
        def body(q, carry):
            for k in range(2):
                total = chip_sum(k, g, q // 2, lax.rem(q, 2), 1 - own[0][k])
                give_two[k, g, q] = total.astype(bf16)
            return carry

        lax.fori_loop(0, 2 * n_i, body, 0)

    def stay_two(g):
        def body(q, carry):
            for k in range(2):
                keep_two[k, g, q] = chip_sum(k, g, q // 2, lax.rem(q, 2), own[0][k])
            return carry

        lax.fori_loop(0, 2 * n_i, body, 0)

    def fill_three(g):
        def body(i, carry):
            for k in range(2):
                q = 2 * i + 1 - own[1][k]
                total = keep_two[k, g, q] + take_two[k, g, q].astype(f32)
                give_three[k, g, i] = total.astype(bf16)
            return carry

        lax.fori_loop(0, n_i, body, 0)

    def stay_three(g):
        def body(i, carry):
            for k in range(2):
                q = 2 * i + own[1][k]
                keep_three[k, g, i] = keep_two[k, g, q] + take_two[k, g, q].astype(f32)
            return carry

        lax.fori_loop(0, n_i, body, 0)

    def slice_sum(k, g, i):
        return keep_three[k, g, i] + take_three[k, g, i].astype(f32)

    def to_pair(p, source):
        return remote(
            give_pair.at[p], take_pair.at[source], send_pair.at[p], recv_pair.at[source],
            (p * 2 + side, opt),
        )

    for copy in first:
        copy.start()
    for g in range(2):
        first[g].wait()
        fill_two(g)
        for copy in second[g]:
            copy.start()
    for g in range(2):
        stay_two(g)
    for g in range(2):
        for copy in second[g]:
            copy.wait()
        fill_three(g)
        for copy in third[g]:
            copy.start()
    for g in range(2):
        stay_three(g)
    for g in range(2):
        for copy in third[g]:
            copy.wait()

        def send_slices(i, carry):
            p = 2 * i + g

            @pl.when(p != pair)
            def _():
                for k in range(2):
                    give_pair[p, k] = slice_sum(k, g, i).astype(bf16)
                to_pair(p, pair).start()

            return carry

        lax.fori_loop(0, n_i, send_slices, 0)
    take_pair[pair] = jnp.zeros_like(take_pair[pair])
    group_of = lax.rem(pair, 2)
    totals = [slice_sum(k, group_of, pair // 2) for k in range(2)]
    turned = jnp.concatenate(totals, axis=0)

    def end_slices(distance, carry):
        p = lax.rem(pair + distance, n_pairs)
        to_pair(p, p).wait()
        return carry

    lax.fori_loop(1, n_pairs, end_slices, 0)

    def gather_pair(p, total):
        return total + jnp.concatenate([take_pair[p, k].astype(f32) for k in range(2)], axis=0)

    turned = lax.fori_loop(0, n_pairs, gather_pair, turned)
    grad = jnp.transpose(turned)

    rows, cols = grad.shape
    width = n * rows
    stats[:, :cols] = jnp.sum(grad * grad, axis=0, keepdims=True)
    row_stat = row_ref[...]
    stats[:, cols:] = jnp.broadcast_to(jnp.sum(row_stat, axis=1, keepdims=True), (1, LANES))
    end_stats = begin_swap(
        n, me, lambda i: stats, lambda i: all_stats.at[i], any_device, send_c, recv_c
    )
    row_raw = jnp.sum(turned * turned, axis=0, keepdims=True)
    old_moment = beta_one * code_ref[...].astype(f32) * scale_ref[...]
    end_stats()
    all_stats[me] = stats[...]
    sums = all_stats[0]
    for i in range(1, n):
        sums += all_stats[i]
    col_raw = sums[:, :cols]
    old_total = sums[:, cols : cols + 1]
    raw_total = jnp.sum(col_raw, axis=1, keepdims=True)
    factor = jnp.minimum(1.0, clip_norm / jnp.sqrt(raw_total + norm_floor))
    moment = old_moment + (1.0 - beta_one) * (grad * factor)
    peak[...] = jnp.max(jnp.abs(moment), axis=0, keepdims=True)
    end_peaks = begin_swap(
        n, me, lambda i: peak, lambda i: all_peaks.at[i], any_device, send_d, recv_d
    )
    col_next = beta_two * col_ref[...] + (1.0 - beta_two) * (
        factor * factor * col_raw / width + tiny_square
    )
    row_next = beta_two * row_stat + (1.0 - beta_two) * (
        factor * factor * row_raw / cols + tiny_square
    )
    row_mean = (
        beta_two * old_total
        + (1.0 - beta_two) * (factor * factor * raw_total / cols + width * tiny_square)
    ) / width
    small_out[1:2, :] = col_next
    small_out[2:3, :rows] = row_next
    row_column = jnp.transpose(jnp.broadcast_to(row_next / row_mean, (8, rows)))[:, :1]
    second_moment = row_column * col_next
    update_ref[...] = moment / (jnp.sqrt(second_moment) + adam_floor) + weight_decay * w_ref[...]
    end_peaks()
    all_peaks[me] = peak[...]
    scale_next = all_peaks[0]
    for i in range(1, n):
        scale_next = jnp.maximum(scale_next, all_peaks[i])
    scale_next = scale_next + peak_floor
    small_out[0:1, :] = scale_next
    code_out[...] = (moment / scale_next).astype(bf16)


def hand_out(update_ref, code_ref, small_ref, update_out, code_out, scale_out, row_out, col_out):
    update_out[...] = update_ref[...]
    code_out[...] = code_ref[...]
    scale_out[...] = small_ref[0:1, :]
    col_out[...] = small_ref[1:2, :]
    row_out[...] = small_ref[2:3, : row_out.shape[1]]


def params(mebibytes, **more):
    return pltpu.CompilerParams(vmem_limit_bytes=mebibytes * 1024 * 1024, **more)


def whole():
    return pl.BlockSpec(memory_space=pltpu.VMEM)


def dma(*counts):
    return [pltpu.SemaphoreType.DMA((count,)) for count in counts for _ in range(2)]


def per_device(
    n_seq, n_opt, layer_in, ssm_input, grad_out, log_decay, skip_gain, w_bc, m_code, m_scale,
    row_stat, col_stat,
):
    layer_rows = layer_in[0]
    x = ssm_input[0]
    dy = grad_out[0]
    length, width = layer_rows.shape
    heads = skip_gain.shape[0]
    head_dim = x.shape[1] // heads
    state_dim = w_bc.shape[1] // 2
    count = length // BLOCK
    n_pairs = n_seq // 2
    own_rows = w_bc.shape[0]

    in_hbm = pl.BlockSpec(memory_space=pltpu.MemorySpace.HBM)
    proj, running, decay = pl.pallas_call(
        functools.partial(gather_kernel, count, n_seq, n_opt),
        in_specs=[whole(), whole(), in_hbm],
        out_specs=[whole()] * 3,
        out_shape=[
            jax.ShapeDtypeStruct((length, 2 * state_dim), bf16),
            jax.ShapeDtypeStruct((heads, count, BLOCK), f32),
            jax.ShapeDtypeStruct((2, heads, 1, LANES), f32),
        ],
        scratch_shapes=[
            pltpu.VMEM((n_pairs, 2, 2, 2, own_rows, 2 * state_dim), bf16),
            pltpu.VMEM((length, width), bf16),
            pltpu.VMEM((length, 2 * state_dim), f32),
            pltpu.VMEM((2, heads, 1, LANES), f32),
            pltpu.SemaphoreType.DMA,
            pltpu.SemaphoreType.DMA,
            pltpu.SemaphoreType.DMA,
        ]
        + [pltpu.SemaphoreType.DMA((n_pairs,))] * 2
        + [pltpu.SemaphoreType.DMA((2, n_pairs))] * 4
        + [pltpu.SemaphoreType.DMA((4, n_pairs))] * 2,
        compiler_params=params(52, collective_id=2, has_side_effects=True),
        name="gather_and_project",
    )(w_bc, log_decay[0], layer_rows)

    per_head = (heads, 2, state_dim, head_dim)
    inner_states = (heads, max(count - 1, 1), state_dim, head_dim)
    grad_input, grad_bc = pl.pallas_call(
        functools.partial(states_kernel, count, heads, n_pairs),
        in_specs=[pl.BlockSpec(memory_space=pltpu.SMEM)] + [whole()] * 5,
        out_specs=[whole()] * 2,
        out_shape=[
            jax.ShapeDtypeStruct(x.shape, bf16),
            jax.ShapeDtypeStruct((length, 2 * state_dim), bf16),
        ],
        scratch_shapes=[
            pltpu.VMEM((state_dim, length), f32),
            pltpu.VMEM((state_dim, length), f32),
            pltpu.VMEM((count, BLOCK, BLOCK), f32),
            pltpu.VMEM((count, BLOCK, BLOCK), f32),
            pltpu.VMEM((length, state_dim), f32),
            pltpu.VMEM((length, state_dim), f32),
            pltpu.VMEM(inner_states, bf16),
            pltpu.VMEM(inner_states, bf16),
            pltpu.VMEM(per_head, bf16),
            pltpu.VMEM(per_head, bf16),
            pltpu.VMEM((2, heads, state_dim, head_dim), bf16),
            pltpu.VMEM((3,) + per_head, bf16),
            pltpu.SemaphoreType.DMA((heads,)),
            pltpu.SemaphoreType.DMA((heads,)),
            pltpu.SemaphoreType.DMA((2, heads)),
            pltpu.SemaphoreType.DMA((2, heads)),
        ],
        compiler_params=params(26, collective_id=0, has_side_effects=True),
        name="states_and_grads",
    )(skip_gain, x, dy, proj, running, decay)

    cols = 2 * state_dim
    n = n_seq * n_opt
    spots = n // 2
    group = max(2, 2 * LANES // own_rows)
    part, grad_input = pl.pallas_call(
        functools.partial(weight_kernel, group),
        in_specs=[whole()] * 3,
        out_specs=[whole(), in_hbm],
        out_shape=[
            jax.ShapeDtypeStruct((2, 2, n_pairs // 2, 2, 4, state_dim, own_rows), bf16),
            jax.ShapeDtypeStruct(x.shape, bf16),
        ],
        scratch_shapes=[
            pltpu.VMEM((cols, length), bf16),
            pltpu.SemaphoreType.DMA,
        ],
        compiler_params=params(28),
        name="weight_gradient",
    )(layer_rows, grad_bc, grad_input)

    block = (state_dim, own_rows)
    tall = jax.ShapeDtypeStruct((own_rows, cols), f32)
    code = jax.ShapeDtypeStruct((own_rows, cols), bf16)
    results = pl.pallas_call(
        functools.partial(step_kernel, n_seq, n_opt),
        in_specs=[whole()] * 6,
        out_specs=[whole()] * 3,
        out_shape=[tall, code, jax.ShapeDtypeStruct((8, cols), f32)],
        scratch_shapes=[
            pltpu.VMEM((2, n_pairs // 2, 2, 4) + block, bf16),
            pltpu.VMEM((2, 2, n_pairs) + block, bf16),
            pltpu.VMEM((2, 2, n_pairs) + block, f32),
            pltpu.VMEM((2, 2, n_pairs) + block, bf16),
            pltpu.VMEM((2, 2, n_pairs // 2) + block, bf16),
            pltpu.VMEM((2, 2, n_pairs // 2) + block, f32),
            pltpu.VMEM((2, 2, n_pairs // 2) + block, bf16),
            pltpu.VMEM((n_pairs, 2) + block, bf16),
            pltpu.VMEM((n_pairs, 2) + block, bf16),
            pltpu.VMEM((1, cols + LANES), f32),
            pltpu.VMEM((n, 1, cols + LANES), f32),
            pltpu.VMEM((1, cols), f32),
            pltpu.VMEM((n, 1, cols), f32),
        ]
        + dma(2)
        + [pltpu.SemaphoreType.DMA((2, 2))] * 4
        + dma(n_pairs, n, n),
        compiler_params=params(28, collective_id=1, has_side_effects=True),
        name="sum_and_step",
    )(part, w_bc, m_code, m_scale[None, :], row_stat[None, :], col_stat[None, :])
    update, code_next, scale_next, row_next, col_next = pl.pallas_call(
        hand_out,
        in_specs=[whole()] * 3,
        out_specs=[whole()] * 5,
        out_shape=[
            tall, code, jax.ShapeDtypeStruct((1, cols), f32),
            jax.ShapeDtypeStruct((1, own_rows), f32), jax.ShapeDtypeStruct((1, cols), f32),
        ],
        compiler_params=params(28),
        name="hand_out",
    )(*results)
    return (grad_input[None], update, code_next, scale_next[0], row_next[0], col_next[0])


def solution(mesh):
    return jax.shard_map(
        functools.partial(per_device, mesh.shape["seq"], mesh.shape["opt"]),
        mesh=mesh,
        in_specs=(
            P("opt", "seq", None),
            P("opt", "seq", None),
            P("opt", "seq", None),
            P("opt", None, "seq"),
            P(),
            P(("seq", "opt"), None),
            P(("seq", "opt"), None),
            P(),
            P(("seq", "opt")),
            P(),
        ),
        out_specs=(
            P("opt", "seq", None),
            P(("seq", "opt"), None),
            P(("seq", "opt"), None),
            P(),
            P(("seq", "opt")),
            P(),
        ),
        check_vma=False,
    )
```

```python
import functools

import jax
import jax.numpy as jnp
from jax import lax
from jax.experimental import pallas as pl
from jax.experimental.pallas import tpu as pltpu
from jax.sharding import PartitionSpec as P

BLOCK = 256
LANES = 128
LAG_SWAP = 3
LAG_CHAIN = 3

beta_one = 0.9
beta_two = 0.95
weight_decay = 0.1
clip_norm = 1.0
tiny_square = 1e-30
adam_floor = 1e-08
peak_floor = 1e-06
norm_floor = 1e-06
highest = lax.Precision.HIGHEST
MESH = pl.DeviceIdType.MESH
f32 = jnp.float32
bf16 = jnp.bfloat16


def dot_nn(a, b):
    return lax.dot_general(a, b, (((1,), (0,)), ((), ())), preferred_element_type=f32)


def dot_nt(a, b):
    return lax.dot_general(a, b, (((1,), (1,)), ((), ())), preferred_element_type=f32)


def dot_tn(a, b):
    return lax.dot_general(a, b, (((0,), (0,)), ((), ())), preferred_element_type=f32)


def as_column(row):
    return jnp.transpose(jnp.broadcast_to(row, (LANES, row.shape[1])))


def widened(column, length):
    return jnp.concatenate([column] * (length // LANES), axis=1)


def gather_kernel(
    count, n_seq, n_opt, w_ref, log_ref, layer_ref, proj_ref, run_ref, decay_ref,
    got, layer, total, decay, load, send_e, recv_e, send_a, recv_a, send_b, recv_b, send_c, recv_c, send_d, recv_d,
):
    seq = lax.axis_index("seq")
    opt = lax.axis_index("opt")
    n_pairs = n_seq // 2
    pair, side, cross, core, twins = place_of(seq, opt)
    core_twin, cross_twin, side_twin = twins
    half = w_ref.shape[0] // 2
    low, high = slice(0, half), slice(half, 2 * half)

    def same(part, send_sem, recv_sem, device):
        return remote(part, part, send_sem, recv_sem, device)

    def along(p, owner):
        block = got.at[owner, side, cross, core]
        other = (p * 2 + side, opt)
        return remote(block, block, send_a.at[p], recv_a.at[owner], other)

    def own_to(k, p, s, x):
        device = (cross_twin, side_twin)[k]
        return same(got.at[p, s, x, core], send_b.at[k, p], recv_b.at[k, p], device)

    def relay_to(k, p, s, x):
        device = (cross_twin, side_twin)[k]
        part = got.at[p, s, x, core, (low, high)[k]]
        return same(part, send_c.at[k, p], recv_c.at[k, p], device)

    def to_core(k, p, c):
        s = side if k % 2 == 0 else 1 - side
        x = cross if k // 2 == 0 else 1 - cross
        return same(got.at[p, s, x, c], send_d.at[k, p], recv_d.at[k, p], core_twin)

    def decay_copy():
        return remote(decay.at[0], decay.at[1], send_e, recv_e, side_twin)

    layer_copy = pltpu.make_async_copy(layer_ref, layer, load)
    layer_copy.start()
    greeted = greet_twins(n_pairs, seq, opt)
    got[pair, side, cross, core] = w_ref[...].astype(bf16)
    greeted()

    def send_along(distance, carry):
        along(pair_at(pair, n_pairs - distance, n_pairs), pair).start()
        return carry

    lax.fori_loop(1, n_pairs, send_along, 0)
    ones = (
        lax.broadcasted_iota(jnp.int32, (BLOCK, BLOCK), 0)
        <= lax.broadcasted_iota(jnp.int32, (BLOCK, BLOCK), 1)
    ).astype(f32)

    def turn(d, carry):
        @pl.when(d < n_pairs)
        def _():
            p = pair_at(pair, d, n_pairs)

            @pl.when(d > 0)
            def _():
                along(p, p).wait_recv()

            own_to(0, p, side, cross).start()
            own_to(1, p, side, cross).start()
            to_core(0, p, core).start()

        @pl.when(d == 0)
        def _():
            closing = None
            for b in range(count):
                sums = jnp.dot(
                    log_ref[:, b * BLOCK : (b + 1) * BLOCK], ones,
                    precision=highest, preferred_element_type=f32,
                )
                run_ref[:, b : b + 1, :] = sums[:, None, :]
                tail = sums[:, BLOCK - 1 :]
                closing = tail if closing is None else closing + tail
            decay[0] = jnp.broadcast_to(jnp.exp(closing), (closing.shape[0], LANES))[:, None, :]
            total[...] = jnp.zeros_like(total)

        @pl.when(d == 1)
        def _():
            decay_copy().start()

        @pl.when(jnp.logical_and(d >= 1, d < n_pairs + 1))
        def _():
            p = pair_at(pair, d - 1, n_pairs)
            own_to(0, p, side, 1 - cross).wait_recv()
            relay_to(1, p, side, 1 - cross).start()
            own_to(1, p, 1 - side, cross).wait_recv()
            relay_to(0, p, 1 - side, cross).start()
            to_core(1, p, core).start()
            to_core(2, p, core).start()

        @pl.when(jnp.logical_and(d >= 2, d < n_pairs + 2))
        def _():
            p = pair_at(pair, d - 2, n_pairs)
            relay_to(0, p, 1 - side, 1 - cross).wait_recv()
            relay_to(1, p, 1 - side, 1 - cross).wait_recv()
            to_core(3, p, core).start()

        @pl.when(d == 3)
        def _():
            layer_copy.wait()

        @pl.when(d >= 3)
        def _():
            p = pair_at(pair, d - 3, n_pairs)
            for k in range(4):
                to_core(k, p, 1 - core).wait_recv()
            w_part = got[p].reshape(-1, got.shape[-1])
            depth = w_part.shape[0]
            columns = pl.ds(pl.multiple_of(p * depth, depth), depth)
            total[...] += dot_nn(layer[:, columns], w_part)

        return carry

    lax.fori_loop(0, n_pairs + 3, turn, 0)
    proj_ref[...] = total[...].astype(bf16)
    decay_copy().wait()
    decay_ref[...] = decay[...]

    def sent(d, carry):
        p = lax.rem(pair + d, n_pairs)

        @pl.when(d > 0)
        def _():
            along(p, pair).wait_send()

        own_to(0, p, side, cross).wait_send()
        own_to(1, p, side, cross).wait_send()
        relay_to(0, p, 1 - side, cross).wait_send()
        relay_to(1, p, side, 1 - cross).wait_send()
        for k in range(4):
            to_core(k, p, core).wait_send()
        return carry

    lax.fori_loop(0, n_pairs, sent, 0)


def pair_at(pair, distance, n_pairs):
    step = jnp.where(2 * pair < n_pairs, distance, n_pairs - distance)
    return lax.rem(pair + step, n_pairs)


def place_of(seq, opt):
    side, core, cross = lax.rem(seq, 2), lax.rem(opt, 2), opt // 2
    twins = (
        (seq, opt + 1 - 2 * core), (seq, opt + 2 - 4 * cross), (seq + 1 - 2 * side, opt)
    )
    return seq // 2, side, cross, core, twins


def greet_twins(n_pairs, seq, opt):
    barrier = pltpu.get_barrier_semaphore()
    pair, side, cross, core, twins = place_of(seq, opt)

    def hello(device):
        pl.semaphore_signal(barrier, inc=1, device_id=device, device_id_type=MESH)

    def hello_pair(distance, carry):
        hello((lax.rem(pair + distance, n_pairs) * 2 + side, opt))
        return carry

    for device in twins:
        hello(device)
    lax.fori_loop(1, n_pairs, hello_pair, 0)
    return lambda: pl.semaphore_wait(barrier, n_pairs + 2)


def remote(src, dst, send_sem, recv_sem, device):
    return pltpu.make_async_remote_copy(
        src_ref=src, dst_ref=dst, send_sem=send_sem, recv_sem=recv_sem,
        device_id=device, device_id_type=MESH,
    )


def states_kernel(
    count, heads, n_pairs, skip_ref, x_hbm, dy_hbm, proj_ref, run_ref, decay_ref,
    gx_ref, gbc_ref,
    b_turned, c_turned, affinity, mixing, acc_b, acc_c, starts, outs, mine, got, chain_in, chain_out,
    x_ref, dy_ref, load, send_y, recv_y, send_c, recv_c,
):
    seq = lax.axis_index("seq")
    opt = lax.axis_index("opt")
    pair = seq // 2
    side = lax.rem(seq, 2)
    state_dim = proj_ref.shape[1] // 2
    head_dim = x_ref.shape[1] // heads
    b_cols, c_cols = slice(0, state_dim), slice(state_dim, 2 * state_dim)
    twin = (seq + 1 - 2 * side, opt)
    ahead = (seq + 2, opt)
    behind = (seq - 2, opt)
    has_source = (pair > 0, pair < n_pairs - 1)
    has_target = (pair < n_pairs - 1, pair > 0)
    places = (pair, n_pairs - 1 - pair)

    late = 5 * heads // 16
    early = heads // 4
    reach = LAG_CHAIN * (n_pairs - 1)
    wait = max(0, reach - heads + late)
    swap_lag = late + LAG_SWAP
    steps = max(heads - late + reach, heads + wait) + swap_lag

    def head_of(slot):
        return jnp.where(
            slot < early, slot, jnp.where(slot < heads - late, slot + late, slot - heads + late + early)
        )

    def lanes_of(h):
        return pl.ds(pl.multiple_of(h * head_dim, head_dim), head_dim)

    def closings_of(h):
        return [run_ref[h, b : b + 1, BLOCK - 1 : BLOCK] for b in range(count)]

    def swap(h):
        return remote(mine.at[h], got.at[h], send_y.at[h], recv_y.at[h], twin)

    def swap_late(h):
        return remote(chain_out.at[2, h], got.at[h], send_y.at[h], recv_y.at[h], twin)

    def pass_on(way, h):
        return remote(
            chain_out.at[way, h, 0], chain_in.at[way, h], send_c.at[way, h], recv_c.at[way, h],
            (ahead, behind)[way],
        )

    def hop(way, h, with_other):
        @pl.when(has_source[way])
        def _():
            pass_on(way, h).wait_recv()

        @pl.when(has_target[way])
        def _():
            own_decay = decay_ref[0, h]
            other_decay = decay_ref[1, h]
            first = side == way
            own_scale = jnp.where(first, other_decay, 1.0)
            total = (
                own_decay * other_decay * chain_in[way, h].astype(f32)
                + own_scale * mine[h, way].astype(f32)
            )
            if with_other:
                other_scale = jnp.where(first, 1.0, own_decay)
                total += other_scale * got[h, way].astype(f32)
            chain_out[way, h, 0] = total.astype(bf16)
            pass_on(way, h).start()

    def local(h):
        adds = []
        for b in range(count):
            rows = slice(b * BLOCK, (b + 1) * BLOCK)
            row = run_ref[h, b : b + 1, :]
            closing = row[:, BLOCK - 1 : BLOCK]
            b_scaled = (b_turned[:, rows] * jnp.exp(closing - row)).astype(bf16)
            c_scaled = (c_turned[:, rows] * jnp.exp(row)).astype(bf16)
            x_blk = x_ref[rows, lanes_of(h)]
            dy_blk = dy_ref[rows, lanes_of(h)]
            adds.append((jnp.exp(closing), dot_nn(b_scaled, x_blk), dot_nn(c_scaled, dy_blk)))
        state = adds[0][1]
        for b in range(1, count):
            starts[h, b - 1] = state.astype(bf16)
            state = adds[b][0] * state + adds[b][1]
        mine[h, 0] = state.astype(bf16)
        carried = adds[count - 1][2]
        for b in reversed(range(count - 1)):
            outs[h, b] = carried.astype(bf16)
            carried = adds[b][0] * carried + adds[b][2]
        mine[h, 1] = carried.astype(bf16)

    def finish(h, swapped_late):
        row_pos = lax.broadcasted_iota(jnp.int32, (BLOCK, BLOCK), 0)
        col_pos = lax.broadcasted_iota(jnp.int32, (BLOCK, BLOCK), 1)
        closings = closings_of(h)
        other_decay = decay_ref[1, h]
        fars = []
        for way in range(2):
            second = side != way
            scale = jnp.where(second, other_decay, 1.0)
            extra = jnp.where(jnp.logical_or(second, swapped_late), jnp.ones((1, LANES), f32), 0.0)
            fars.append(scale * chain_in[way, h].astype(f32) + extra * got[h, way].astype(f32))
        far_state, far_grad = fars
        for b in range(count):
            rows = slice(b * BLOCK, (b + 1) * BLOCK)
            row = run_ref[h, b : b + 1, :]
            column = as_column(row)
            before = sum(closings[:b], jnp.zeros((1, 1), f32))
            after = sum(closings[b + 1 :], jnp.zeros((1, 1), f32))
            if b == 0:
                state_in = far_state.astype(bf16)
            else:
                state_in = (starts[h, b - 1].astype(f32) + jnp.exp(before) * far_state).astype(bf16)
            if b == count - 1:
                grad_in = far_grad.astype(bf16)
            else:
                grad_in = (outs[h, b].astype(f32) + jnp.exp(after) * far_grad).astype(bf16)
            grow = jnp.exp(column)
            shrink = jnp.exp(closings[b] - column)
            x_blk = x_ref[rows, lanes_of(h)]
            dy_blk = dy_ref[rows, lanes_of(h)]
            spread = row - widened(column, BLOCK)
            decays = jnp.exp(jnp.where(col_pos >= row_pos, spread, -jnp.inf))
            mixing[b] += decays * dot_nt(x_blk, dy_blk)
            weighted = (decays * affinity[b]).astype(bf16)
            inner = dot_nn(weighted, dy_blk)
            outer = dot_nn(proj_ref[rows, b_cols], grad_in) * shrink
            full = inner + outer + skip_ref[h] * dy_blk.astype(f32)
            gx_ref[rows, lanes_of(h)] = full.astype(bf16)
            acc_c[rows, :] += grow * dot_nt(dy_blk, state_in)
            acc_b[rows, :] += shrink * dot_nt(x_blk, grad_in)

    pieces = load.shape[1]
    piece_heads = heads // pieces

    def bring(k):
        lanes = pl.ds(pl.multiple_of(k * piece_heads * head_dim, head_dim), piece_heads * head_dim)
        pairs = ((x_hbm, x_ref), (dy_hbm, dy_ref))
        return [
            pltpu.make_async_copy(source.at[:, lanes], held.at[:, lanes], load.at[n, k])
            for n, (source, held) in enumerate(pairs)
        ]

    for k in range(pieces):
        for copy in bring(k):
            copy.start()
    barrier = pltpu.get_barrier_semaphore()
    pl.semaphore_signal(barrier, inc=1, device_id=twin, device_id_type=MESH)
    for way in range(2):
        @pl.when(has_target[way])
        def _():
            pl.semaphore_signal(barrier, inc=1, device_id=(ahead, behind)[way], device_id_type=MESH)

    b_turned[...] = jnp.transpose(proj_ref[:, b_cols].astype(f32))
    c_turned[...] = jnp.transpose(proj_ref[:, c_cols].astype(f32))
    for way in range(2):
        @pl.when(jnp.logical_not(has_source[way]))
        def _():
            chain_in[way] = jnp.zeros_like(chain_in[way])
    neighbours = 1 + (pair > 0).astype(jnp.int32) + (pair < n_pairs - 1).astype(jnp.int32)
    pl.semaphore_wait(barrier, neighbours)

    def step(i, carry):
        is_late = jnp.logical_and(i >= early, i < early + late)

        @pl.when(jnp.logical_and(i < heads, lax.rem(i, piece_heads) == 0))
        def _():
            for copy in bring(i // piece_heads):
                copy.wait()

        @pl.when(i < heads)
        def _():
            local(i)

            @pl.when(jnp.logical_not(is_late))
            def _():
                swap(i).start()

        @pl.when(i == early)
        def _():
            mixing[...] = jnp.zeros_like(mixing)
            acc_b[...] = jnp.zeros_like(acc_b)
            acc_c[...] = jnp.zeros_like(acc_c)
            for b in range(count):
                rows = slice(b * BLOCK, (b + 1) * BLOCK)
                affinity[b] = dot_nt(proj_ref[rows, b_cols], proj_ref[rows, c_cols])

        for way in range(2):
            h = i - 1 - LAG_CHAIN * places[way]

            @pl.when(jnp.logical_and(h >= early, h < early + late))
            def _():
                hop(way, h, False)

        slot = i - late - wait

        @pl.when(jnp.logical_and(slot >= heads - late, slot < heads))
        def _():
            h = head_of(slot)
            own_decay = decay_ref[0, h]
            for way in range(2):
                first = side == way
                scale = jnp.where(first, own_decay, 1.0)
                extra = jnp.where(first, jnp.ones((1, LANES), f32), 0.0)
                total = scale * chain_in[way, h].astype(f32) + extra * mine[h, way].astype(f32)
                chain_out[2, h, way] = total.astype(bf16)
            swap_late(h).start()

        slot = i - swap_lag

        @pl.when(jnp.logical_and(slot >= 0, slot < heads - late))
        def _():
            swap(head_of(slot)).wait_recv()

        for way in range(2):
            slot = i - swap_lag - LAG_CHAIN * places[way]

            @pl.when(jnp.logical_and(slot >= 0, slot < heads - late))
            def _():
                hop(way, head_of(slot), True)

        slot = i - swap_lag - reach

        @pl.when(jnp.logical_and(slot >= 0, slot < heads - late))
        def _():
            finish(head_of(slot), False)

        slot = i - swap_lag - wait

        @pl.when(jnp.logical_and(slot >= heads - late, slot < heads))
        def _():
            h = head_of(slot)
            swap_late(h).wait_recv()
            finish(h, True)

        return carry

    lax.fori_loop(0, steps, step, 0)
    for b in range(count):
        rows = slice(b * BLOCK, (b + 1) * BLOCK)
        mixed = mixing[b].astype(bf16)
        gbc_ref[rows, b_cols] = (acc_b[rows, :] + dot_nn(mixed, proj_ref[rows, c_cols])).astype(bf16)
        gbc_ref[rows, c_cols] = (acc_c[rows, :] + dot_tn(mixed, proj_ref[rows, b_cols])).astype(bf16)

    def sent(h, carry):
        is_late = jnp.logical_and(h >= early, h < early + late)

        @pl.when(is_late)
        def _():
            swap_late(h).wait_send()

        @pl.when(jnp.logical_not(is_late))
        def _():
            swap(h).wait_send()

        for way in range(2):
            @pl.when(has_target[way])
            def _():
                pass_on(way, h).wait_send()

        return carry

    lax.fori_loop(0, heads, sent, 0)


def swap_all(n, me, src_of, dst_of, device_of, send_sem, recv_sem):
    def copy_to(distance):
        other = lax.rem(me + distance, n)
        return pltpu.make_async_remote_copy(
            src_ref=src_of(other), dst_ref=dst_of(me), send_sem=send_sem.at[other],
            recv_sem=recv_sem.at[me], device_id=device_of(other), device_id_type=MESH,
        )

    def copy_from(distance):
        other = lax.rem(me + distance, n)
        return pltpu.make_async_remote_copy(
            src_ref=src_of(other), dst_ref=dst_of(other), send_sem=send_sem.at[other],
            recv_sem=recv_sem.at[other], device_id=device_of(other), device_id_type=MESH,
        )

    def start(distance, carry):
        copy_to(distance).start()
        return carry

    def finish(distance, carry):
        copy = copy_from(distance)
        copy.wait_send()
        copy.wait_recv()
        return carry

    return lambda: lax.fori_loop(1, n, start, 0), lambda: lax.fori_loop(1, n, finish, 0)


def begin_swap(*args):
    start, finish = swap_all(*args)
    start()
    return finish


def step_kernel(
    n_seq, n_opt, layer_ref, grad_ref, w_ref, code_ref, scale_ref, row_ref, col_ref,
    update_ref, code_out, small_out,
    grad_turned, part_ref, take_core, give_two, keep_two, take_two, give_three, keep_three, take_three, give_pair, take_pair,
    stats, all_stats, peak, all_peaks,
    send_core, recv_core, send_two, recv_two, send_three, recv_three, send_pair, recv_pair,
    send_c, recv_c, send_d, recv_d,
):
    seq = lax.axis_index("seq")
    opt = lax.axis_index("opt")
    n = n_seq * n_opt
    n_pairs = n_seq // 2
    me = seq * n_opt + opt
    pair, side, cross, core, twins = place_of(seq, opt)
    core_twin, cross_twin, side_twin = twins

    def any_device(i):
        return (i // n_opt, lax.rem(i, n_opt))

    greeted = greet_twins(n_pairs, seq, opt)
    targets = ((cross_twin, side_twin), (side_twin, cross_twin))
    own = ((cross, side), (side, cross))
    order = [pair_at(pair, n_pairs - 1 - d, n_pairs) for d in range(n_pairs)]

    def first(p):
        return remote(
            part_ref.at[1 - core, :, p], take_core.at[:, p], send_core.at[p], recv_core.at[p],
            core_twin,
        )

    def second(k, p):
        return remote(
            give_two.at[k, p], take_two.at[k, p], send_two.at[k, p], recv_two.at[k, p],
            targets[0][k],
        )

    def third(k, p):
        return remote(
            give_three.at[k, p], take_three.at[k, p], send_three.at[k, p], recv_three.at[k, p],
            targets[1][k],
        )

    def chip_sum(k, p, a, b):
        r = a * 2 + b if k == 0 else b * 2 + a
        return part_ref[core, k, p, r].astype(f32) + take_core[k, p, r].astype(f32)

    def slice_sum(k, p):
        return keep_three[k, p] + take_three[k, p].astype(f32)

    def to_pair(p, source):
        return remote(
            give_pair.at[p], take_pair.at[source], send_pair.at[p], recv_pair.at[source],
            (p * 2 + side, opt),
        )

    grad_turned[...] = jnp.transpose(grad_ref[...].astype(f32)).astype(bf16)
    _, _, _, n_r, half, own_rows = part_ref.shape
    reach = 2 * n_r * own_rows

    def fill_part(p):
        columns = pl.ds(pl.multiple_of(p * reach, reach), reach)
        both = dot_nn(grad_turned[...], layer_ref[:, columns]).astype(bf16)
        for t in range(n_r):
            for c in range(2):
                lanes = slice((2 * t + c) * own_rows, (2 * t + c + 1) * own_rows)
                for k in range(2):
                    part_ref[c, k, p, t] = both[k * half : (k + 1) * half, lanes]

    for n_done, p in enumerate(order):
        fill_part(p)
        if n_done == 0:
            greeted()
        first(p).start()
    for p in order:
        first(p).wait()
        for k in range(2):
            for a in range(2):
                give_two[k, p, a] = chip_sum(k, p, a, 1 - own[0][k]).astype(bf16)
            second(k, p).start()
    for p in order:
        for k in range(2):
            for a in range(2):
                keep_two[k, p, a] = chip_sum(k, p, a, own[0][k])

    def finish_third(p):
        for k in range(2):
            third(k, p).wait()

        if p is not order[-1]:
            for k in range(2):
                give_pair[p, k] = slice_sum(k, p).astype(bf16)
            to_pair(p, pair).start()

    for n_done, p in enumerate(order):
        for k in range(2):
            second(k, p).wait()
            a = 1 - own[1][k]
            total = keep_two[k, p, a] + take_two[k, p, a].astype(f32)
            give_three[k, p] = total.astype(bf16)
            third(k, p).start()
            a = own[1][k]
            keep_three[k, p] = keep_two[k, p, a] + take_two[k, p, a].astype(f32)
        if n_done > 0:
            finish_third(order[n_done - 1])
    finish_third(order[-1])
    take_pair[pair] = jnp.zeros_like(take_pair[pair])
    totals = [slice_sum(k, pair) for k in range(2)]
    turned = jnp.concatenate(totals, axis=0)

    def end_slices(distance, carry):
        p = lax.rem(pair + distance, n_pairs)
        to_pair(p, p).wait()
        return carry

    lax.fori_loop(1, n_pairs, end_slices, 0)

    def gather_pair(p, total):
        return total + jnp.concatenate([take_pair[p, k].astype(f32) for k in range(2)], axis=0)

    turned = lax.fori_loop(0, n_pairs, gather_pair, turned)
    grad = jnp.transpose(turned)

    rows, cols = grad.shape
    width = n * rows
    stats[:, :cols] = jnp.sum(grad * grad, axis=0, keepdims=True)
    row_stat = row_ref[...]
    stats[:, cols:] = jnp.broadcast_to(jnp.sum(row_stat, axis=1, keepdims=True), (1, LANES))
    end_stats = begin_swap(
        n, me, lambda i: stats, lambda i: all_stats.at[i], any_device, send_c, recv_c
    )
    row_raw = jnp.sum(turned * turned, axis=0, keepdims=True)
    old_moment = beta_one * code_ref[...].astype(f32) * scale_ref[...]
    end_stats()
    all_stats[me] = stats[...]
    sums = all_stats[0]
    for i in range(1, n):
        sums += all_stats[i]
    col_raw = sums[:, :cols]
    old_total = sums[:, cols : cols + 1]
    raw_total = jnp.sum(col_raw, axis=1, keepdims=True)
    factor = jnp.minimum(1.0, clip_norm / jnp.sqrt(raw_total + norm_floor))
    moment = old_moment + (1.0 - beta_one) * (grad * factor)
    peak[...] = jnp.max(jnp.abs(moment), axis=0, keepdims=True)
    end_peaks = begin_swap(
        n, me, lambda i: peak, lambda i: all_peaks.at[i], any_device, send_d, recv_d
    )
    col_next = beta_two * col_ref[...] + (1.0 - beta_two) * (
        factor * factor * col_raw / width + tiny_square
    )
    row_next = beta_two * row_stat + (1.0 - beta_two) * (
        factor * factor * row_raw / cols + tiny_square
    )
    row_mean = (
        beta_two * old_total
        + (1.0 - beta_two) * (factor * factor * raw_total / cols + width * tiny_square)
    ) / width
    small_out[1:2, :] = col_next
    small_out[2:3, :rows] = row_next
    row_column = jnp.transpose(jnp.broadcast_to(row_next / row_mean, (8, rows)))[:, :1]
    second_moment = row_column * col_next
    update_ref[...] = moment / (jnp.sqrt(second_moment) + adam_floor) + weight_decay * w_ref[...]
    end_peaks()
    all_peaks[me] = peak[...]
    scale_next = all_peaks[0]
    for i in range(1, n):
        scale_next = jnp.maximum(scale_next, all_peaks[i])
    scale_next = scale_next + peak_floor
    small_out[0:1, :] = scale_next
    code_out[...] = (moment / scale_next).astype(bf16)


def hand_out(
    gx_ref, update_ref, code_ref, small_ref,
    gx_out, update_out, code_out, scale_out, row_out, col_out, store,
):
    put = pltpu.make_async_copy(gx_ref, gx_out, store)
    put.start()
    update_out[...] = update_ref[...]
    code_out[...] = code_ref[...]
    scale_out[...] = small_ref[0:1, :]
    col_out[...] = small_ref[1:2, :]
    row_out[...] = small_ref[2:3, : row_out.shape[1]]
    put.wait()


def params(mebibytes, **more):
    return pltpu.CompilerParams(vmem_limit_bytes=mebibytes * 1024 * 1024, **more)


def whole():
    return pl.BlockSpec(memory_space=pltpu.VMEM)


def dma(*counts):
    return [pltpu.SemaphoreType.DMA((count,)) for count in counts for _ in range(2)]


def per_device(
    n_seq, n_opt, layer_in, ssm_input, grad_out, log_decay, skip_gain, w_bc, m_code, m_scale,
    row_stat, col_stat,
):
    layer_rows = layer_in[0]
    x = ssm_input[0]
    dy = grad_out[0]
    length, width = layer_rows.shape
    heads = skip_gain.shape[0]
    head_dim = x.shape[1] // heads
    state_dim = w_bc.shape[1] // 2
    count = length // BLOCK
    n_pairs = n_seq // 2
    own_rows = w_bc.shape[0]

    in_hbm = pl.BlockSpec(memory_space=pltpu.MemorySpace.HBM)
    proj, running, decay = pl.pallas_call(
        functools.partial(gather_kernel, count, n_seq, n_opt),
        in_specs=[whole(), whole(), in_hbm],
        out_specs=[whole()] * 3,
        out_shape=[
            jax.ShapeDtypeStruct((length, 2 * state_dim), bf16),
            jax.ShapeDtypeStruct((heads, count, BLOCK), f32),
            jax.ShapeDtypeStruct((2, heads, 1, LANES), f32),
        ],
        scratch_shapes=[
            pltpu.VMEM((n_pairs, 2, 2, 2, own_rows, 2 * state_dim), bf16),
            pltpu.VMEM((length, width), bf16),
            pltpu.VMEM((length, 2 * state_dim), f32),
            pltpu.VMEM((2, heads, 1, LANES), f32),
            pltpu.SemaphoreType.DMA,
            pltpu.SemaphoreType.DMA,
            pltpu.SemaphoreType.DMA,
        ]
        + [pltpu.SemaphoreType.DMA((n_pairs,))] * 2
        + [pltpu.SemaphoreType.DMA((2, n_pairs))] * 4
        + [pltpu.SemaphoreType.DMA((4, n_pairs))] * 2,
        compiler_params=params(52, collective_id=2, has_side_effects=True),
        name="gather_and_project",
    )(w_bc, log_decay[0], layer_rows)

    per_head = (heads, 2, state_dim, head_dim)
    inner_states = (heads, max(count - 1, 1), state_dim, head_dim)
    grad_input, grad_bc = pl.pallas_call(
        functools.partial(states_kernel, count, heads, n_pairs),
        in_specs=[pl.BlockSpec(memory_space=pltpu.SMEM), in_hbm, in_hbm] + [whole()] * 3,
        out_specs=[whole()] * 2,
        out_shape=[
            jax.ShapeDtypeStruct(x.shape, bf16),
            jax.ShapeDtypeStruct((length, 2 * state_dim), bf16),
        ],
        scratch_shapes=[
            pltpu.VMEM((state_dim, length), f32),
            pltpu.VMEM((state_dim, length), f32),
            pltpu.VMEM((count, BLOCK, BLOCK), f32),
            pltpu.VMEM((count, BLOCK, BLOCK), f32),
            pltpu.VMEM((length, state_dim), f32),
            pltpu.VMEM((length, state_dim), f32),
            pltpu.VMEM(inner_states, bf16),
            pltpu.VMEM(inner_states, bf16),
            pltpu.VMEM(per_head, bf16),
            pltpu.VMEM(per_head, bf16),
            pltpu.VMEM((2, heads, state_dim, head_dim), bf16),
            pltpu.VMEM((3,) + per_head, bf16),
            pltpu.VMEM(x.shape, bf16),
            pltpu.VMEM(x.shape, bf16),
            pltpu.SemaphoreType.DMA((2, 8)),
            pltpu.SemaphoreType.DMA((heads,)),
            pltpu.SemaphoreType.DMA((heads,)),
            pltpu.SemaphoreType.DMA((2, heads)),
            pltpu.SemaphoreType.DMA((2, heads)),
        ],
        compiler_params=params(46, collective_id=0, has_side_effects=True),
        name="states_and_grads",
    )(skip_gain, x, dy, proj, running, decay)

    cols = 2 * state_dim
    n = n_seq * n_opt
    block = (state_dim, own_rows)
    tall = jax.ShapeDtypeStruct((own_rows, cols), f32)
    code = jax.ShapeDtypeStruct((own_rows, cols), bf16)
    results = pl.pallas_call(
        functools.partial(step_kernel, n_seq, n_opt),
        in_specs=[whole()] * 7,
        out_specs=[whole()] * 3,
        out_shape=[tall, code, jax.ShapeDtypeStruct((8, cols), f32)],
        scratch_shapes=[
            pltpu.VMEM((cols, length), bf16),
            pltpu.VMEM((2, 2, n_pairs, 4) + block, bf16),
            pltpu.VMEM((2, n_pairs, 4) + block, bf16),
            pltpu.VMEM((2, n_pairs, 2) + block, bf16),
            pltpu.VMEM((2, n_pairs, 2) + block, f32),
            pltpu.VMEM((2, n_pairs, 2) + block, bf16),
            pltpu.VMEM((2, n_pairs) + block, bf16),
            pltpu.VMEM((2, n_pairs) + block, f32),
            pltpu.VMEM((2, n_pairs) + block, bf16),
            pltpu.VMEM((n_pairs, 2) + block, bf16),
            pltpu.VMEM((n_pairs, 2) + block, bf16),
            pltpu.VMEM((1, cols + LANES), f32),
            pltpu.VMEM((n, 1, cols + LANES), f32),
            pltpu.VMEM((1, cols), f32),
            pltpu.VMEM((n, 1, cols), f32),
        ]
        + dma(n_pairs)
        + [pltpu.SemaphoreType.DMA((2, n_pairs))] * 4
        + dma(n_pairs, n, n),
        compiler_params=params(40, collective_id=1, has_side_effects=True),
        name="sum_and_step",
    )(layer_rows, grad_bc, w_bc, m_code, m_scale[None, :], row_stat[None, :], col_stat[None, :])
    grad_input, update, code_next, scale_next, row_next, col_next = pl.pallas_call(
        hand_out,
        in_specs=[whole()] * 4,
        out_specs=[in_hbm] + [whole()] * 5,
        out_shape=[
            jax.ShapeDtypeStruct(x.shape, bf16), tall, code, jax.ShapeDtypeStruct((1, cols), f32),
            jax.ShapeDtypeStruct((1, own_rows), f32), jax.ShapeDtypeStruct((1, cols), f32),
        ],
        scratch_shapes=[pltpu.SemaphoreType.DMA],
        compiler_params=params(28),
        name="hand_out",
    )(grad_input, *results)
    return (grad_input[None], update, code_next, scale_next[0], row_next[0], col_next[0])


def solution(mesh):
    return jax.shard_map(
        functools.partial(per_device, mesh.shape["seq"], mesh.shape["opt"]),
        mesh=mesh,
        in_specs=(
            P("opt", "seq", None),
            P("opt", "seq", None),
            P("opt", "seq", None),
            P("opt", None, "seq"),
            P(),
            P(("seq", "opt"), None),
            P(("seq", "opt"), None),
            P(),
            P(("seq", "opt")),
            P(),
        ),
        out_specs=(
            P("opt", "seq", None),
            P(("seq", "opt"), None),
            P(("seq", "opt"), None),
            P(),
            P(("seq", "opt")),
            P(),
        ),
        check_vma=False,
    )
```

```python
import functools

import jax
import jax.numpy as jnp
from jax import lax
from jax.experimental import pallas as pl
from jax.experimental.pallas import tpu as pltpu
from jax.sharding import PartitionSpec as P

BLOCK = 256
LANES = 128
LAG_SWAP = 3
LAG_CHAIN = 3
GATHER_SCRATCH = 14

beta_one = 0.9
beta_two = 0.95
weight_decay = 0.1
clip_norm = 1.0
tiny_square = 1e-30
adam_floor = 1e-08
peak_floor = 1e-06
norm_floor = 1e-06
highest = lax.Precision.HIGHEST
MESH = pl.DeviceIdType.MESH
f32 = jnp.float32
bf16 = jnp.bfloat16


def dot_nn(a, b):
    return lax.dot_general(a, b, (((1,), (0,)), ((), ())), preferred_element_type=f32)


def dot_nt(a, b):
    return lax.dot_general(a, b, (((1,), (1,)), ((), ())), preferred_element_type=f32)


def dot_tn(a, b):
    return lax.dot_general(a, b, (((0,), (0,)), ((), ())), preferred_element_type=f32)


def as_column(row):
    return jnp.transpose(jnp.broadcast_to(row, (LANES, row.shape[1])))


def widened(column, length):
    return jnp.concatenate([column] * (length // LANES), axis=1)


def gather_part(
    count, n_seq, n_opt, bring_all, w_ref, log_ref, layer_ref, proj_ref, run_ref, decay,
    got, layer, total, load, send_e, recv_e, send_a, recv_a, send_b, recv_b, send_c, recv_c, send_d, recv_d,
):
    seq = lax.axis_index("seq")
    opt = lax.axis_index("opt")
    n_pairs = n_seq // 2
    pair, side, cross, core, twins = place_of(seq, opt)
    core_twin, cross_twin, side_twin = twins
    half = w_ref.shape[0] // 2
    low, high = slice(0, half), slice(half, 2 * half)

    def same(part, send_sem, recv_sem, device):
        return remote(part, part, send_sem, recv_sem, device)

    def along(p, owner):
        block = got.at[owner, side, cross, core]
        other = (p * 2 + side, opt)
        return remote(block, block, send_a.at[p], recv_a.at[owner], other)

    def own_to(k, p, s, x):
        device = (cross_twin, side_twin)[k]
        return same(got.at[p, s, x, core], send_b.at[k, p], recv_b.at[k, p], device)

    def relay_to(k, p, s, x):
        device = (cross_twin, side_twin)[k]
        part = got.at[p, s, x, core, (low, high)[k]]
        return same(part, send_c.at[k, p], recv_c.at[k, p], device)

    def to_core(k, p, c):
        s = side if k % 2 == 0 else 1 - side
        x = cross if k // 2 == 0 else 1 - cross
        return same(got.at[p, s, x, c], send_d.at[k, p], recv_d.at[k, p], core_twin)

    def decay_copy():
        return remote(decay.at[0], decay.at[1], send_e, recv_e, side_twin)

    layer_copy = pltpu.make_async_copy(layer_ref, layer, load)
    layer_copy.start()
    greeted = greet_twins(n_pairs, seq, opt)
    got[pair, side, cross, core] = w_ref[...].astype(bf16)
    greeted()

    def send_along(distance, carry):
        along(pair_at(pair, n_pairs - distance, n_pairs), pair).start()
        return carry

    lax.fori_loop(1, n_pairs, send_along, 0)
    bring_all()
    ones = (
        lax.broadcasted_iota(jnp.int32, (BLOCK, BLOCK), 0)
        <= lax.broadcasted_iota(jnp.int32, (BLOCK, BLOCK), 1)
    ).astype(f32)

    def turn(d, carry):
        @pl.when(d < n_pairs)
        def _():
            p = pair_at(pair, d, n_pairs)

            @pl.when(d > 0)
            def _():
                along(p, p).wait_recv()

            own_to(0, p, side, cross).start()
            own_to(1, p, side, cross).start()
            to_core(0, p, core).start()

        @pl.when(d == 0)
        def _():
            closing = None
            for b in range(count):
                sums = jnp.dot(
                    log_ref[:, b * BLOCK : (b + 1) * BLOCK], ones,
                    precision=highest, preferred_element_type=f32,
                )
                run_ref[:, b : b + 1, :] = sums[:, None, :]
                tail = sums[:, BLOCK - 1 :]
                closing = tail if closing is None else closing + tail
            decay[0] = jnp.broadcast_to(jnp.exp(closing), (closing.shape[0], LANES))[:, None, :]
            total[...] = jnp.zeros_like(total)

        @pl.when(d == 1)
        def _():
            decay_copy().start()

        @pl.when(jnp.logical_and(d >= 1, d < n_pairs + 1))
        def _():
            p = pair_at(pair, d - 1, n_pairs)
            own_to(0, p, side, 1 - cross).wait_recv()
            relay_to(1, p, side, 1 - cross).start()
            own_to(1, p, 1 - side, cross).wait_recv()
            relay_to(0, p, 1 - side, cross).start()
            to_core(1, p, core).start()
            to_core(2, p, core).start()

        @pl.when(jnp.logical_and(d >= 2, d < n_pairs + 2))
        def _():
            p = pair_at(pair, d - 2, n_pairs)
            relay_to(0, p, 1 - side, 1 - cross).wait_recv()
            relay_to(1, p, 1 - side, 1 - cross).wait_recv()
            to_core(3, p, core).start()

        @pl.when(d == 3)
        def _():
            layer_copy.wait()

        @pl.when(d >= 3)
        def _():
            p = pair_at(pair, d - 3, n_pairs)
            for k in range(4):
                to_core(k, p, 1 - core).wait_recv()
            w_part = got[p].reshape(-1, got.shape[-1])
            depth = w_part.shape[0]
            columns = pl.ds(pl.multiple_of(p * depth, depth), depth)
            total[...] += dot_nn(layer[:, columns], w_part)

        return carry

    lax.fori_loop(0, n_pairs + 3, turn, 0)
    proj_ref[...] = total[...].astype(bf16)
    decay_copy().wait()

    def sent(d, carry):
        p = lax.rem(pair + d, n_pairs)

        @pl.when(d > 0)
        def _():
            along(p, pair).wait_send()

        own_to(0, p, side, cross).wait_send()
        own_to(1, p, side, cross).wait_send()
        relay_to(0, p, 1 - side, cross).wait_send()
        relay_to(1, p, side, 1 - cross).wait_send()
        for k in range(4):
            to_core(k, p, core).wait_send()
        return carry

    return lambda: lax.fori_loop(0, n_pairs, sent, 0)


def pair_at(pair, distance, n_pairs):
    step = jnp.where(2 * pair < n_pairs, distance, n_pairs - distance)
    return lax.rem(pair + step, n_pairs)


def place_of(seq, opt):
    side, core, cross = lax.rem(seq, 2), lax.rem(opt, 2), opt // 2
    twins = (
        (seq, opt + 1 - 2 * core), (seq, opt + 2 - 4 * cross), (seq + 1 - 2 * side, opt)
    )
    return seq // 2, side, cross, core, twins


def greet_twins(n_pairs, seq, opt):
    barrier = pltpu.get_barrier_semaphore()
    pair, side, cross, core, twins = place_of(seq, opt)

    def hello(device):
        pl.semaphore_signal(barrier, inc=1, device_id=device, device_id_type=MESH)

    def hello_pair(distance, carry):
        hello((lax.rem(pair + distance, n_pairs) * 2 + side, opt))
        return carry

    for device in twins:
        hello(device)
    lax.fori_loop(1, n_pairs, hello_pair, 0)
    return lambda: pl.semaphore_wait(barrier, n_pairs + 2)


def remote(src, dst, send_sem, recv_sem, device):
    return pltpu.make_async_remote_copy(
        src_ref=src, dst_ref=dst, send_sem=send_sem, recv_sem=recv_sem,
        device_id=device, device_id_type=MESH,
    )


def states_part(
    count, heads, n_pairs, bring, skip_ref, proj_ref, run_ref, decay_ref, gx_ref, gbc_ref,
    b_turned, c_turned, affinity, mixing, acc_b, acc_c, starts, outs, mine, got, chain_in, chain_out,
    x_ref, dy_ref, load, send_y, recv_y, send_c, recv_c,
):
    seq = lax.axis_index("seq")
    opt = lax.axis_index("opt")
    pair = seq // 2
    side = lax.rem(seq, 2)
    state_dim = proj_ref.shape[1] // 2
    head_dim = x_ref.shape[1] // heads
    b_cols, c_cols = slice(0, state_dim), slice(state_dim, 2 * state_dim)
    twin = (seq + 1 - 2 * side, opt)
    ahead = (seq + 2, opt)
    behind = (seq - 2, opt)
    has_source = (pair > 0, pair < n_pairs - 1)
    has_target = (pair < n_pairs - 1, pair > 0)
    places = (pair, n_pairs - 1 - pair)

    late = 5 * heads // 16
    early = 5 * heads // 16
    reach = LAG_CHAIN * (n_pairs - 1)
    wait = max(0, reach - heads + late)
    swap_lag = late + LAG_SWAP
    steps = max(heads - late + reach, heads + wait) + swap_lag

    def head_of(slot):
        return jnp.where(
            slot < early, slot, jnp.where(slot < heads - late, slot + late, slot - heads + late + early)
        )

    def lanes_of(h):
        return pl.ds(pl.multiple_of(h * head_dim, head_dim), head_dim)

    def closings_of(h):
        return [run_ref[h, b : b + 1, BLOCK - 1 : BLOCK] for b in range(count)]

    def swap(h):
        return remote(mine.at[h], got.at[h], send_y.at[h], recv_y.at[h], twin)

    def swap_late(h):
        return remote(chain_out.at[2, h], got.at[h], send_y.at[h], recv_y.at[h], twin)

    def pass_on(way, h):
        return remote(
            chain_out.at[way, h, 0], chain_in.at[way, h], send_c.at[way, h], recv_c.at[way, h],
            (ahead, behind)[way],
        )

    def hop(way, h, with_other):
        @pl.when(has_source[way])
        def _():
            pass_on(way, h).wait_recv()

        @pl.when(has_target[way])
        def _():
            own_decay = decay_ref[0, h]
            other_decay = decay_ref[1, h]
            first = side == way
            own_scale = jnp.where(first, other_decay, 1.0)
            total = (
                own_decay * other_decay * chain_in[way, h].astype(f32)
                + own_scale * mine[h, way].astype(f32)
            )
            if with_other:
                other_scale = jnp.where(first, 1.0, own_decay)
                total += other_scale * got[h, way].astype(f32)
            chain_out[way, h, 0] = total.astype(bf16)
            pass_on(way, h).start()

    def end_hops(h):
        for way in range(2):
            @pl.when(has_target[way])
            def _():
                pass_on(way, h).wait_send()

    def local(h):
        adds = []
        for b in range(count):
            rows = slice(b * BLOCK, (b + 1) * BLOCK)
            row = run_ref[h, b : b + 1, :]
            closing = row[:, BLOCK - 1 : BLOCK]
            b_scaled = (b_turned[:, rows] * jnp.exp(closing - row)).astype(bf16)
            c_scaled = (c_turned[:, rows] * jnp.exp(row)).astype(bf16)
            x_blk = x_ref[rows, lanes_of(h)]
            dy_blk = dy_ref[rows, lanes_of(h)]
            adds.append((jnp.exp(closing), dot_nn(b_scaled, x_blk), dot_nn(c_scaled, dy_blk)))
        state = adds[0][1]
        for b in range(1, count):
            starts[h, b - 1] = state.astype(bf16)
            state = adds[b][0] * state + adds[b][1]
        mine[h, 0] = state.astype(bf16)
        carried = adds[count - 1][2]
        for b in reversed(range(count - 1)):
            outs[h, b] = carried.astype(bf16)
            carried = adds[b][0] * carried + adds[b][2]
        mine[h, 1] = carried.astype(bf16)

    def finish(h, swapped_late):
        row_pos = lax.broadcasted_iota(jnp.int32, (BLOCK, BLOCK), 0)
        col_pos = lax.broadcasted_iota(jnp.int32, (BLOCK, BLOCK), 1)
        closings = closings_of(h)
        other_decay = decay_ref[1, h]
        fars = []
        for way in range(2):
            second = side != way
            scale = jnp.where(second, other_decay, 1.0)
            extra = jnp.where(jnp.logical_or(second, swapped_late), jnp.ones((1, LANES), f32), 0.0)
            fars.append(scale * chain_in[way, h].astype(f32) + extra * got[h, way].astype(f32))
        far_state, far_grad = fars
        for b in range(count):
            rows = slice(b * BLOCK, (b + 1) * BLOCK)
            row = run_ref[h, b : b + 1, :]
            column = as_column(row)
            before = sum(closings[:b], jnp.zeros((1, 1), f32))
            after = sum(closings[b + 1 :], jnp.zeros((1, 1), f32))
            if b == 0:
                state_in = far_state.astype(bf16)
            else:
                state_in = (starts[h, b - 1].astype(f32) + jnp.exp(before) * far_state).astype(bf16)
            if b == count - 1:
                grad_in = far_grad.astype(bf16)
            else:
                grad_in = (outs[h, b].astype(f32) + jnp.exp(after) * far_grad).astype(bf16)
            grow = jnp.exp(column)
            shrink = jnp.exp(closings[b] - column)
            x_blk = x_ref[rows, lanes_of(h)]
            dy_blk = dy_ref[rows, lanes_of(h)]
            spread = row - widened(column, BLOCK)
            decays = jnp.exp(jnp.where(col_pos >= row_pos, spread, -jnp.inf))
            mixing[b] += decays * dot_nt(x_blk, dy_blk)
            weighted = (decays * affinity[b]).astype(bf16)
            inner = dot_nn(weighted, dy_blk)
            outer = dot_nn(proj_ref[rows, b_cols], grad_in) * shrink
            full = inner + outer + skip_ref[h] * dy_blk.astype(f32)
            gx_ref[rows, lanes_of(h)] = full.astype(bf16)
            acc_c[rows, :] += grow * dot_nt(dy_blk, state_in)
            acc_b[rows, :] += shrink * dot_nt(x_blk, grad_in)

    piece_heads = heads // load.shape[1]

    b_turned[...] = jnp.transpose(proj_ref[:, b_cols].astype(f32))
    c_turned[...] = jnp.transpose(proj_ref[:, c_cols].astype(f32))
    def step(i, carry):
        is_late = jnp.logical_and(i >= early, i < early + late)

        @pl.when(jnp.logical_and(i < heads, lax.rem(i, piece_heads) == 0))
        def _():
            for copy in bring(i // piece_heads):
                copy.wait()

        @pl.when(i < heads)
        def _():
            local(i)

            @pl.when(jnp.logical_not(is_late))
            def _():
                swap(i).start()

        @pl.when(i == early)
        def _():
            mixing[...] = jnp.zeros_like(mixing)
            acc_b[...] = jnp.zeros_like(acc_b)
            acc_c[...] = jnp.zeros_like(acc_c)
            for b in range(count):
                rows = slice(b * BLOCK, (b + 1) * BLOCK)
                affinity[b] = dot_nt(proj_ref[rows, b_cols], proj_ref[rows, c_cols])

        for way in range(2):
            h = i - 1 - LAG_CHAIN * places[way]

            @pl.when(jnp.logical_and(h >= early, h < early + late))
            def _():
                hop(way, h, False)

        slot = i - late - wait

        @pl.when(jnp.logical_and(slot >= heads - late, slot < heads))
        def _():
            h = head_of(slot)
            own_decay = decay_ref[0, h]
            for way in range(2):
                first = side == way
                scale = jnp.where(first, own_decay, 1.0)
                extra = jnp.where(first, jnp.ones((1, LANES), f32), 0.0)
                total = scale * chain_in[way, h].astype(f32) + extra * mine[h, way].astype(f32)
                chain_out[2, h, way] = total.astype(bf16)
            swap_late(h).start()

        slot = i - swap_lag

        @pl.when(jnp.logical_and(slot >= 0, slot < heads - late))
        def _():
            swap(head_of(slot)).wait()

        for way in range(2):
            slot = i - swap_lag - LAG_CHAIN * places[way]

            @pl.when(jnp.logical_and(slot >= 0, slot < heads - late))
            def _():
                hop(way, head_of(slot), True)

        slot = i - swap_lag - reach

        @pl.when(jnp.logical_and(slot >= 0, slot < heads - late))
        def _():
            finish(head_of(slot), False)
            end_hops(head_of(slot))

        slot = i - swap_lag - wait

        @pl.when(jnp.logical_and(slot >= heads - late, slot < heads))
        def _():
            h = head_of(slot)
            swap_late(h).wait()
            finish(h, True)
            end_hops(h)

        return carry

    lax.fori_loop(0, steps, step, 0)
    for b in range(count):
        rows = slice(b * BLOCK, (b + 1) * BLOCK)
        mixed = mixing[b].astype(bf16)
        gbc_ref[rows, b_cols] = (acc_b[rows, :] + dot_nn(mixed, proj_ref[rows, c_cols])).astype(bf16)
        gbc_ref[rows, c_cols] = (acc_c[rows, :] + dot_tn(mixed, proj_ref[rows, b_cols])).astype(bf16)


def swap_all(n, me, src_of, dst_of, device_of, send_sem, recv_sem):
    def copy_to(distance):
        other = lax.rem(me + distance, n)
        return pltpu.make_async_remote_copy(
            src_ref=src_of(other), dst_ref=dst_of(me), send_sem=send_sem.at[other],
            recv_sem=recv_sem.at[me], device_id=device_of(other), device_id_type=MESH,
        )

    def copy_from(distance):
        other = lax.rem(me + distance, n)
        return pltpu.make_async_remote_copy(
            src_ref=src_of(other), dst_ref=dst_of(other), send_sem=send_sem.at[other],
            recv_sem=recv_sem.at[other], device_id=device_of(other), device_id_type=MESH,
        )

    def start(distance, carry):
        copy_to(distance).start()
        return carry

    def finish(distance, carry):
        copy = copy_from(distance)
        copy.wait_send()
        copy.wait_recv()
        return carry

    return lambda: lax.fori_loop(1, n, start, 0), lambda: lax.fori_loop(1, n, finish, 0)


def main_kernel(
    count, heads, n_seq, n_opt, skip_ref, w_ref, log_ref, layer_hbm, x_hbm, dy_hbm, gx_ref, gbc_ref,
    proj, running, decay, *scratch,
):
    gather_scratch, states_scratch = scratch[:GATHER_SCRATCH], scratch[GATHER_SCRATCH:]
    chain_in = states_scratch[10]
    x_ref, dy_ref, load = states_scratch[12:15]
    pieces = load.shape[1]
    wide = x_ref.shape[1] // pieces

    def bring(k):
        lanes = pl.ds(pl.multiple_of(k * wide, wide), wide)
        pairs = ((x_hbm, x_ref), (dy_hbm, dy_ref))
        return [
            pltpu.make_async_copy(source.at[:, lanes], held.at[:, lanes], load.at[n, k])
            for n, (source, held) in enumerate(pairs)
        ]

    def bring_all():
        for k in range(pieces):
            for copy in bring(k):
                copy.start()
        pair = lax.axis_index("seq") // 2
        for way, end in enumerate((0, n_seq // 2 - 1)):
            @pl.when(pair == end)
            def _():
                chain_in[way] = jnp.zeros_like(chain_in[way])

    end_sends = gather_part(
        count, n_seq, n_opt, bring_all, w_ref, log_ref, layer_hbm, proj, running, decay,
        *gather_scratch,
    )
    states_part(
        count, heads, n_seq // 2, bring, skip_ref, proj, running, decay, gx_ref, gbc_ref,
        *states_scratch,
    )
    end_sends()


def begin_swap(*args):
    start, finish = swap_all(*args)
    start()
    return finish


def step_kernel(
    n_seq, n_opt, layer_ref, grad_ref, w_ref, code_ref, scale_ref, row_ref, col_ref,
    update_ref, code_out, small_out,
    grad_turned, part_ref, take_core, give_two, keep_two, take_two, give_three, keep_three, take_three, give_pair, take_pair,
    stats, all_stats, peak, all_peaks,
    send_core, recv_core, send_two, recv_two, send_three, recv_three, send_pair, recv_pair,
    send_c, recv_c, send_d, recv_d,
):
    seq = lax.axis_index("seq")
    opt = lax.axis_index("opt")
    n = n_seq * n_opt
    n_pairs = n_seq // 2
    me = seq * n_opt + opt
    pair, side, cross, core, twins = place_of(seq, opt)
    core_twin, cross_twin, side_twin = twins

    def any_device(i):
        return (i // n_opt, lax.rem(i, n_opt))

    greeted = greet_twins(n_pairs, seq, opt)
    targets = ((cross_twin, side_twin), (side_twin, cross_twin))
    own = ((cross, side), (side, cross))
    order = [pair_at(pair, n_pairs - 1 - d, n_pairs) for d in range(n_pairs)]

    def first(p):
        return remote(
            part_ref.at[1 - core, :, p], take_core.at[:, p], send_core.at[p], recv_core.at[p],
            core_twin,
        )

    def second(k, p):
        return remote(
            give_two.at[k, p], take_two.at[k, p], send_two.at[k, p], recv_two.at[k, p],
            targets[0][k],
        )

    def third(k, p):
        return remote(
            give_three.at[k, p], take_three.at[k, p], send_three.at[k, p], recv_three.at[k, p],
            targets[1][k],
        )

    def chip_sum(k, p, a, b):
        r = a * 2 + b if k == 0 else b * 2 + a
        return part_ref[core, k, p, r].astype(f32) + take_core[k, p, r].astype(f32)

    def slice_sum(k, p):
        return keep_three[k, p] + take_three[k, p].astype(f32)

    def to_pair(p, source):
        return remote(
            give_pair.at[p], take_pair.at[source], send_pair.at[p], recv_pair.at[source],
            (p * 2 + side, opt),
        )

    grad_turned[...] = jnp.transpose(grad_ref[...].astype(f32)).astype(bf16)
    _, _, _, n_r, half, own_rows = part_ref.shape
    reach = 2 * n_r * own_rows

    def fill_part(p):
        columns = pl.ds(pl.multiple_of(p * reach, reach), reach)
        both = dot_nn(grad_turned[...], layer_ref[:, columns]).astype(bf16)
        for t in range(n_r):
            for c in range(2):
                lanes = slice((2 * t + c) * own_rows, (2 * t + c + 1) * own_rows)
                for k in range(2):
                    part_ref[c, k, p, t] = both[k * half : (k + 1) * half, lanes]

    for n_done, p in enumerate(order):
        fill_part(p)
        if n_done == 0:
            greeted()
        first(p).start()
    for p in order:
        first(p).wait()
        for k in range(2):
            for a in range(2):
                give_two[k, p, a] = chip_sum(k, p, a, 1 - own[0][k]).astype(bf16)
            second(k, p).start()
    for p in order:
        for k in range(2):
            for a in range(2):
                keep_two[k, p, a] = chip_sum(k, p, a, own[0][k])

    def finish_third(p):
        for k in range(2):
            third(k, p).wait()

        if p is not order[-1]:
            for k in range(2):
                give_pair[p, k] = slice_sum(k, p).astype(bf16)
            to_pair(p, pair).start()

    for n_done, p in enumerate(order):
        for k in range(2):
            second(k, p).wait()
            a = 1 - own[1][k]
            total = keep_two[k, p, a] + take_two[k, p, a].astype(f32)
            give_three[k, p] = total.astype(bf16)
            third(k, p).start()
            a = own[1][k]
            keep_three[k, p] = keep_two[k, p, a] + take_two[k, p, a].astype(f32)
        if n_done > 0:
            finish_third(order[n_done - 1])
    finish_third(order[-1])
    take_pair[pair] = jnp.zeros_like(take_pair[pair])
    totals = [slice_sum(k, pair) for k in range(2)]
    turned = jnp.concatenate(totals, axis=0)

    def end_slices(distance, carry):
        p = lax.rem(pair + distance, n_pairs)
        to_pair(p, p).wait()
        return carry

    lax.fori_loop(1, n_pairs, end_slices, 0)

    def gather_pair(p, total):
        return total + jnp.concatenate([take_pair[p, k].astype(f32) for k in range(2)], axis=0)

    turned = lax.fori_loop(0, n_pairs, gather_pair, turned)
    grad = jnp.transpose(turned)

    rows, cols = grad.shape
    width = n * rows
    stats[:, :cols] = jnp.sum(grad * grad, axis=0, keepdims=True)
    row_stat = row_ref[...]
    stats[:, cols:] = jnp.broadcast_to(jnp.sum(row_stat, axis=1, keepdims=True), (1, LANES))
    end_stats = begin_swap(
        n, me, lambda i: stats, lambda i: all_stats.at[i], any_device, send_c, recv_c
    )
    row_raw = jnp.sum(turned * turned, axis=0, keepdims=True)
    old_moment = beta_one * code_ref[...].astype(f32) * scale_ref[...]
    end_stats()
    all_stats[me] = stats[...]
    sums = all_stats[0]
    for i in range(1, n):
        sums += all_stats[i]
    col_raw = sums[:, :cols]
    old_total = sums[:, cols : cols + 1]
    raw_total = jnp.sum(col_raw, axis=1, keepdims=True)
    factor = jnp.minimum(1.0, clip_norm / jnp.sqrt(raw_total + norm_floor))
    moment = old_moment + (1.0 - beta_one) * (grad * factor)
    peak[...] = jnp.max(jnp.abs(moment), axis=0, keepdims=True)
    end_peaks = begin_swap(
        n, me, lambda i: peak, lambda i: all_peaks.at[i], any_device, send_d, recv_d
    )
    col_next = beta_two * col_ref[...] + (1.0 - beta_two) * (
        factor * factor * col_raw / width + tiny_square
    )
    row_next = beta_two * row_stat + (1.0 - beta_two) * (
        factor * factor * row_raw / cols + tiny_square
    )
    row_mean = (
        beta_two * old_total
        + (1.0 - beta_two) * (factor * factor * raw_total / cols + width * tiny_square)
    ) / width
    small_out[1:2, :] = col_next
    small_out[2:3, :rows] = row_next
    row_column = jnp.transpose(jnp.broadcast_to(row_next / row_mean, (8, rows)))[:, :1]
    second_moment = row_column * col_next
    update_ref[...] = moment / (jnp.sqrt(second_moment) + adam_floor) + weight_decay * w_ref[...]
    end_peaks()
    all_peaks[me] = peak[...]
    scale_next = all_peaks[0]
    for i in range(1, n):
        scale_next = jnp.maximum(scale_next, all_peaks[i])
    scale_next = scale_next + peak_floor
    small_out[0:1, :] = scale_next
    code_out[...] = (moment / scale_next).astype(bf16)


def hand_out(
    gx_ref, update_ref, code_ref, small_ref,
    gx_out, update_out, code_out, scale_out, row_out, col_out, store,
):
    pieces = store.shape[0]
    tall = gx_ref.shape[0] // pieces
    puts = [
        pltpu.make_async_copy(
            gx_ref.at[k * tall : (k + 1) * tall], gx_out.at[k * tall : (k + 1) * tall], store.at[k]
        )
        for k in range(pieces)
    ]
    for put in puts:
        put.start()
    update_out[...] = update_ref[...]
    code_out[...] = code_ref[...]
    scale_out[...] = small_ref[0:1, :]
    col_out[...] = small_ref[1:2, :]
    row_out[...] = small_ref[2:3, : row_out.shape[1]]
    for put in puts:
        put.wait()


def params(mebibytes, **more):
    return pltpu.CompilerParams(vmem_limit_bytes=mebibytes * 1024 * 1024, **more)


def whole():
    return pl.BlockSpec(memory_space=pltpu.VMEM)


def dma(*counts):
    return [pltpu.SemaphoreType.DMA((count,)) for count in counts for _ in range(2)]


def per_device(
    n_seq, n_opt, layer_in, ssm_input, grad_out, log_decay, skip_gain, w_bc, m_code, m_scale,
    row_stat, col_stat,
):
    layer_rows = layer_in[0]
    x = ssm_input[0]
    dy = grad_out[0]
    length, width = layer_rows.shape
    heads = skip_gain.shape[0]
    head_dim = x.shape[1] // heads
    state_dim = w_bc.shape[1] // 2
    count = length // BLOCK
    n_pairs = n_seq // 2
    own_rows = w_bc.shape[0]

    in_hbm = pl.BlockSpec(memory_space=pltpu.MemorySpace.HBM)
    per_head = (heads, 2, state_dim, head_dim)
    inner_states = (heads, max(count - 1, 1), state_dim, head_dim)
    gather_scratch = (
        [
            pltpu.VMEM((n_pairs, 2, 2, 2, own_rows, 2 * state_dim), bf16),
            pltpu.VMEM((length, width), bf16),
            pltpu.VMEM((length, 2 * state_dim), f32),
            pltpu.SemaphoreType.DMA,
            pltpu.SemaphoreType.DMA,
            pltpu.SemaphoreType.DMA,
        ]
        + [pltpu.SemaphoreType.DMA((n_pairs,))] * 2
        + [pltpu.SemaphoreType.DMA((2, n_pairs))] * 4
        + [pltpu.SemaphoreType.DMA((4, n_pairs))] * 2
    )
    states_scratch = [
        pltpu.VMEM((state_dim, length), f32),
        pltpu.VMEM((state_dim, length), f32),
        pltpu.VMEM((count, BLOCK, BLOCK), f32),
        pltpu.VMEM((count, BLOCK, BLOCK), f32),
        pltpu.VMEM((length, state_dim), f32),
        pltpu.VMEM((length, state_dim), f32),
        pltpu.VMEM(inner_states, bf16),
        pltpu.VMEM(inner_states, bf16),
        pltpu.VMEM(per_head, bf16),
        pltpu.VMEM(per_head, bf16),
        pltpu.VMEM((2, heads, state_dim, head_dim), bf16),
        pltpu.VMEM((3,) + per_head, bf16),
        pltpu.VMEM(x.shape, bf16),
        pltpu.VMEM(x.shape, bf16),
        pltpu.SemaphoreType.DMA((2, 8)),
        pltpu.SemaphoreType.DMA((heads,)),
        pltpu.SemaphoreType.DMA((heads,)),
        pltpu.SemaphoreType.DMA((2, heads)),
        pltpu.SemaphoreType.DMA((2, heads)),
    ]
    grad_input, grad_bc = pl.pallas_call(
        functools.partial(main_kernel, count, heads, n_seq, n_opt),
        in_specs=[pl.BlockSpec(memory_space=pltpu.SMEM), whole(), whole(), in_hbm, in_hbm, in_hbm],
        out_specs=[whole()] * 2,
        out_shape=[
            jax.ShapeDtypeStruct(x.shape, bf16),
            jax.ShapeDtypeStruct((length, 2 * state_dim), bf16),
        ],
        scratch_shapes=[
            pltpu.VMEM((length, 2 * state_dim), bf16),
            pltpu.VMEM((heads, count, BLOCK), f32),
            pltpu.VMEM((2, heads, 1, LANES), f32),
        ]
        + gather_scratch
        + states_scratch,
        compiler_params=params(46, collective_id=0, has_side_effects=True),
        name="gather_states_and_grads",
    )(skip_gain, w_bc, log_decay[0], layer_rows, x, dy)

    cols = 2 * state_dim
    n = n_seq * n_opt
    block = (state_dim, own_rows)
    tall = jax.ShapeDtypeStruct((own_rows, cols), f32)
    code = jax.ShapeDtypeStruct((own_rows, cols), bf16)
    results = pl.pallas_call(
        functools.partial(step_kernel, n_seq, n_opt),
        in_specs=[whole()] * 7,
        out_specs=[whole()] * 3,
        out_shape=[tall, code, jax.ShapeDtypeStruct((8, cols), f32)],
        scratch_shapes=[
            pltpu.VMEM((cols, length), bf16),
            pltpu.VMEM((2, 2, n_pairs, 4) + block, bf16),
            pltpu.VMEM((2, n_pairs, 4) + block, bf16),
            pltpu.VMEM((2, n_pairs, 2) + block, bf16),
            pltpu.VMEM((2, n_pairs, 2) + block, f32),
            pltpu.VMEM((2, n_pairs, 2) + block, bf16),
            pltpu.VMEM((2, n_pairs) + block, bf16),
            pltpu.VMEM((2, n_pairs) + block, f32),
            pltpu.VMEM((2, n_pairs) + block, bf16),
            pltpu.VMEM((n_pairs, 2) + block, bf16),
            pltpu.VMEM((n_pairs, 2) + block, bf16),
            pltpu.VMEM((1, cols + LANES), f32),
            pltpu.VMEM((n, 1, cols + LANES), f32),
            pltpu.VMEM((1, cols), f32),
            pltpu.VMEM((n, 1, cols), f32),
        ]
        + dma(n_pairs)
        + [pltpu.SemaphoreType.DMA((2, n_pairs))] * 4
        + dma(n_pairs, n, n),
        compiler_params=params(40, collective_id=1, has_side_effects=True),
        name="sum_and_step",
    )(layer_rows, grad_bc, w_bc, m_code, m_scale[None, :], row_stat[None, :], col_stat[None, :])
    grad_input, update, code_next, scale_next, row_next, col_next = pl.pallas_call(
        hand_out,
        in_specs=[whole()] * 4,
        out_specs=[in_hbm] + [whole()] * 5,
        out_shape=[
            jax.ShapeDtypeStruct(x.shape, bf16), tall, code, jax.ShapeDtypeStruct((1, cols), f32),
            jax.ShapeDtypeStruct((1, own_rows), f32), jax.ShapeDtypeStruct((1, cols), f32),
        ],
        scratch_shapes=[pltpu.SemaphoreType.DMA((8,))],
        compiler_params=params(28),
        name="hand_out",
    )(grad_input, *results)
    return (grad_input[None], update, code_next, scale_next[0], row_next[0], col_next[0])


def solution(mesh):
    return jax.shard_map(
        functools.partial(per_device, mesh.shape["seq"], mesh.shape["opt"]),
        mesh=mesh,
        in_specs=(
            P("opt", "seq", None),
            P("opt", "seq", None),
            P("opt", "seq", None),
            P("opt", None, "seq"),
            P(),
            P(("seq", "opt"), None),
            P(("seq", "opt"), None),
            P(),
            P(("seq", "opt")),
            P(),
        ),
        out_specs=(
            P("opt", "seq", None),
            P(("seq", "opt"), None),
            P(("seq", "opt"), None),
            P(),
            P(("seq", "opt")),
            P(),
        ),
        check_vma=False,
    )
```

```python
import functools

import jax
import jax.numpy as jnp
from jax import lax
from jax.experimental import pallas as pl
from jax.experimental.pallas import tpu as pltpu
from jax.sharding import PartitionSpec as P

BLOCK = 256
LANES = 128
LAG_SWAP = 3
LAG_CHAIN = 3
GATHER_SCRATCH = 14

beta_one = 0.9
beta_two = 0.95
weight_decay = 0.1
clip_norm = 1.0
tiny_square = 1e-30
adam_floor = 1e-08
peak_floor = 1e-06
norm_floor = 1e-06
highest = lax.Precision.HIGHEST
MESH = pl.DeviceIdType.MESH
f32 = jnp.float32
bf16 = jnp.bfloat16


def dot_nn(a, b):
    return lax.dot_general(a, b, (((1,), (0,)), ((), ())), preferred_element_type=f32)


def dot_nt(a, b):
    return lax.dot_general(a, b, (((1,), (1,)), ((), ())), preferred_element_type=f32)


def dot_tn(a, b):
    return lax.dot_general(a, b, (((0,), (0,)), ((), ())), preferred_element_type=f32)


def as_column(row):
    return jnp.transpose(jnp.broadcast_to(row, (LANES, row.shape[1])))


def widened(column, length):
    return jnp.concatenate([column] * (length // LANES), axis=1)


def gather_part(
    count, n_seq, n_opt, bring_all, w_ref, log_ref, layer_ref, proj_ref, run_ref, decay,
    got, layer, total, load, send_e, recv_e, send_a, recv_a, send_b, recv_b, send_c, recv_c, send_d, recv_d,
):
    seq = lax.axis_index("seq")
    opt = lax.axis_index("opt")
    n_pairs = n_seq // 2
    pair, side, cross, core, twins = place_of(seq, opt)
    core_twin, cross_twin, side_twin = twins
    half = w_ref.shape[0] // 2
    low, high = slice(0, half), slice(half, 2 * half)

    def same(part, send_sem, recv_sem, device):
        return remote(part, part, send_sem, recv_sem, device)

    def along(p, owner):
        block = got.at[owner, side, cross, core]
        other = (p * 2 + side, opt)
        return remote(block, block, send_a.at[p], recv_a.at[owner], other)

    def own_to(k, p, s, x):
        device = (cross_twin, side_twin)[k]
        return same(got.at[p, s, x, core], send_b.at[k, p], recv_b.at[k, p], device)

    def relay_to(k, p, s, x):
        device = (cross_twin, side_twin)[k]
        part = got.at[p, s, x, core, (low, high)[k]]
        return same(part, send_c.at[k, p], recv_c.at[k, p], device)

    def to_core(k, p, c):
        s = side if k % 2 == 0 else 1 - side
        x = cross if k // 2 == 0 else 1 - cross
        return same(got.at[p, s, x, c], send_d.at[k, p], recv_d.at[k, p], core_twin)

    def decay_copy():
        return remote(decay.at[0], decay.at[1], send_e, recv_e, side_twin)

    layer_copy = pltpu.make_async_copy(layer_ref, layer, load)
    layer_copy.start()
    greeted = greet_twins(n_pairs, seq, opt)
    got[pair, side, cross, core] = w_ref[...].astype(bf16)
    greeted()

    def send_along(distance, carry):
        along(pair_at(pair, n_pairs - distance, n_pairs), pair).start()
        return carry

    lax.fori_loop(1, n_pairs, send_along, 0)
    bring_all()
    ones = (
        lax.broadcasted_iota(jnp.int32, (BLOCK, BLOCK), 0)
        <= lax.broadcasted_iota(jnp.int32, (BLOCK, BLOCK), 1)
    ).astype(f32)

    def turn(d, carry):
        @pl.when(d < n_pairs)
        def _():
            p = pair_at(pair, d, n_pairs)

            @pl.when(d > 0)
            def _():
                along(p, p).wait_recv()

            own_to(0, p, side, cross).start()
            own_to(1, p, side, cross).start()
            to_core(0, p, core).start()

        @pl.when(d == 0)
        def _():
            closing = None
            for b in range(count):
                sums = jnp.dot(
                    log_ref[:, b * BLOCK : (b + 1) * BLOCK], ones,
                    precision=highest, preferred_element_type=f32,
                )
                run_ref[:, b : b + 1, :] = sums[:, None, :]
                tail = sums[:, BLOCK - 1 :]
                closing = tail if closing is None else closing + tail
            decay[0] = jnp.broadcast_to(jnp.exp(closing), (closing.shape[0], LANES))[:, None, :]
            total[...] = jnp.zeros_like(total)

        @pl.when(d == 1)
        def _():
            decay_copy().start()

        @pl.when(jnp.logical_and(d >= 1, d < n_pairs + 1))
        def _():
            p = pair_at(pair, d - 1, n_pairs)
            own_to(0, p, side, 1 - cross).wait_recv()
            relay_to(1, p, side, 1 - cross).start()
            own_to(1, p, 1 - side, cross).wait_recv()
            relay_to(0, p, 1 - side, cross).start()
            to_core(1, p, core).start()
            to_core(2, p, core).start()

        @pl.when(jnp.logical_and(d >= 2, d < n_pairs + 2))
        def _():
            p = pair_at(pair, d - 2, n_pairs)
            relay_to(0, p, 1 - side, 1 - cross).wait_recv()
            relay_to(1, p, 1 - side, 1 - cross).wait_recv()
            to_core(3, p, core).start()

        @pl.when(d == 3)
        def _():
            layer_copy.wait()

        @pl.when(d >= 3)
        def _():
            p = pair_at(pair, d - 3, n_pairs)
            for k in range(4):
                to_core(k, p, 1 - core).wait_recv()
            w_part = got[p].reshape(-1, got.shape[-1])
            depth = w_part.shape[0]
            columns = pl.ds(pl.multiple_of(p * depth, depth), depth)
            total[...] += dot_nn(layer[:, columns], w_part)

        return carry

    lax.fori_loop(0, n_pairs + 3, turn, 0)
    proj_ref[...] = total[...].astype(bf16)
    decay_copy().wait()

    def sent(d, carry):
        p = lax.rem(pair + d, n_pairs)

        @pl.when(d > 0)
        def _():
            along(p, pair).wait_send()

        own_to(0, p, side, cross).wait_send()
        own_to(1, p, side, cross).wait_send()
        relay_to(0, p, 1 - side, cross).wait_send()
        relay_to(1, p, side, 1 - cross).wait_send()
        for k in range(4):
            to_core(k, p, core).wait_send()
        return carry

    return lambda: lax.fori_loop(0, n_pairs, sent, 0)


def pair_at(pair, distance, n_pairs):
    step = jnp.where(2 * pair < n_pairs, distance, n_pairs - distance)
    return lax.rem(pair + step, n_pairs)


def place_of(seq, opt):
    side, core, cross = lax.rem(seq, 2), lax.rem(opt, 2), opt // 2
    twins = (
        (seq, opt + 1 - 2 * core), (seq, opt + 2 - 4 * cross), (seq + 1 - 2 * side, opt)
    )
    return seq // 2, side, cross, core, twins


def greet_twins(n_pairs, seq, opt):
    barrier = pltpu.get_barrier_semaphore()
    pair, side, cross, core, twins = place_of(seq, opt)

    def hello(device):
        pl.semaphore_signal(barrier, inc=1, device_id=device, device_id_type=MESH)

    def hello_pair(distance, carry):
        hello((lax.rem(pair + distance, n_pairs) * 2 + side, opt))
        return carry

    for device in twins:
        hello(device)
    lax.fori_loop(1, n_pairs, hello_pair, 0)
    return lambda: pl.semaphore_wait(barrier, n_pairs + 2)


def remote(src, dst, send_sem, recv_sem, device):
    return pltpu.make_async_remote_copy(
        src_ref=src, dst_ref=dst, send_sem=send_sem, recv_sem=recv_sem,
        device_id=device, device_id_type=MESH,
    )


def states_part(
    count, heads, n_pairs, bring, skip_ref, proj_ref, run_ref, decay_ref, gx_ref, gbc_ref,
    b_turned, c_turned, affinity, mixing, acc_b, acc_c, starts, outs, mine, got, chain_in, chain_out,
    x_ref, dy_ref, load, send_y, recv_y, send_c, recv_c,
):
    seq = lax.axis_index("seq")
    opt = lax.axis_index("opt")
    pair = seq // 2
    side = lax.rem(seq, 2)
    state_dim = proj_ref.shape[1] // 2
    head_dim = x_ref.shape[1] // heads
    b_cols, c_cols = slice(0, state_dim), slice(state_dim, 2 * state_dim)
    twin = (seq + 1 - 2 * side, opt)
    ahead = (seq + 2, opt)
    behind = (seq - 2, opt)
    has_source = (pair > 0, pair < n_pairs - 1)
    has_target = (pair < n_pairs - 1, pair > 0)
    places = (pair, n_pairs - 1 - pair)

    late = 5 * heads // 16
    early = 5 * heads // 16
    reach = LAG_CHAIN * (n_pairs - 1)
    wait = max(0, reach - heads + late)
    swap_lag = late + LAG_SWAP
    steps = max(heads - late + reach, heads + wait) + swap_lag

    def head_of(slot):
        return jnp.where(
            slot < early, slot, jnp.where(slot < heads - late, slot + late, slot - heads + late + early)
        )

    def lanes_of(h):
        return pl.ds(pl.multiple_of(h * head_dim, head_dim), head_dim)

    def closings_of(h):
        return [run_ref[h, b : b + 1, BLOCK - 1 : BLOCK] for b in range(count)]

    def swap(h):
        return remote(mine.at[h], got.at[h], send_y.at[h], recv_y.at[h], twin)

    def swap_late(h):
        return remote(chain_out.at[2, h], got.at[h], send_y.at[h], recv_y.at[h], twin)

    def pass_on(way, h):
        return remote(
            chain_out.at[way, h, 0], chain_in.at[way, h], send_c.at[way, h], recv_c.at[way, h],
            (ahead, behind)[way],
        )

    def hop(way, h, with_other):
        @pl.when(has_source[way])
        def _():
            pass_on(way, h).wait_recv()

        @pl.when(has_target[way])
        def _():
            own_decay = decay_ref[0, h]
            other_decay = decay_ref[1, h]
            first = side == way
            own_scale = jnp.where(first, other_decay, 1.0)
            total = (
                own_decay * other_decay * chain_in[way, h].astype(f32)
                + own_scale * mine[h, way].astype(f32)
            )
            if with_other:
                other_scale = jnp.where(first, 1.0, own_decay)
                total += other_scale * got[h, way].astype(f32)
            chain_out[way, h, 0] = total.astype(bf16)
            pass_on(way, h).start()

    def end_hops(h):
        for way in range(2):
            @pl.when(has_target[way])
            def _():
                pass_on(way, h).wait_send()

    def local(h):
        adds = []
        for b in range(count):
            rows = slice(b * BLOCK, (b + 1) * BLOCK)
            row = run_ref[h, b : b + 1, :]
            closing = row[:, BLOCK - 1 : BLOCK]
            b_scaled = (b_turned[:, rows] * jnp.exp(closing - row)).astype(bf16)
            c_scaled = (c_turned[:, rows] * jnp.exp(row)).astype(bf16)
            x_blk = x_ref[rows, lanes_of(h)]
            dy_blk = dy_ref[rows, lanes_of(h)]
            adds.append((jnp.exp(closing), dot_nn(b_scaled, x_blk), dot_nn(c_scaled, dy_blk)))
        state = adds[0][1]
        for b in range(1, count):
            starts[h, b - 1] = state.astype(bf16)
            state = adds[b][0] * state + adds[b][1]
        mine[h, 0] = state.astype(bf16)
        carried = adds[count - 1][2]
        for b in reversed(range(count - 1)):
            outs[h, b] = carried.astype(bf16)
            carried = adds[b][0] * carried + adds[b][2]
        mine[h, 1] = carried.astype(bf16)

    def finish(h, swapped_late):
        row_pos = lax.broadcasted_iota(jnp.int32, (BLOCK, BLOCK), 0)
        col_pos = lax.broadcasted_iota(jnp.int32, (BLOCK, BLOCK), 1)
        closings = closings_of(h)
        other_decay = decay_ref[1, h]
        fars = []
        for way in range(2):
            second = side != way
            scale = jnp.where(second, other_decay, 1.0)
            extra = jnp.where(jnp.logical_or(second, swapped_late), jnp.ones((1, LANES), f32), 0.0)
            fars.append(scale * chain_in[way, h].astype(f32) + extra * got[h, way].astype(f32))
        far_state, far_grad = fars
        for b in range(count):
            rows = slice(b * BLOCK, (b + 1) * BLOCK)
            row = run_ref[h, b : b + 1, :]
            column = as_column(row)
            before = sum(closings[:b], jnp.zeros((1, 1), f32))
            after = sum(closings[b + 1 :], jnp.zeros((1, 1), f32))
            if b == 0:
                state_in = far_state.astype(bf16)
            else:
                state_in = (starts[h, b - 1].astype(f32) + jnp.exp(before) * far_state).astype(bf16)
            if b == count - 1:
                grad_in = far_grad.astype(bf16)
            else:
                grad_in = (outs[h, b].astype(f32) + jnp.exp(after) * far_grad).astype(bf16)
            grow = jnp.exp(column)
            shrink = jnp.exp(closings[b] - column)
            x_blk = x_ref[rows, lanes_of(h)]
            dy_blk = dy_ref[rows, lanes_of(h)]
            spread = row - widened(column, BLOCK)
            decays = jnp.exp(jnp.where(col_pos >= row_pos, spread, -jnp.inf))
            mixing[b] += decays * dot_nt(x_blk, dy_blk)
            weighted = (decays * affinity[b]).astype(bf16)
            inner = dot_nn(weighted, dy_blk)
            outer = dot_nn(proj_ref[rows, b_cols], grad_in) * shrink
            full = inner + outer + skip_ref[h] * dy_blk.astype(f32)
            gx_ref[rows, lanes_of(h)] = full.astype(bf16)
            acc_c[rows, :] += grow * dot_nt(dy_blk, state_in)
            acc_b[rows, :] += shrink * dot_nt(x_blk, grad_in)

    piece_heads = heads // load.shape[1]

    b_turned[...] = jnp.transpose(proj_ref[:, b_cols].astype(f32))
    c_turned[...] = jnp.transpose(proj_ref[:, c_cols].astype(f32))
    def step(i, carry):
        is_late = jnp.logical_and(i >= early, i < early + late)

        @pl.when(jnp.logical_and(i < heads, lax.rem(i, piece_heads) == 0))
        def _():
            for copy in bring(i // piece_heads):
                copy.wait()

        @pl.when(i < heads)
        def _():
            local(i)

            @pl.when(jnp.logical_not(is_late))
            def _():
                swap(i).start()

        @pl.when(i == early)
        def _():
            mixing[...] = jnp.zeros_like(mixing)
            acc_b[...] = jnp.zeros_like(acc_b)
            acc_c[...] = jnp.zeros_like(acc_c)
            for b in range(count):
                rows = slice(b * BLOCK, (b + 1) * BLOCK)
                affinity[b] = dot_nt(proj_ref[rows, b_cols], proj_ref[rows, c_cols])

        for way in range(2):
            h = i - 1 - LAG_CHAIN * places[way]

            @pl.when(jnp.logical_and(h >= early, h < early + late))
            def _():
                hop(way, h, False)

        slot = i - late - wait

        @pl.when(jnp.logical_and(slot >= heads - late, slot < heads))
        def _():
            h = head_of(slot)
            own_decay = decay_ref[0, h]
            for way in range(2):
                first = side == way
                scale = jnp.where(first, own_decay, 1.0)
                extra = jnp.where(first, jnp.ones((1, LANES), f32), 0.0)
                total = scale * chain_in[way, h].astype(f32) + extra * mine[h, way].astype(f32)
                chain_out[2, h, way] = total.astype(bf16)
            swap_late(h).start()

        slot = i - swap_lag

        @pl.when(jnp.logical_and(slot >= 0, slot < heads - late))
        def _():
            swap(head_of(slot)).wait()

        for way in range(2):
            slot = i - swap_lag - LAG_CHAIN * places[way]

            @pl.when(jnp.logical_and(slot >= 0, slot < heads - late))
            def _():
                hop(way, head_of(slot), True)

        slot = i - swap_lag - reach

        @pl.when(jnp.logical_and(slot >= 0, slot < heads - late))
        def _():
            finish(head_of(slot), False)
            end_hops(head_of(slot))

        slot = i - swap_lag - wait

        @pl.when(jnp.logical_and(slot >= heads - late, slot < heads))
        def _():
            h = head_of(slot)
            swap_late(h).wait()
            finish(h, True)
            end_hops(h)

        return carry

    lax.fori_loop(0, steps, step, 0)
    for b in range(count):
        rows = slice(b * BLOCK, (b + 1) * BLOCK)
        mixed = mixing[b].astype(bf16)
        gbc_ref[rows, b_cols] = (acc_b[rows, :] + dot_nn(mixed, proj_ref[rows, c_cols])).astype(bf16)
        gbc_ref[rows, c_cols] = (acc_c[rows, :] + dot_tn(mixed, proj_ref[rows, b_cols])).astype(bf16)


def swap_all(n, me, src_of, dst_of, device_of, send_sem, recv_sem):
    def copy_to(distance):
        other = lax.rem(me + distance, n)
        return pltpu.make_async_remote_copy(
            src_ref=src_of(other), dst_ref=dst_of(me), send_sem=send_sem.at[other],
            recv_sem=recv_sem.at[me], device_id=device_of(other), device_id_type=MESH,
        )

    def copy_from(distance):
        other = lax.rem(me + distance, n)
        return pltpu.make_async_remote_copy(
            src_ref=src_of(other), dst_ref=dst_of(other), send_sem=send_sem.at[other],
            recv_sem=recv_sem.at[other], device_id=device_of(other), device_id_type=MESH,
        )

    def start(distance, carry):
        copy_to(distance).start()
        return carry

    def arrived(distance, carry):
        copy_from(distance).wait_recv()
        return carry

    def left(distance, carry):
        copy_from(distance).wait_send()
        return carry

    return [functools.partial(lax.fori_loop, 1, n, body, 0) for body in (start, arrived, left)]


def main_kernel(
    count, heads, n_seq, n_opt, skip_ref, w_ref, log_ref, layer_hbm, x_hbm, dy_hbm, gx_ref, gbc_ref,
    proj, running, decay, *scratch,
):
    gather_scratch, states_scratch = scratch[:GATHER_SCRATCH], scratch[GATHER_SCRATCH:]
    chain_in = states_scratch[10]
    x_ref, dy_ref, load = states_scratch[12:15]
    pieces = load.shape[1]
    wide = x_ref.shape[1] // pieces

    def bring(k):
        lanes = pl.ds(pl.multiple_of(k * wide, wide), wide)
        pairs = ((x_hbm, x_ref), (dy_hbm, dy_ref))
        return [
            pltpu.make_async_copy(source.at[:, lanes], held.at[:, lanes], load.at[n, k])
            for n, (source, held) in enumerate(pairs)
        ]

    def bring_all():
        for k in range(pieces):
            for copy in bring(k):
                copy.start()
        pair = lax.axis_index("seq") // 2
        for way, end in enumerate((0, n_seq // 2 - 1)):
            @pl.when(pair == end)
            def _():
                chain_in[way] = jnp.zeros_like(chain_in[way])

    end_sends = gather_part(
        count, n_seq, n_opt, bring_all, w_ref, log_ref, layer_hbm, proj, running, decay,
        *gather_scratch,
    )
    states_part(
        count, heads, n_seq // 2, bring, skip_ref, proj, running, decay, gx_ref, gbc_ref,
        *states_scratch,
    )
    end_sends()


def begin_swap(*args):
    start, arrived, left = swap_all(*args)
    start()
    return arrived, left


def step_kernel(
    n_seq, n_opt, layer_ref, grad_ref, w_ref, code_ref, scale_ref, row_ref, col_ref,
    update_ref, code_out, small_out,
    grad_turned, part_ref, take_core, give_two, keep_two, take_two, give_three, keep_three, take_three, give_pair, take_pair,
    stats, all_stats, peak, all_peaks,
    send_core, recv_core, send_two, recv_two, send_three, recv_three, send_pair, recv_pair,
    send_c, recv_c, send_d, recv_d,
):
    seq = lax.axis_index("seq")
    opt = lax.axis_index("opt")
    n = n_seq * n_opt
    n_pairs = n_seq // 2
    me = seq * n_opt + opt
    pair, side, cross, core, twins = place_of(seq, opt)
    core_twin, cross_twin, side_twin = twins

    def any_device(i):
        return (i // n_opt, lax.rem(i, n_opt))

    greeted = greet_twins(n_pairs, seq, opt)
    targets = ((cross_twin, side_twin), (side_twin, cross_twin))
    own = ((cross, side), (side, cross))
    order = [pair_at(pair, n_pairs - 1 - d, n_pairs) for d in range(n_pairs)]

    def first(p):
        return remote(
            part_ref.at[1 - core, :, p], take_core.at[:, p], send_core.at[p], recv_core.at[p],
            core_twin,
        )

    def second(k, p):
        return remote(
            give_two.at[k, p], take_two.at[k, p], send_two.at[k, p], recv_two.at[k, p],
            targets[0][k],
        )

    def third(k, p):
        return remote(
            give_three.at[k, p], take_three.at[k, p], send_three.at[k, p], recv_three.at[k, p],
            targets[1][k],
        )

    def chip_sum(k, p, a, b):
        r = a * 2 + b if k == 0 else b * 2 + a
        return part_ref[core, k, p, r].astype(f32) + take_core[k, p, r].astype(f32)

    def slice_sum(k, p):
        return keep_three[k, p] + take_three[k, p].astype(f32)

    def to_pair(p, source):
        return remote(
            give_pair.at[p], take_pair.at[source], send_pair.at[p], recv_pair.at[source],
            (p * 2 + side, opt),
        )

    grad_turned[...] = jnp.transpose(grad_ref[...].astype(f32)).astype(bf16)
    _, _, _, n_r, half, own_rows = part_ref.shape
    reach = 2 * n_r * own_rows

    def fill_part(p):
        columns = pl.ds(pl.multiple_of(p * reach, reach), reach)
        both = dot_nn(grad_turned[...], layer_ref[:, columns]).astype(bf16)
        for t in range(n_r):
            for c in range(2):
                lanes = slice((2 * t + c) * own_rows, (2 * t + c + 1) * own_rows)
                for k in range(2):
                    part_ref[c, k, p, t] = both[k * half : (k + 1) * half, lanes]

    for n_done, p in enumerate(order):
        fill_part(p)
        if n_done == 0:
            greeted()
        first(p).start()
    for p in order:
        first(p).wait()
        for k in range(2):
            for a in range(2):
                give_two[k, p, a] = chip_sum(k, p, a, 1 - own[0][k]).astype(bf16)
            second(k, p).start()
    for p in order:
        for k in range(2):
            for a in range(2):
                keep_two[k, p, a] = chip_sum(k, p, a, own[0][k])

    def finish_third(p):
        for k in range(2):
            third(k, p).wait()

        if p is not order[-1]:
            for k in range(2):
                give_pair[p, k] = slice_sum(k, p).astype(bf16)
            to_pair(p, pair).start()

    for n_done, p in enumerate(order):
        for k in range(2):
            second(k, p).wait()
            a = 1 - own[1][k]
            total = keep_two[k, p, a] + take_two[k, p, a].astype(f32)
            give_three[k, p] = total.astype(bf16)
            third(k, p).start()
            a = own[1][k]
            keep_three[k, p] = keep_two[k, p, a] + take_two[k, p, a].astype(f32)
        if n_done > 0:
            finish_third(order[n_done - 1])
    finish_third(order[-1])
    take_pair[pair] = jnp.zeros_like(take_pair[pair])
    totals = [slice_sum(k, pair) for k in range(2)]
    turned = jnp.concatenate(totals, axis=0)

    def end_slices(distance, carry):
        p = lax.rem(pair + distance, n_pairs)
        to_pair(p, p).wait()
        return carry

    lax.fori_loop(1, n_pairs, end_slices, 0)

    def gather_pair(p, total):
        return total + jnp.concatenate([take_pair[p, k].astype(f32) for k in range(2)], axis=0)

    turned = lax.fori_loop(0, n_pairs, gather_pair, turned)
    grad = jnp.transpose(turned)

    rows, cols = grad.shape
    width = n * rows
    stats[:, :cols] = jnp.sum(grad * grad, axis=0, keepdims=True)
    row_stat = row_ref[...]
    stats[:, cols:] = jnp.broadcast_to(jnp.sum(row_stat, axis=1, keepdims=True), (1, LANES))
    end_stats, stats_left = begin_swap(
        n, me, lambda i: stats, lambda i: all_stats.at[i], any_device, send_c, recv_c
    )
    row_raw = jnp.sum(turned * turned, axis=0, keepdims=True)
    old_moment = beta_one * code_ref[...].astype(f32) * scale_ref[...]
    end_stats()
    all_stats[me] = stats[...]
    sums = all_stats[0]
    for i in range(1, n):
        sums += all_stats[i]
    col_raw = sums[:, :cols]
    old_total = sums[:, cols : cols + 1]
    raw_total = jnp.sum(col_raw, axis=1, keepdims=True)
    factor = jnp.minimum(1.0, clip_norm / jnp.sqrt(raw_total + norm_floor))
    moment = old_moment + (1.0 - beta_one) * (grad * factor)
    peak[...] = jnp.max(jnp.abs(moment), axis=0, keepdims=True)
    end_peaks, peaks_left = begin_swap(
        n, me, lambda i: peak, lambda i: all_peaks.at[i], any_device, send_d, recv_d
    )
    col_next = beta_two * col_ref[...] + (1.0 - beta_two) * (
        factor * factor * col_raw / width + tiny_square
    )
    row_next = beta_two * row_stat + (1.0 - beta_two) * (
        factor * factor * row_raw / cols + tiny_square
    )
    row_mean = (
        beta_two * old_total
        + (1.0 - beta_two) * (factor * factor * raw_total / cols + width * tiny_square)
    ) / width
    small_out[1:2, :] = col_next
    small_out[2:3, :rows] = row_next
    row_column = jnp.transpose(jnp.broadcast_to(row_next / row_mean, (8, rows)))[:, :1]
    second_moment = row_column * col_next
    update_ref[...] = moment / (jnp.sqrt(second_moment) + adam_floor) + weight_decay * w_ref[...]
    stats_left()
    end_peaks()
    all_peaks[me] = peak[...]
    scale_next = all_peaks[0]
    for i in range(1, n):
        scale_next = jnp.maximum(scale_next, all_peaks[i])
    scale_next = scale_next + peak_floor
    small_out[0:1, :] = scale_next
    code_out[...] = (moment / scale_next).astype(bf16)
    peaks_left()


def hand_out(
    gx_ref, update_ref, code_ref, small_ref,
    gx_out, update_out, code_out, scale_out, row_out, col_out, store,
):
    pieces = store.shape[0]
    tall = gx_ref.shape[0] // pieces
    puts = [
        pltpu.make_async_copy(
            gx_ref.at[k * tall : (k + 1) * tall], gx_out.at[k * tall : (k + 1) * tall], store.at[k]
        )
        for k in range(pieces)
    ]
    for put in puts:
        put.start()
    update_out[...] = update_ref[...]
    code_out[...] = code_ref[...]
    scale_out[...] = small_ref[0:1, :]
    col_out[...] = small_ref[1:2, :]
    row_out[...] = small_ref[2:3, : row_out.shape[1]]
    for put in puts:
        put.wait()


def params(mebibytes, **more):
    return pltpu.CompilerParams(vmem_limit_bytes=mebibytes * 1024 * 1024, **more)


def whole():
    return pl.BlockSpec(memory_space=pltpu.VMEM)


def dma(*counts):
    return [pltpu.SemaphoreType.DMA((count,)) for count in counts for _ in range(2)]


def per_device(
    n_seq, n_opt, layer_in, ssm_input, grad_out, log_decay, skip_gain, w_bc, m_code, m_scale,
    row_stat, col_stat,
):
    layer_rows = layer_in[0]
    x = ssm_input[0]
    dy = grad_out[0]
    length, width = layer_rows.shape
    heads = skip_gain.shape[0]
    head_dim = x.shape[1] // heads
    state_dim = w_bc.shape[1] // 2
    count = length // BLOCK
    n_pairs = n_seq // 2
    own_rows = w_bc.shape[0]

    in_hbm = pl.BlockSpec(memory_space=pltpu.MemorySpace.HBM)
    per_head = (heads, 2, state_dim, head_dim)
    inner_states = (heads, max(count - 1, 1), state_dim, head_dim)
    gather_scratch = (
        [
            pltpu.VMEM((n_pairs, 2, 2, 2, own_rows, 2 * state_dim), bf16),
            pltpu.VMEM((length, width), bf16),
            pltpu.VMEM((length, 2 * state_dim), f32),
            pltpu.SemaphoreType.DMA,
            pltpu.SemaphoreType.DMA,
            pltpu.SemaphoreType.DMA,
        ]
        + [pltpu.SemaphoreType.DMA((n_pairs,))] * 2
        + [pltpu.SemaphoreType.DMA((2, n_pairs))] * 4
        + [pltpu.SemaphoreType.DMA((4, n_pairs))] * 2
    )
    states_scratch = [
        pltpu.VMEM((state_dim, length), f32),
        pltpu.VMEM((state_dim, length), f32),
        pltpu.VMEM((count, BLOCK, BLOCK), f32),
        pltpu.VMEM((count, BLOCK, BLOCK), f32),
        pltpu.VMEM((length, state_dim), f32),
        pltpu.VMEM((length, state_dim), f32),
        pltpu.VMEM(inner_states, bf16),
        pltpu.VMEM(inner_states, bf16),
        pltpu.VMEM(per_head, bf16),
        pltpu.VMEM(per_head, bf16),
        pltpu.VMEM((2, heads, state_dim, head_dim), bf16),
        pltpu.VMEM((3,) + per_head, bf16),
        pltpu.VMEM(x.shape, bf16),
        pltpu.VMEM(x.shape, bf16),
        pltpu.SemaphoreType.DMA((2, 8)),
        pltpu.SemaphoreType.DMA((heads,)),
        pltpu.SemaphoreType.DMA((heads,)),
        pltpu.SemaphoreType.DMA((2, heads)),
        pltpu.SemaphoreType.DMA((2, heads)),
    ]
    grad_input, grad_bc = pl.pallas_call(
        functools.partial(main_kernel, count, heads, n_seq, n_opt),
        in_specs=[pl.BlockSpec(memory_space=pltpu.SMEM), whole(), whole(), in_hbm, in_hbm, in_hbm],
        out_specs=[whole()] * 2,
        out_shape=[
            jax.ShapeDtypeStruct(x.shape, bf16),
            jax.ShapeDtypeStruct((length, 2 * state_dim), bf16),
        ],
        scratch_shapes=[
            pltpu.VMEM((length, 2 * state_dim), bf16),
            pltpu.VMEM((heads, count, BLOCK), f32),
            pltpu.VMEM((2, heads, 1, LANES), f32),
        ]
        + gather_scratch
        + states_scratch,
        compiler_params=params(46, collective_id=0, has_side_effects=True),
        name="gather_states_and_grads",
    )(skip_gain, w_bc, log_decay[0], layer_rows, x, dy)

    cols = 2 * state_dim
    n = n_seq * n_opt
    block = (state_dim, own_rows)
    tall = jax.ShapeDtypeStruct((own_rows, cols), f32)
    code = jax.ShapeDtypeStruct((own_rows, cols), bf16)
    results = pl.pallas_call(
        functools.partial(step_kernel, n_seq, n_opt),
        in_specs=[whole()] * 7,
        out_specs=[whole()] * 3,
        out_shape=[tall, code, jax.ShapeDtypeStruct((8, cols), f32)],
        scratch_shapes=[
            pltpu.VMEM((cols, length), bf16),
            pltpu.VMEM((2, 2, n_pairs, 4) + block, bf16),
            pltpu.VMEM((2, n_pairs, 4) + block, bf16),
            pltpu.VMEM((2, n_pairs, 2) + block, bf16),
            pltpu.VMEM((2, n_pairs, 2) + block, f32),
            pltpu.VMEM((2, n_pairs, 2) + block, bf16),
            pltpu.VMEM((2, n_pairs) + block, bf16),
            pltpu.VMEM((2, n_pairs) + block, f32),
            pltpu.VMEM((2, n_pairs) + block, bf16),
            pltpu.VMEM((n_pairs, 2) + block, bf16),
            pltpu.VMEM((n_pairs, 2) + block, bf16),
            pltpu.VMEM((1, cols + LANES), f32),
            pltpu.VMEM((n, 1, cols + LANES), f32),
            pltpu.VMEM((1, cols), f32),
            pltpu.VMEM((n, 1, cols), f32),
        ]
        + dma(n_pairs)
        + [pltpu.SemaphoreType.DMA((2, n_pairs))] * 4
        + dma(n_pairs, n, n),
        compiler_params=params(40, collective_id=1, has_side_effects=True),
        name="sum_and_step",
    )(layer_rows, grad_bc, w_bc, m_code, m_scale[None, :], row_stat[None, :], col_stat[None, :])
    grad_input, update, code_next, scale_next, row_next, col_next = pl.pallas_call(
        hand_out,
        in_specs=[whole()] * 4,
        out_specs=[in_hbm] + [whole()] * 5,
        out_shape=[
            jax.ShapeDtypeStruct(x.shape, bf16), tall, code, jax.ShapeDtypeStruct((1, cols), f32),
            jax.ShapeDtypeStruct((1, own_rows), f32), jax.ShapeDtypeStruct((1, cols), f32),
        ],
        scratch_shapes=[pltpu.SemaphoreType.DMA((8,))],
        compiler_params=params(28),
        name="hand_out",
    )(grad_input, *results)
    return (grad_input[None], update, code_next, scale_next[0], row_next[0], col_next[0])


def solution(mesh):
    return jax.shard_map(
        functools.partial(per_device, mesh.shape["seq"], mesh.shape["opt"]),
        mesh=mesh,
        in_specs=(
            P("opt", "seq", None),
            P("opt", "seq", None),
            P("opt", "seq", None),
            P("opt", None, "seq"),
            P(),
            P(("seq", "opt"), None),
            P(("seq", "opt"), None),
            P(),
            P(("seq", "opt")),
            P(),
        ),
        out_specs=(
            P("opt", "seq", None),
            P(("seq", "opt"), None),
            P(("seq", "opt"), None),
            P(),
            P(("seq", "opt")),
            P(),
        ),
        check_vma=False,
    )
```
